32 devices in a mesh: dp: 1 (over z), cp: 4 (over y), tp: 8 (over x, core).
Axes of the slice: x: 4, y: 4, z: 1, core: 2. Of those that a mesh axis runs over, the one named last changes fastest.
The devices are a block of a 4x4x8 slice.
Arguments:
- hidden_in: bfloat16 [6144, 2048], P(('dp', 'cp', 'tp'))
- w_query: bfloat16 [2048, 16, 128], P(None, 'tp')
- w_key: bfloat16 [2048, 16, 128], P(None, 'tp')
- w_value: bfloat16 [2048, 16, 128], P(None, 'tp')
- w_out: bfloat16 [16, 128, 2048], P('tp')
- expert_idx: int32 [6144, 8], P(('dp', 'cp', 'tp'))
- gate_vals: float32 [6144, 8], P(('dp', 'cp', 'tp'))
- w_gate: bfloat16 [64, 2048, 1024], P(('cp', 'tp'))
- w_up: bfloat16 [64, 2048, 1024], P(('cp', 'tp'))
- w_down: bfloat16 [64, 1024, 2048], P(('cp', 'tp'))
Outputs:
- output: bfloat16 [6144, 2048], P(('dp', 'cp', 'tp'))
All inputs are finite; a program needn't handle non-finite values.
Results may differ from the reference program's by a relative error of at most 0.0150772.
Values are sent between devices in bfloat16 or wider.
A program may use at most 768 MiB of HBM per device.

```python
import jax
import jax.numpy as jnp
from jax import lax

HIDDEN = 2048
FFN_DIM = 1024
Q_HEADS = 16
KV_HEADS = 16
HEAD_DIM = 128
EXPERTS = 64
TOP_K = 8
DEV_LIMIT = 8
TOK_DEV = 192
CP_DEVS = 4
TP_DEVS = 8

GROUP_DEVS = CP_DEVS * TP_DEVS
SEQ_LEN = TOK_DEV * GROUP_DEVS
BLOCK_ROWS = SEQ_LEN // CP_DEVS
CHUNK_ROWS = BLOCK_ROWS // 2
QUERY_ROWS = min(64, SEQ_LEN)
PER_EXPERT = SEQ_LEN * TOP_K // EXPERTS


def draw_routing(rand_key):
    local_exp = EXPERTS // GROUP_DEVS
    per_dev = TOK_DEV * DEV_LIMIT // GROUP_DEVS
    per_tok = TOP_K // DEV_LIMIT
    capacity = TOK_DEV * TOP_K // EXPERTS
    key_dev, key_loc, key_tok = jax.random.split(rand_key, 3)
    dev_perm = jax.vmap(lambda sub_key: jax.random.permutation(sub_key, GROUP_DEVS))(jax.random.split(key_dev, GROUP_DEVS))
    loc_perm = jax.vmap(lambda sub_key: jax.random.permutation(sub_key, local_exp))(jax.random.split(key_loc, GROUP_DEVS * GROUP_DEVS)).reshape(GROUP_DEVS, GROUP_DEVS, local_exp)
    tok_perm = jax.vmap(lambda sub_key: jax.random.permutation(sub_key, TOK_DEV))(jax.random.split(key_tok, GROUP_DEVS))
    place_ids = jnp.arange(TOK_DEV)[:, None] + TOK_DEV * jnp.arange(DEV_LIMIT)[None, :]
    dev_block = place_ids // per_dev
    dev_rank = place_ids - dev_block * per_dev
    target = dev_perm[:, dev_block]
    sub_place = dev_rank[:, :, None] + per_dev * jnp.arange(per_tok)[None, None, :]
    loc_block = sub_place // capacity
    src_ids = jnp.arange(GROUP_DEVS)[:, None, None, None]
    local_ids = loc_perm[src_ids, target[:, :, :, None], loc_block[None]]
    expert = target[:, :, :, None] * local_exp + local_ids
    expert = expert.reshape(GROUP_DEVS, TOK_DEV, TOP_K)
    expert = jnp.take_along_axis(expert, tok_perm[:, :, None], axis=1)
    return expert.reshape(SEQ_LEN, TOP_K).astype(jnp.int32)


def setup_inputs(seed: int = 0, part: int = 0) -> dict:
    base_key = jax.random.key(seed)
    shared = jax.random.split(base_key, 7)
    own = jax.random.split(jax.random.fold_in(base_key, part), 3)
    q_scale = 2.0 * HIDDEN ** -0.5
    hidden_in = jax.random.normal(own[0], (SEQ_LEN, HIDDEN), jnp.float32)
    w_query = q_scale * jax.random.normal(shared[0], (HIDDEN, Q_HEADS, HEAD_DIM), jnp.float32)
    w_key = q_scale * jax.random.normal(shared[1], (HIDDEN, KV_HEADS, HEAD_DIM), jnp.float32)
    w_value = HIDDEN ** -0.5 * jax.random.normal(shared[2], (HIDDEN, KV_HEADS, HEAD_DIM), jnp.float32)
    w_out = (Q_HEADS * HEAD_DIM) ** -0.5 * jax.random.normal(shared[3], (Q_HEADS, HEAD_DIM, HIDDEN), jnp.float32)
    w_gate = HIDDEN ** -0.5 * jax.random.normal(shared[4], (EXPERTS, HIDDEN, FFN_DIM), jnp.float32)
    w_up = HIDDEN ** -0.5 * jax.random.normal(shared[5], (EXPERTS, HIDDEN, FFN_DIM), jnp.float32)
    w_down = FFN_DIM ** -0.5 * jax.random.normal(shared[6], (EXPERTS, FFN_DIM, HIDDEN), jnp.float32)
    expert_idx = draw_routing(own[1])
    gate_vals = jax.random.uniform(own[2], (SEQ_LEN, TOP_K), jnp.float32, 0.2, 0.6)
    return dict(hidden_in=hidden_in.astype(jnp.bfloat16), w_query=w_query.astype(jnp.bfloat16), w_key=w_key.astype(jnp.bfloat16), w_value=w_value.astype(jnp.bfloat16), w_out=w_out.astype(jnp.bfloat16), expert_idx=expert_idx, gate_vals=gate_vals, w_gate=w_gate.astype(jnp.bfloat16), w_up=w_up.astype(jnp.bfloat16), w_down=w_down.astype(jnp.bfloat16))


def row_positions(row_ids):
    block_id = row_ids // BLOCK_ROWS
    offset_in = row_ids % BLOCK_ROWS
    return jnp.where(offset_in < CHUNK_ROWS, block_id * CHUNK_ROWS + offset_in, (2 * CP_DEVS - 1 - block_id) * CHUNK_ROWS + offset_in - CHUNK_ROWS)


def reference(hidden_in, w_query, w_key, w_value, w_out, expert_idx, gate_vals, w_gate, w_up, w_down):
    group_size = Q_HEADS // KV_HEADS
    position = row_positions(jnp.arange(SEQ_LEN))
    query_vecs = jnp.dot(hidden_in, w_query.reshape(HIDDEN, -1), preferred_element_type=jnp.float32).astype(jnp.bfloat16)
    key_vecs = jnp.dot(hidden_in, w_key.reshape(HIDDEN, -1), preferred_element_type=jnp.float32).astype(jnp.bfloat16)
    value_vecs = jnp.dot(hidden_in, w_value.reshape(HIDDEN, -1), preferred_element_type=jnp.float32).astype(jnp.bfloat16)
    query_vecs = query_vecs.astype(jnp.float32).reshape(SEQ_LEN // QUERY_ROWS, QUERY_ROWS, KV_HEADS, group_size, HEAD_DIM)
    key_vecs = key_vecs.astype(jnp.float32).reshape(SEQ_LEN, KV_HEADS, HEAD_DIM)
    value_vecs = value_vecs.astype(jnp.float32).reshape(SEQ_LEN, KV_HEADS, HEAD_DIM)
    score_scale = HEAD_DIM ** -0.5

    def attend(operands):
        q_blk, q_place = operands
        scores = jnp.einsum('qgrd,kgd->qgrk', q_blk, key_vecs) * score_scale
        allowed = position[None, None, None, :] <= q_place[:, None, None, None]
        scores = jnp.where(allowed, scores, -1e30)
        attn_prob = jax.nn.softmax(scores, axis=-1)
        attn_out = jnp.einsum('qgrk,kgd->qgrd', attn_prob, value_vecs)
        return attn_out.reshape(QUERY_ROWS, Q_HEADS * HEAD_DIM).astype(jnp.bfloat16)

    attn_all = lax.map(attend, (query_vecs, position.reshape(-1, QUERY_ROWS))).reshape(SEQ_LEN, Q_HEADS * HEAD_DIM)
    proj_sum = jnp.dot(attn_all, w_out.reshape(-1, HIDDEN), preferred_element_type=jnp.float32)
    resid_f = (hidden_in.astype(jnp.float32) + proj_sum).astype(jnp.bfloat16).astype(jnp.float32)
    sort_order = jnp.argsort(expert_idx.reshape(-1), stable=True)
    tok_rows = (sort_order // TOP_K).reshape(EXPERTS, PER_EXPERT)

    def expert_fn(operands):
        row_ids, gate_w, up_w, down_w = operands
        rows_in = resid_f[row_ids]
        gate_act = jnp.dot(rows_in, gate_w.astype(jnp.float32), preferred_element_type=jnp.float32)
        up_act = jnp.dot(rows_in, up_w.astype(jnp.float32), preferred_element_type=jnp.float32)
        hidden_act = (jax.nn.silu(gate_act) * up_act).astype(jnp.bfloat16).astype(jnp.float32)
        return jnp.dot(hidden_act, down_w.astype(jnp.float32), preferred_element_type=jnp.float32).astype(jnp.bfloat16)

    expert_out = lax.map(expert_fn, (tok_rows, w_gate, w_up, w_down)).reshape(SEQ_LEN * TOP_K, HIDDEN)
    inverse = jnp.argsort(sort_order)
    per_choice = expert_out[inverse].reshape(SEQ_LEN, TOP_K, HIDDEN).astype(jnp.float32)
    moe_sum = jnp.sum(gate_vals[:, :, None] * per_choice, axis=1)
    return (resid_f + moe_sum).astype(jnp.bfloat16)
```

```python
import functools
import math
import jax
import jax.numpy as jnp
from jax import lax
from jax.experimental import pallas as pl
from jax.experimental.pallas import tpu as pltpu
from jax.sharding import PartitionSpec as P

MESH = pl.DeviceIdType.MESH


def row_positions(row_ids, block_rows, cp_devs):
    chunk_rows = block_rows // 2
    block_id = row_ids // block_rows
    offset_in = row_ids % block_rows
    return jnp.where(offset_in < chunk_rows, block_id * chunk_rows + offset_in, (2 * cp_devs - 1 - block_id) * chunk_rows + offset_in - chunk_rows)


def attend_blocks(query_vecs, key_all, value_all, q_position, k_position):
    row_count, kv_heads, group_size, head_dim = query_vecs.shape
    q_block = math.gcd(row_count, 128)
    n_blocks = row_count // q_block
    score_scale = head_dim ** -0.5

    def one_block(operands):
        q_blk, q_place = operands
        scores = jnp.einsum('qgrd,kgd->qgrk', q_blk, key_all, preferred_element_type=jnp.float32) * score_scale
        allowed = k_position[None, None, None, :] <= q_place[:, None, None, None]
        scores = jnp.where(allowed, scores, -1e30)
        attn_prob = jax.nn.softmax(scores, axis=-1).astype(jnp.bfloat16)
        attn_out = jnp.einsum('qgrk,kgd->qgrd', attn_prob, value_all, preferred_element_type=jnp.float32)
        return attn_out.astype(jnp.bfloat16)

    blocks = lax.map(one_block, (query_vecs.reshape(n_blocks, q_block, kv_heads, group_size, head_dim), q_position.reshape(n_blocks, q_block)))
    return blocks.reshape(row_count, kv_heads * group_size * head_dim)


def attention_residual(hidden_in, w_query, w_key, w_value, w_out, cp_devs):
    hidden = hidden_in.shape[1]
    kv_heads = w_key.shape[1]
    head_dim = w_key.shape[2]
    group_size = w_query.shape[1] // kv_heads
    gathered = lax.all_gather(hidden_in, 'tp', axis=0, tiled=True)
    block_rows = gathered.shape[0]
    query_vecs = jnp.dot(gathered, w_query.reshape(hidden, -1), preferred_element_type=jnp.float32).astype(jnp.bfloat16).reshape(block_rows, kv_heads, group_size, head_dim)
    key_loc = jnp.dot(gathered, w_key.reshape(hidden, -1), preferred_element_type=jnp.float32).astype(jnp.bfloat16)
    value_loc = jnp.dot(gathered, w_value.reshape(hidden, -1), preferred_element_type=jnp.float32).astype(jnp.bfloat16)
    key_all = lax.all_gather(key_loc, 'cp', axis=0, tiled=True).reshape(-1, kv_heads, head_dim)
    value_all = lax.all_gather(value_loc, 'cp', axis=0, tiled=True).reshape(-1, kv_heads, head_dim)
    cp_rank = lax.axis_index('cp')
    q_position = row_positions(cp_rank * block_rows + jnp.arange(block_rows), block_rows, cp_devs)
    k_position = row_positions(jnp.arange(block_rows * cp_devs), block_rows, cp_devs)
    attn_all = attend_blocks(query_vecs, key_all, value_all, q_position, k_position)
    part_sum = jnp.dot(attn_all, w_out.reshape(-1, hidden), preferred_element_type=jnp.float32)
    reduced = lax.psum_scatter(part_sum, 'tp', scatter_dimension=0, tiled=True)
    return (hidden_in.astype(jnp.float32) + reduced).astype(jnp.bfloat16)


def moe_kernel(dims, h_in, idx_ref, gate_ref, wg_hbm, wu_hbm, wd_hbm, y_ref,
               wg, wu, wd, send, recv, ret, slots, gates, dmat, gmat, acc, hid,
               wsem, ssem, rsem, bsem, csem):
    n_cp, n_x, top_k, experts, cap, local_exp = dims
    per_grp = 2 * n_x
    rows = h_in.shape[0]
    hidden = h_in.shape[1]
    cp, tp = lax.axis_index('cp'), lax.axis_index('tp')
    x_pos, core = tp // 2, tp % 2

    def fwd(j, r):
        dx, dc = r // 2, r % 2
        return (cp + (dx + j) % n_cp) % n_cp, ((x_pos + dx) % n_x) * 2 + (core + dc) % 2

    def back(j, r):
        dx, dc = r // 2, r % 2
        return (cp + n_cp - (dx + j) % n_cp) % n_cp, ((x_pos + n_x - dx) % n_x) * 2 + (core + dc) % 2

    barrier = pltpu.get_barrier_semaphore()
    for j in range(n_cp):
        for r in range(per_grp):
            if j or r:
                c, t = fwd(j, r)
                pl.semaphore_signal(barrier, inc=1, device_id={'cp': c, 'tp': t}, device_id_type=MESH)
    loads = [pltpu.make_async_copy(wg_hbm, wg, wsem.at[0]), pltpu.make_async_copy(wu_hbm, wu, wsem.at[1]), pltpu.make_async_copy(wd_hbm, wd, wsem.at[2])]
    for ld in loads:
        ld.start()

    e_iota = lax.broadcasted_iota(jnp.int32, (experts, rows), 0)
    hit = jnp.zeros((experts, rows), jnp.float32)
    gsel = jnp.zeros((experts, rows), jnp.float32)
    for k in range(top_k):
        m = idx_ref[k:k + 1, :] == e_iota
        hit = hit + jnp.where(m, 1.0, 0.0)
        gsel = gsel + jnp.where(m, gate_ref[k:k + 1, :], 0.0)
    before = jnp.where(lax.broadcasted_iota(jnp.int32, (rows, rows), 0) < lax.broadcasted_iota(jnp.int32, (rows, rows), 1), 1.0, 0.0)
    count = jnp.dot(hit.astype(jnp.bfloat16), before.astype(jnp.bfloat16), preferred_element_type=jnp.float32)
    slots[...] = jnp.where(hit > 0.5, count, -1.0)
    gates[...] = gsel
    c_iota = lax.broadcasted_iota(jnp.int32, (cap, rows), 0).astype(jnp.float32)

    def build(j, ref, gated):
        for e in range(local_exp):
            for r in range(per_grp):
                c, t = fwd(j, r)
                expert = (c * (2 * n_x) + t) * local_exp + e
                eq = jnp.broadcast_to(slots[pl.ds(expert, 1), :], (cap, rows)) == c_iota
                val = jnp.broadcast_to(gates[pl.ds(expert, 1), :], (cap, rows)) if gated else 1.0
                ref[pl.ds((e * per_grp + r) * cap, cap), :] = jnp.where(eq, val, 0.0)

    def dispatch(j, r):
        c, t = fwd(j, r)
        out = []
        for e in range(local_exp):
            if j == 0 and r == 0:
                out.append(pltpu.make_async_copy(send.at[j, e * per_grp + r], recv.at[j, e * per_grp + r], rsem.at[j, e * per_grp + r]))
            else:
                out.append(pltpu.make_async_remote_copy(send.at[j, e * per_grp + r], recv.at[j, e * per_grp + r], ssem.at[j, e * per_grp + r], rsem.at[j, e * per_grp + r], device_id={'cp': c, 'tp': t}, device_id_type=MESH))
        return out

    def giveback(j, r):
        c, t = back(j, r)
        out = []
        for e in range(local_exp):
            if j == 0 and r == 0:
                out.append(pltpu.make_async_copy(recv.at[j, e * per_grp + r], ret.at[j, e * per_grp + r], csem.at[j, e * per_grp + r]))
            else:
                out.append(pltpu.make_async_remote_copy(recv.at[j, e * per_grp + r], ret.at[j, e * per_grp + r], bsem.at[j, e * per_grp + r], csem.at[j, e * per_grp + r], device_id={'cp': c, 'tp': t}, device_id_type=MESH))
        return out

    grp_rows = local_exp * per_grp * cap
    half = per_grp * cap
    wide = 512
    order = [r for r in range(per_grp) if r >= 2] + [1, 0]
    for j in range(n_cp):
        build(j, dmat, False)

        def fill(n, carry, j=j):
            cols = pl.ds(pl.multiple_of(n * wide, wide), wide)
            picked = jnp.dot(dmat[...].astype(jnp.bfloat16), h_in[:, cols], preferred_element_type=jnp.float32).astype(jnp.bfloat16)
            send[j, :, :, cols] = picked.reshape(local_exp * per_grp, cap, wide)
            return carry

        lax.fori_loop(0, hidden // wide, fill, 0)
        if j == 0:
            pl.semaphore_wait(barrier, n_cp * per_grp - 1)
        for r in order:
            for cpy in dispatch(j, r):
                cpy.start()

    def init(n, carry):
        cols = pl.ds(pl.multiple_of(n * wide, wide), wide)
        acc[:, cols] = h_in[:, cols].astype(jnp.float32)
        return carry

    lax.fori_loop(0, hidden // wide, init, 0)
    for ld in loads:
        ld.wait()
    ffn = wg.shape[2]
    for j in range(n_cp):
        for r in order:
            for cpy in dispatch(j, r):
                if j == 0 and r == 0:
                    cpy.wait()
                else:
                    cpy.wait_recv()
        for e in range(local_exp):
            def up(n, carry, j=j, e=e):
                cols = pl.ds(pl.multiple_of(n * 256, 256), 256)
                rows_in = recv[j, pl.ds(e * per_grp, per_grp)].reshape(half, hidden)
                g = jnp.dot(rows_in, wg[e, :, cols], preferred_element_type=jnp.float32)
                u = jnp.dot(rows_in, wu[e, :, cols], preferred_element_type=jnp.float32)
                hid[:, cols] = (g * (1.0 / (1.0 + jnp.exp(-g))) * u).astype(jnp.bfloat16)
                return carry

            def down(n, carry, j=j, e=e):
                cols = pl.ds(pl.multiple_of(n * wide, wide), wide)
                z = jnp.dot(hid[...], wd[e, :, cols], preferred_element_type=jnp.float32).astype(jnp.bfloat16)
                recv[j, pl.ds(e * per_grp, per_grp), :, cols] = z.reshape(per_grp, cap, wide)
                return carry

            lax.fori_loop(0, ffn // 256, up, 0)
            lax.fori_loop(0, hidden // wide, down, 0)
            for r in order:
                giveback(j, r)[e].start()

    for j in range(n_cp):
        build(j, gmat, True)
        for r in order:
            for cpy in giveback(j, r):
                if j == 0 and r == 0:
                    cpy.wait()
                else:
                    cpy.wait_recv()

        def comb(n, carry, j=j):
            cols = pl.ds(pl.multiple_of(n * wide, wide), wide)
            g0 = gmat[...]
            hi = g0.astype(jnp.bfloat16)
            g1 = g0 - hi.astype(jnp.float32)
            mid = g1.astype(jnp.bfloat16)
            lo = (g1 - mid.astype(jnp.float32)).astype(jnp.bfloat16)
            z = ret[j, :, :, cols].reshape(grp_rows, wide)
            dims_t = (((0,), (0,)), ((), ()))
            tot = lax.dot_general(lo, z, dims_t, preferred_element_type=jnp.float32)
            tot = tot + lax.dot_general(mid, z, dims_t, preferred_element_type=jnp.float32)
            tot = tot + lax.dot_general(hi, z, dims_t, preferred_element_type=jnp.float32)
            acc[:, cols] += tot
            return carry

        lax.fori_loop(0, hidden // wide, comb, 0)

    def fin(n, carry):
        cols = pl.ds(pl.multiple_of(n * wide, wide), wide)
        y_ref[:, cols] = acc[:, cols].astype(jnp.bfloat16)
        return carry

    lax.fori_loop(0, hidden // wide, fin, 0)
    for j in range(n_cp):
        for r in range(per_grp):
            if j or r:
                for cpy in dispatch(j, r) + giveback(j, r):
                    cpy.wait_send()


def expert_layer(mesh, resid_h, expert_idx, gate_vals, w_gate, w_up, w_down):
    n_cp, n_x = mesh.shape['cp'], mesh.shape['tp'] // 2
    rows, hidden = resid_h.shape
    top_k = expert_idx.shape[1]
    local_exp, _, ffn = w_gate.shape
    experts = local_exp * n_cp * n_x * 2
    cap = rows * top_k // experts
    slots = local_exp * 2 * n_x
    dims = (n_cp, n_x, top_k, experts, cap, local_exp)
    vm = pl.BlockSpec(memory_space=pltpu.VMEM)
    hb = pl.BlockSpec(memory_space=pl.ANY)
    sems = [pltpu.SemaphoreType.DMA((n_cp, slots)) for _ in range(4)]
    return pl.pallas_call(
        functools.partial(moe_kernel, dims),
        out_shape=jax.ShapeDtypeStruct((rows, hidden), jnp.bfloat16),
        in_specs=[vm, vm, vm, hb, hb, hb],
        out_specs=vm,
        scratch_shapes=[
            pltpu.VMEM((local_exp, hidden, ffn), jnp.bfloat16),
            pltpu.VMEM((local_exp, hidden, ffn), jnp.bfloat16),
            pltpu.VMEM((local_exp, ffn, hidden), jnp.bfloat16),
            pltpu.VMEM((n_cp, slots, cap, hidden), jnp.bfloat16),
            pltpu.VMEM((n_cp, slots, cap, hidden), jnp.bfloat16),
            pltpu.VMEM((n_cp, slots, cap, hidden), jnp.bfloat16),
            pltpu.VMEM((experts, rows), jnp.float32),
            pltpu.VMEM((experts, rows), jnp.float32),
            pltpu.VMEM((slots * cap, rows), jnp.float32),
            pltpu.VMEM((slots * cap, rows), jnp.float32),
            pltpu.VMEM((rows, hidden), jnp.float32),
            pltpu.VMEM((2 * n_x * cap, ffn), jnp.bfloat16),
            pltpu.SemaphoreType.DMA((3,)),
        ] + sems,
        compiler_params=pltpu.CompilerParams(collective_id=1, has_side_effects=True, vmem_limit_bytes=64 * 1024 * 1024 - 65536),
        name='moe',
    )(resid_h, expert_idx.T, gate_vals.T, w_gate, w_up, w_down)


def solution(mesh):
    cp_devs = mesh.shape['cp']
    row_spec = P(('dp', 'cp', 'tp'), None)
    head_spec = P(None, 'tp', None)
    expert_spec = P(('cp', 'tp'), None, None)

    def device_step(hidden_in, w_query, w_key, w_value, w_out, expert_idx, gate_vals, w_gate, w_up, w_down):
        resid_h = attention_residual(hidden_in, w_query, w_key, w_value, w_out, cp_devs)
        return expert_layer(mesh, resid_h, expert_idx, gate_vals, w_gate, w_up, w_down)

    return jax.shard_map(device_step, mesh=mesh, in_specs=(row_spec, head_spec, head_spec, head_spec, P('tp', None, None), row_spec, row_spec, expert_spec, expert_spec, expert_spec), out_specs=row_spec, check_vma=False)
```

```python
import functools
import jax
import jax.numpy as jnp
from jax import lax
from jax.experimental import pallas as pl
from jax.experimental.pallas import tpu as pltpu
from jax.sharding import PartitionSpec as P

MESH = pl.DeviceIdType.MESH


def attn_kernel(dims, x_in, wqkv, wo, h_ref,
                xbuf, wall, snd, land, kvp, mask, osnd, oland, wfull,
                lsem, xs, xr, ws, wr, qs, qr, ks, kr, os_, orr, gs, gr, ps, pr):
    n_cp, n_x, hd = dims
    rows, hidden = x_in.shape
    half = rows // 2
    units = n_x // 2
    n_units = n_cp * n_x
    blk = units * rows
    bf, f32 = jnp.bfloat16, jnp.float32
    cp, tp = lax.axis_index('cp'), lax.axis_index('tp')
    x_pos, core = tp // 2, tp % 2
    head = x_pos * n_cp + cp
    nbr = lambda d: (x_pos + d + n_x) % n_x
    at_x = lambda xx: {'cp': cp, 'tp': xx * 2 + core}
    at_y = lambda yy: {'cp': yy, 'tp': tp}
    partner = {'cp': cp, 'tp': x_pos * 2 + 1 - core}

    def remote(src, dst, s_sem, r_sem, dev):
        return pltpu.make_async_remote_copy(src, dst, s_sem, r_sem, device_id=dev, device_id_type=MESH)

    def place(c, xx):
        hi = xx // units
        return (c * (1 - hi) + (2 * n_cp - 1 - c) * hi) * units + xx % units

    barrier = pltpu.get_barrier_semaphore()
    offs = [(dy, dx) for dy in range(n_cp) for dx in range(n_x) if dy or dx]
    for dy, dx in offs:
        pl.semaphore_signal(barrier, inc=1, device_id={'cp': (cp + dy) % n_cp, 'tp': nbr(dx) * 2 + core}, device_id_type=MESH)
    pl.semaphore_signal(barrier, inc=1, device_id=partner, device_id_type=MESH)
    load_w = pltpu.make_async_copy(wqkv, wall.at[core], lsem.at[0])
    load_o = pltpu.make_async_copy(wo, wfull.at[tp], lsem.at[1])
    load_w.start()
    load_o.start()
    pl.semaphore_wait(barrier, len(offs) + 1)

    parts = [pl.ds(0, half), pl.ds(half, half)]
    def x_own(d, p):
        slot = 0 if d == 1 else n_x - 2
        return remote(x_in.at[parts[p]], xbuf.at[slot, parts[p]], xs.at[slot, p], xr.at[slot, p], at_x(nbr(d)))

    def x_fwd(d):
        slot, p = (0, 0) if d == 1 else (n_x - 2, 1)
        return remote(xbuf.at[slot, parts[p]], xbuf.at[1, parts[p]], xs.at[1, p], xr.at[1, p], at_x(nbr(d)))

    for d, p in ((1, 0), (-1, 1), (1, 1), (-1, 0)):
        x_own(d, p).start()
    w_part = remote(wqkv, wall.at[core], gs.at[0], gr.at[0], partner)
    w_part.start()

    r_io = lax.broadcasted_iota(jnp.int32, (blk, blk), 0)
    c_io = lax.broadcasted_iota(jnp.int32, (blk, blk), 1)
    q_pos = r_io + jnp.where(r_io >= rows, rows, 0) + core * rows
    k_pos = c_io + jnp.where(c_io >= rows, rows, 0)
    mask[:, 0:blk] = jnp.where(k_pos + core * rows <= q_pos, 1.0, 0.0)
    mask[:, blk:] = jnp.where(k_pos + (1 - core) * rows <= q_pos, 1.0, 0.0)

    def q_send(s, dy):
        u = place(cp, nbr(-s))
        return remote(snd.at[s, dy - 1], land.at[u], qs.at[s, dy - 1], qr.at[s, dy - 1], at_y((cp + dy) % n_cp))

    def q_recv(s, dy):
        u = place((cp - dy + n_cp) % n_cp, nbr(-s))
        return remote(snd.at[s, dy - 1], land.at[u], qs.at[s, dy - 1], qr.at[s, dy - 1], at_y((cp + dy) % n_cp))

    def kv_send(s, dy):
        u = place((cp - dy + n_cp) % n_cp, nbr(-s))
        return remote(land.at[u, :, pl.ds(hd, 2 * hd)], kvp.at[u], ks.at[s, dy], kr.at[s, dy], partner)

    def project(s):
        for dy in (1, n_cp - 1, 2, 0):
            i = (cp + dy) % n_cp
            cols = pl.ds(pl.multiple_of((i % 2) * 3 * hd, 3 * hd), 3 * hd)
            xv = x_in[...] if s == 0 else xbuf[s - 1]
            res = jnp.dot(xv, wall[i // 2, :, cols], preferred_element_type=f32).astype(bf)
            if dy:
                snd[s, dy - 1] = res
                q_send(s, dy).start()
            else:
                land[place(cp, nbr(-s))] = res
                kv_send(s, 0).start()

    def relay(s):
        for dy in (1, n_cp - 1, 2):
            q_recv(s, dy).wait_recv()
            kv_send(s, dy).start()

    load_w.wait()
    w_part.wait()
    project(0)
    x_own(1, 0).wait_recv()
    x_fwd(1).start()
    x_own(-1, 1).wait_recv()
    x_fwd(-1).start()

    def w_own(d, p):
        slot = 0 if d == 1 else n_x - 2
        return remote(wfull.at[tp, w_parts[p]], wfull.at[tp, w_parts[p]], ws.at[slot, p], wr.at[slot, p], at_x(nbr(d)))

    def w_fwd(d):
        p = 0 if d == 1 else 1
        t = nbr(-d) * 2 + core
        return remote(wfull.at[t, w_parts[p]], wfull.at[t, w_parts[p]], ws.at[1, p], wr.at[1, p], at_x(nbr(d)))

    def w_pass(s):
        t = nbr(-s) * 2 + core
        return remote(wfull.at[t], wfull.at[t], ps.at[s], pr.at[s], partner)

    w_half = wo.shape[0] // 2
    w_parts = [pl.ds(0, w_half), pl.ds(w_half, w_half)]
    load_o.wait()
    for d, p in ((1, 0), (-1, 1), (1, 1), (-1, 0)):
        w_own(d, p).start()
    w_pass(0).start()

    x_own(1, 1).wait_recv()
    project(1)
    x_own(-1, 0).wait_recv()
    project(n_x - 1)
    relay(0)
    x_fwd(1).wait_recv()
    x_fwd(-1).wait_recv()
    project(2)
    for s in (1, n_x - 1, 2):
        relay(s)
    for s in range(n_x):
        for dy in range(n_cp):
            kv_send(s, dy).wait_recv()

    c_exp = hd ** -0.5 * 1.4426950408889634
    nt = (((1,), (1,)), ((), ()))

    def o_copy(b, u):
        hi = b // n_cp
        dst_cp = b * (1 - hi) + (2 * n_cp - 1 - b) * hi
        dst_x = hi * units + u
        cols = pl.ds(pl.multiple_of(head * hd, hd), hd)
        cpy = remote(osnd.at[b * units + u], oland.at[:, cols], os_.at[b * units + u], orr.at[head], {'cp': dst_cp, 'tp': dst_x * 2 + core})
        own = jnp.logical_and(dst_cp == cp, dst_x == x_pos)
        return cpy, own, cols

    def step(b, t, carry, masked):
        mx, den, acc = carry
        q = land[pl.ds(b * units, units), :, 0:hd].reshape(blk, hd)
        own_u = pl.ds(t * units, units)
        k1 = land[own_u, :, hd:2 * hd].reshape(blk, hd)
        k2 = kvp[own_u, :, 0:hd].reshape(blk, hd)
        s1 = lax.dot_general(q, k1, nt, preferred_element_type=f32)
        s2 = lax.dot_general(q, k2, nt, preferred_element_type=f32)
        if masked:
            s1 = jnp.where(mask[:, 0:blk] > 0.5, s1, -1e30)
            s2 = jnp.where(mask[:, blk:] > 0.5, s2, -1e30)
        top = jnp.maximum(jnp.max(s1, axis=1, keepdims=True), jnp.max(s2, axis=1, keepdims=True))
        new = jnp.maximum(mx, top)
        keep = jnp.exp2((mx - new) * c_exp)
        p1 = jnp.exp2((s1 - new) * c_exp)
        p2 = jnp.exp2((s2 - new) * c_exp)
        den = den * keep + jnp.sum(p1, axis=1, keepdims=True) + jnp.sum(p2, axis=1, keepdims=True)
        v1 = land[own_u, :, 2 * hd:3 * hd].reshape(blk, hd)
        v2 = kvp[own_u, :, hd:2 * hd].reshape(blk, hd)
        acc = acc * keep + jnp.dot(p1.astype(bf), v1, preferred_element_type=f32) + jnp.dot(p2.astype(bf), v2, preferred_element_type=f32)
        return new, den, acc

    def attend(b, carry):
        @pl.when(b == RELAY_AT)
        def _():
            for d, p in ((1, 0), (-1, 1)):
                w_own(d, p).wait_recv()
                w_fwd(d).start()
            for d, p in ((1, 1), (-1, 0)):
                w_own(d, p).wait_recv()
            w_pass(1).start()
            w_pass(n_x - 1).start()

        start = (jnp.full((blk, 1), -1e30, f32), jnp.zeros((blk, 1), f32), jnp.zeros((blk, hd), f32))
        start = step(b, b, start, True)
        mx, den, acc = lax.fori_loop(0, b, lambda t, c: step(b, t, c, False), start)
        o = (acc / den).astype(bf)
        for u in range(units):
            cpy, own, cols = o_copy(b, u)
            osnd[b * units + u] = o[u * rows:(u + 1) * rows]

            @pl.when(own)
            def _():
                oland[:, cols] = o[u * rows:(u + 1) * rows]

            @pl.when(jnp.logical_not(own))
            def _():
                cpy.start()
        return carry

    lax.fori_loop(0, 2 * n_cp, attend, 0)
    w_fwd(1).wait_recv()
    w_fwd(-1).wait_recv()
    w_pass(2).start()
    for dy, dx in offs:
        src = nbr(dx) * n_cp + (cp + dy) % n_cp
        cols = pl.ds(pl.multiple_of(src * hd, hd), hd)
        remote(osnd.at[0], oland.at[:, cols], os_.at[0], orr.at[src], partner).wait_recv()
    for s in range(n_x):
        w_pass(s).wait_recv()

    wide = 512
    def out(n, carry):
        cols = pl.ds(pl.multiple_of(n * wide, wide), wide)
        tot = jnp.dot(oland[...], wfull[:, :, cols].reshape(hidden_o, wide), preferred_element_type=f32)
        h_ref[:, cols] = (x_in[:, cols].astype(f32) + tot).astype(bf)
        return carry

    hidden_o = n_x * 2 * wo.shape[0]
    lax.fori_loop(0, hidden // wide, out, 0)

    for d, p in ((1, 0), (-1, 1), (1, 1), (-1, 0)):
        x_own(d, p).wait_send()
        w_own(d, p).wait_send()
    for d in (1, -1):
        x_fwd(d).wait_send()
        w_fwd(d).wait_send()
    for s in range(n_x):
        w_pass(s).wait_send()
        for dy in range(n_cp):
            kv_send(s, dy).wait_send()
            if dy:
                q_send(s, dy).wait_send()

    def drain(b, carry):
        for u in range(units):
            cpy, own, cols = o_copy(b, u)

            @pl.when(jnp.logical_not(own))
            def _():
                cpy.wait_send()
        return carry

    lax.fori_loop(0, 2 * n_cp, drain, 0)


RELAY_AT = 6


def attention_residual(mesh, hidden_in, w_query, w_key, w_value, w_out):
    n_cp, n_x = mesh.shape['cp'], mesh.shape['tp'] // 2
    rows, hidden = hidden_in.shape
    heads, hd = w_query.shape[1:]
    wqkv = jnp.stack([w_query, w_key, w_value], axis=2).reshape(hidden, heads * 3 * hd)
    wo = w_out.reshape(heads * hd, hidden)
    units = n_x // 2
    n_units = n_cp * n_x
    blk = units * rows
    bf = jnp.bfloat16
    dma = pltpu.SemaphoreType.DMA
    vm = pl.BlockSpec(memory_space=pltpu.VMEM)
    hb = pl.BlockSpec(memory_space=pl.ANY)
    return pl.pallas_call(
        functools.partial(attn_kernel, (n_cp, n_x, hd)),
        out_shape=jax.ShapeDtypeStruct((rows, hidden), bf),
        in_specs=[vm, hb, hb],
        out_specs=vm,
        scratch_shapes=[
            pltpu.VMEM((n_x - 1, rows, hidden), bf),
            pltpu.VMEM((2, hidden, heads * 3 * hd), bf),
            pltpu.VMEM((n_x, n_cp - 1, rows, 3 * hd), bf),
            pltpu.VMEM((n_units, rows, 3 * hd), bf),
            pltpu.VMEM((n_units, rows, 2 * hd), bf),
            pltpu.VMEM((blk, 2 * blk), jnp.float32),
            pltpu.VMEM((n_units, rows, hd), bf),
            pltpu.VMEM((rows, n_units * hd), bf),
            pltpu.VMEM((2 * n_x, heads * hd, hidden), bf),
            dma((2,)), dma((n_x - 1, 2)), dma((n_x - 1, 2)), dma((n_x - 1, 2)), dma((n_x - 1, 2)),
            dma((n_x, n_cp - 1)), dma((n_x, n_cp - 1)), dma((n_x, n_cp)), dma((n_x, n_cp)),
            dma((n_units,)), dma((n_units,)), dma((1,)), dma((1,)), dma((n_x,)), dma((n_x,)),
        ],
        compiler_params=pltpu.CompilerParams(collective_id=2, has_side_effects=True, vmem_limit_bytes=60 * 1024 * 1024),
        name='attn',
    )(hidden_in, wqkv, wo)


def moe_kernel(dims, h_in, idx_ref, gate_ref, wg_hbm, wu_hbm, wd_hbm, y_ref,
               wg, wu, wd, send, recv, ret, slots, gates, dmat, gmat, acc, hid,
               wsem, ssem, rsem, bsem, csem):
    n_cp, n_x, top_k, experts, cap, local_exp = dims
    per_grp = 2 * n_x
    rows = h_in.shape[0]
    hidden = h_in.shape[1]
    cp, tp = lax.axis_index('cp'), lax.axis_index('tp')
    x_pos, core = tp // 2, tp % 2

    chips = [(dy, dx) for dy in range(n_cp) for dx in range(n_x)]
    near = [(0, 1), (1, 0), (0, n_x - 1), (n_cp - 1, 0)]
    odd = [o for o in chips if o[0] % 2 and o[1] % 2]
    even = [o for o in chips if not (o[0] % 2 or o[1] % 2)][::-1]
    rest = [o for o in chips if o not in near + odd + even]
    plan = [[(dy, dx, dc) for dc in range(2) for dy, dx in g] for g in (near, odd, even, rest)]
    n_grp = len(plan)

    def fwd(j, r):
        dy, dx, dc = plan[j][r]
        return (cp + dy) % n_cp, ((x_pos + dx) % n_x) * 2 + (core + dc) % 2

    def back(j, r):
        dy, dx, dc = plan[j][r]
        return (cp + n_cp - dy) % n_cp, ((x_pos + n_x - dx) % n_x) * 2 + (core + dc) % 2

    def local(j, r):
        return plan[j][r] == (0, 0, 0)

    barrier = pltpu.get_barrier_semaphore()
    for j in range(n_grp):
        for r in range(per_grp):
            if not local(j, r):
                c, t = fwd(j, r)
                pl.semaphore_signal(barrier, inc=1, device_id={'cp': c, 'tp': t}, device_id_type=MESH)
    loads = [pltpu.make_async_copy(wg_hbm, wg, wsem.at[0]), pltpu.make_async_copy(wu_hbm, wu, wsem.at[1]), pltpu.make_async_copy(wd_hbm, wd, wsem.at[2])]
    for ld in loads:
        ld.start()

    e_iota = lax.broadcasted_iota(jnp.int32, (experts, rows), 0)
    hit = jnp.zeros((experts, rows), jnp.float32)
    gsel = jnp.zeros((experts, rows), jnp.float32)
    for k in range(top_k):
        m = idx_ref[k:k + 1, :] == e_iota
        hit = hit + jnp.where(m, 1.0, 0.0)
        gsel = gsel + jnp.where(m, gate_ref[k:k + 1, :], 0.0)
    before = jnp.where(lax.broadcasted_iota(jnp.int32, (rows, rows), 0) < lax.broadcasted_iota(jnp.int32, (rows, rows), 1), 1.0, 0.0)
    count = jnp.dot(hit.astype(jnp.bfloat16), before.astype(jnp.bfloat16), preferred_element_type=jnp.float32)
    slots[...] = jnp.where(hit > 0.5, count, -1.0)
    gates[...] = gsel
    c_iota = lax.broadcasted_iota(jnp.int32, (cap, rows), 0).astype(jnp.float32)

    def build(j, ref, gated):
        for e in range(local_exp):
            for r in range(per_grp):
                c, t = fwd(j, r)
                expert = (c * (2 * n_x) + t) * local_exp + e
                eq = jnp.broadcast_to(slots[pl.ds(expert, 1), :], (cap, rows)) == c_iota
                val = jnp.broadcast_to(gates[pl.ds(expert, 1), :], (cap, rows)) if gated else 1.0
                ref[pl.ds((e * per_grp + r) * cap, cap), :] = jnp.where(eq, val, 0.0)

    def dispatch(j, r, e):
        c, t = fwd(j, r)
        if local(j, r):
            return (pltpu.make_async_copy(send.at[j, e * per_grp + r], recv.at[j, e * per_grp + r], rsem.at[j, e * per_grp + r]))
        return (pltpu.make_async_remote_copy(send.at[j, e * per_grp + r], recv.at[j, e * per_grp + r], ssem.at[j, e * per_grp + r], rsem.at[j, e * per_grp + r], device_id={'cp': c, 'tp': t}, device_id_type=MESH))

    def giveback(j, r, e):
        c, t = back(j, r)
        if local(j, r):
            return (pltpu.make_async_copy(recv.at[j, e * per_grp + r], ret.at[j, e * per_grp + r], csem.at[j, e * per_grp + r]))
        return (pltpu.make_async_remote_copy(recv.at[j, e * per_grp + r], ret.at[j, e * per_grp + r], bsem.at[j, e * per_grp + r], csem.at[j, e * per_grp + r], device_id={'cp': c, 'tp': t}, device_id_type=MESH))

    grp_rows = local_exp * per_grp * cap
    half = per_grp * cap
    wide = 512
    order = range(per_grp)
    for j in range(n_grp):
        build(j, dmat, False)

        def fill(n, carry, j=j):
            cols = pl.ds(pl.multiple_of(n * wide, wide), wide)
            picked = jnp.dot(dmat[...].astype(jnp.bfloat16), h_in[:, cols], preferred_element_type=jnp.float32).astype(jnp.bfloat16)
            send[j, :, :, cols] = picked.reshape(local_exp * per_grp, cap, wide)
            return carry

        lax.fori_loop(0, hidden // wide, fill, 0)
        if j == 0:
            pl.semaphore_wait(barrier, n_cp * per_grp - 1)
        for e in range(local_exp):
            for r in order:
                dispatch(j, r, e).start()

    def init(n, carry):
        cols = pl.ds(pl.multiple_of(n * wide, wide), wide)
        acc[:, cols] = h_in[:, cols].astype(jnp.float32)
        return carry

    lax.fori_loop(0, hidden // wide, init, 0)
    for ld in loads:
        ld.wait()
    ffn = wg.shape[2]
    for j in range(n_grp):
        for e in range(local_exp):
            for r in order:
                if local(j, r):
                    dispatch(j, r, e).wait()
                else:
                    dispatch(j, r, e).wait_recv()

            def up(n, carry, j=j, e=e):
                cols = pl.ds(pl.multiple_of(n * 256, 256), 256)
                rows_in = recv[j, pl.ds(e * per_grp, per_grp)].reshape(half, hidden)
                g = jnp.dot(rows_in, wg[e, :, cols], preferred_element_type=jnp.float32)
                u = jnp.dot(rows_in, wu[e, :, cols], preferred_element_type=jnp.float32)
                hid[:, cols] = (g * (1.0 / (1.0 + jnp.exp(-g))) * u).astype(jnp.bfloat16)
                return carry

            def down(n, carry, j=j, e=e):
                cols = pl.ds(pl.multiple_of(n * wide, wide), wide)
                z = jnp.dot(hid[...], wd[e, :, cols], preferred_element_type=jnp.float32).astype(jnp.bfloat16)
                recv[j, pl.ds(e * per_grp, per_grp), :, cols] = z.reshape(per_grp, cap, wide)
                return carry

            lax.fori_loop(0, ffn // 256, up, 0)
            lax.fori_loop(0, hidden // wide, down, 0)
            for r in order:
                giveback(j, r, e).start()

    for j in range(n_grp):
        build(j, gmat, True)
        for e in range(local_exp):
            for r in order:
                if local(j, r):
                    giveback(j, r, e).wait()
                else:
                    giveback(j, r, e).wait_recv()

        def comb(n, carry, j=j):
            cols = pl.ds(pl.multiple_of(n * wide, wide), wide)
            g0 = gmat[...]
            hi = g0.astype(jnp.bfloat16)
            g1 = g0 - hi.astype(jnp.float32)
            mid = g1.astype(jnp.bfloat16)
            lo = (g1 - mid.astype(jnp.float32)).astype(jnp.bfloat16)
            z = ret[j, :, :, cols].reshape(grp_rows, wide)
            dims_t = (((0,), (0,)), ((), ()))
            tot = lax.dot_general(lo, z, dims_t, preferred_element_type=jnp.float32)
            tot = tot + lax.dot_general(mid, z, dims_t, preferred_element_type=jnp.float32)
            tot = tot + lax.dot_general(hi, z, dims_t, preferred_element_type=jnp.float32)
            acc[:, cols] += tot
            return carry

        lax.fori_loop(0, hidden // wide, comb, 0)

    def fin(n, carry):
        cols = pl.ds(pl.multiple_of(n * wide, wide), wide)
        y_ref[:, cols] = acc[:, cols].astype(jnp.bfloat16)
        return carry

    lax.fori_loop(0, hidden // wide, fin, 0)
    for j in range(n_grp):
        for r in range(per_grp):
            if not local(j, r):
                for e in range(local_exp):
                    dispatch(j, r, e).wait_send()
                    giveback(j, r, e).wait_send()


def expert_layer(mesh, resid_h, expert_idx, gate_vals, w_gate, w_up, w_down):
    n_cp, n_x = mesh.shape['cp'], mesh.shape['tp'] // 2
    rows, hidden = resid_h.shape
    top_k = expert_idx.shape[1]
    local_exp, _, ffn = w_gate.shape
    experts = local_exp * n_cp * n_x * 2
    cap = rows * top_k // experts
    slots = local_exp * 2 * n_x
    dims = (n_cp, n_x, top_k, experts, cap, local_exp)
    vm = pl.BlockSpec(memory_space=pltpu.VMEM)
    hb = pl.BlockSpec(memory_space=pl.ANY)
    sems = [pltpu.SemaphoreType.DMA((n_cp, slots)) for _ in range(4)]
    return pl.pallas_call(
        functools.partial(moe_kernel, dims),
        out_shape=jax.ShapeDtypeStruct((rows, hidden), jnp.bfloat16),
        in_specs=[vm, vm, vm, hb, hb, hb],
        out_specs=vm,
        scratch_shapes=[
            pltpu.VMEM((local_exp, hidden, ffn), jnp.bfloat16),
            pltpu.VMEM((local_exp, hidden, ffn), jnp.bfloat16),
            pltpu.VMEM((local_exp, ffn, hidden), jnp.bfloat16),
            pltpu.VMEM((n_cp, slots, cap, hidden), jnp.bfloat16),
            pltpu.VMEM((n_cp, slots, cap, hidden), jnp.bfloat16),
            pltpu.VMEM((n_cp, slots, cap, hidden), jnp.bfloat16),
            pltpu.VMEM((experts, rows), jnp.float32),
            pltpu.VMEM((experts, rows), jnp.float32),
            pltpu.VMEM((slots * cap, rows), jnp.float32),
            pltpu.VMEM((slots * cap, rows), jnp.float32),
            pltpu.VMEM((rows, hidden), jnp.float32),
            pltpu.VMEM((2 * n_x * cap, ffn), jnp.bfloat16),
            pltpu.SemaphoreType.DMA((3,)),
        ] + sems,
        compiler_params=pltpu.CompilerParams(collective_id=1, has_side_effects=True, vmem_limit_bytes=64 * 1024 * 1024 - 65536),
        name='moe',
    )(resid_h, expert_idx.T, gate_vals.T, w_gate, w_up, w_down)


def solution(mesh):
    row_spec = P(('dp', 'cp', 'tp'), None)
    head_spec = P(None, 'tp', None)
    expert_spec = P(('cp', 'tp'), None, None)

    def device_step(hidden_in, w_query, w_key, w_value, w_out, expert_idx, gate_vals, w_gate, w_up, w_down):
        resid_h = attention_residual(mesh, hidden_in, w_query, w_key, w_value, w_out)
        return expert_layer(mesh, resid_h, expert_idx, gate_vals, w_gate, w_up, w_down)

    return jax.shard_map(device_step, mesh=mesh, in_specs=(row_spec, head_spec, head_spec, head_spec, P('tp', None, None), row_spec, row_spec, expert_spec, expert_spec, expert_spec), out_specs=row_spec, check_vma=False)
```

```python
import functools
import jax
import jax.numpy as jnp
from jax import lax
from jax.experimental import pallas as pl
from jax.experimental.pallas import tpu as pltpu
from jax.sharding import PartitionSpec as P

MESH = pl.DeviceIdType.MESH


def attn_kernel(dims, x_in, wq, wk, wv, wo, h_ref,
                stage, pair, xbuf, wall, snd, land, kvp, vt, mask, osnd, oland, wfull,
                lsem, xs, xr, ws, wr, qs, qr, ks, kr, os_, orr, gs, gr, ps, pr, ys, yr):
    n_cp, n_x, hd = dims
    rows, hidden = x_in.shape
    half = rows // 2
    units = n_x // 2
    n_units = n_cp * n_x
    blk = units * rows
    bf, f32 = jnp.bfloat16, jnp.float32
    cp, tp = lax.axis_index('cp'), lax.axis_index('tp')
    x_pos, core = tp // 2, tp % 2
    head = x_pos * n_cp + cp
    nbr = lambda d: (x_pos + d + n_x) % n_x
    at_x = lambda xx: {'cp': cp, 'tp': xx * 2 + core}
    at_y = lambda yy: {'cp': yy, 'tp': tp}
    partner = {'cp': cp, 'tp': x_pos * 2 + 1 - core}

    def remote(src, dst, s_sem, r_sem, dev):
        return pltpu.make_async_remote_copy(src, dst, s_sem, r_sem, device_id=dev, device_id_type=MESH)

    def place(c, xx):
        hi = xx // units
        return (c * (1 - hi) + (2 * n_cp - 1 - c) * hi) * units + xx % units

    barrier = pltpu.get_barrier_semaphore()
    offs = [(dy, dx) for dy in range(n_cp) for dx in range(n_x) if dy or dx]
    for dy, dx in offs:
        pl.semaphore_signal(barrier, inc=1, device_id={'cp': (cp + dy) % n_cp, 'tp': nbr(dx) * 2 + core}, device_id_type=MESH)
    pl.semaphore_signal(barrier, inc=1, device_id=partner, device_id_type=MESH)
    loads = [pltpu.make_async_copy(w, stage.at[m], lsem.at[m + 1]) for m, w in enumerate((wq, wk, wv))]
    load_o = pltpu.make_async_copy(wo, wfull.at[tp], lsem.at[0])
    for ld in loads:
        ld.start()
    load_o.start()
    pl.semaphore_wait(barrier, len(offs) + 1)

    parts = [pl.ds(0, half), pl.ds(half, half)]
    def x_own(d, p):
        slot = 0 if d == 1 else n_x - 2
        return remote(x_in.at[parts[p]], xbuf.at[slot, parts[p]], xs.at[slot, p], xr.at[slot, p], at_x(nbr(d)))

    def x_fwd(d):
        slot, p = (0, 0) if d == 1 else (n_x - 2, 1)
        return remote(xbuf.at[slot, parts[p]], xbuf.at[1, parts[p]], xs.at[1, p], xr.at[1, p], at_x(nbr(d)))

    for d, p in ((1, 0), (-1, 1), (1, 1), (-1, 0)):
        x_own(d, p).start()
    w_part = remote(wall.at[core], wall.at[core], gs.at[0], gr.at[0], partner)
    heads = wall.shape[2] // (3 * hd)
    rows_d = pair.shape[0] // heads
    for ld in loads:
        ld.wait()

    def unpack(n, carry):
        for m in range(3):
            pair[...] = stage[m, pl.ds(pl.multiple_of(n * rows_d * heads, rows_d * heads), rows_d * heads), :].astype(f32)
            for i in range(heads):
                wall[core, pl.ds(pl.multiple_of(n * rows_d, rows_d), rows_d), (i * 3 + m) * hd:(i * 3 + m + 1) * hd] = pair[pl.ds(i, rows_d, stride=heads), :].astype(bf)
        return carry

    lax.fori_loop(0, hidden // rows_d, unpack, 0)
    w_part.start()

    r_io = lax.broadcasted_iota(jnp.int32, (blk, blk), 0)
    c_io = lax.broadcasted_iota(jnp.int32, (blk, blk), 1)
    q_pos = c_io + jnp.where(c_io >= rows, rows, 0) + core * rows
    k_pos = r_io + jnp.where(r_io >= rows, rows, 0)
    mask[0:blk, :] = jnp.where(k_pos + core * rows <= q_pos, 1.0, 0.0)
    mask[blk:, :] = jnp.where(k_pos + (1 - core) * rows <= q_pos, 1.0, 0.0)

    def q_send(s, dy):
        u = place(cp, nbr(-s))
        return remote(snd.at[s, dy - 1], land.at[u], qs.at[s, dy - 1], qr.at[s, dy - 1], at_y((cp + dy) % n_cp))

    def q_recv(s, dy):
        u = place((cp - dy + n_cp) % n_cp, nbr(-s))
        return remote(snd.at[s, dy - 1], land.at[u], qs.at[s, dy - 1], qr.at[s, dy - 1], at_y((cp + dy) % n_cp))

    def kv_send(s, dy):
        u = place((cp - dy + n_cp) % n_cp, nbr(-s))
        return remote(land.at[u, :, pl.ds(hd, 2 * hd)], kvp.at[u], ks.at[s, dy], kr.at[s, dy], partner)

    def project(s):
        for dy in (1, n_cp - 1, 2, 0):
            i = (cp + dy) % n_cp
            cols = pl.ds(pl.multiple_of((i % 2) * 3 * hd, 3 * hd), 3 * hd)
            xv = x_in[...] if s == 0 else xbuf[s - 1]
            res = jnp.dot(xv, wall[i // 2, :, cols], preferred_element_type=f32).astype(bf)
            if dy:
                snd[s, dy - 1] = res
                q_send(s, dy).start()
            else:
                land[place(cp, nbr(-s))] = res
                kv_send(s, 0).start()

    def relay(s):
        for dy in (1, n_cp - 1, 2):
            q_recv(s, dy).wait_recv()
            kv_send(s, dy).start()

    x_own(1, 0).wait_recv()
    x_fwd(1).start()
    x_own(-1, 1).wait_recv()
    x_fwd(-1).start()
    w_part.wait_recv()
    project(0)

    w_mid = wo.shape[0] // 2
    w_qtr = w_mid // n_cp
    w_cut = w_mid * 5 // 8
    tp_at = lambda s: nbr(-s) * 2 + core

    def w_rows(p, y):
        if p == 0:
            return pl.ds(0, w_cut)
        if p == 1:
            return pl.ds(w_cut, w_mid - w_cut)
        return pl.ds(pl.multiple_of(w_mid + y * w_qtr, w_qtr), w_qtr)

    def w_own(d, p):
        slot = 0 if d == 1 else n_x - 2
        blk_ref = wfull.at[tp, w_rows(p, cp)]
        return remote(blk_ref, blk_ref, ws.at[slot, p], wr.at[slot, p], at_x(nbr(d)))

    def w_fwd(d, p):
        blk_ref = wfull.at[nbr(-d) * 2 + core, w_rows(p, cp)]
        return remote(blk_ref, blk_ref, ws.at[1, p], wr.at[1, p], at_x(nbr(d)))

    def w_share(s, dy):
        blk_ref = wfull.at[tp_at(s), w_rows(2, cp)]
        return remote(blk_ref, blk_ref, ys.at[s - 1, dy - 1], yr.at[s - 1, dy - 1], at_y((cp + dy) % n_cp))

    def w_pass(s, p):
        blk_ref = wfull.at[tp_at(s), pl.ds(p * w_mid, w_mid)]
        return remote(blk_ref, blk_ref, ps.at[s, p], pr.at[s, p], partner)

    relays = ((1, 0), (-1, 1), (-1, 2))
    own_sends = ((1, 0), (-1, 1), (-1, 2), (1, 1), (-1, 0), (1, 2))
    y_offs = (1, n_cp - 1, 2)

    def w_step1():
        for d, p in relays:
            w_own(d, p).wait_recv()
            w_fwd(d, p).start()
        w_own(1, 2).wait_recv()
        for dy in y_offs:
            w_share(1, dy).start()
            w_share(n_x - 1, dy).start()
        w_own(1, 1).wait_recv()
        w_own(-1, 0).wait_recv()
        w_pass(1, 0).start()
        w_pass(n_x - 1, 0).start()

    def w_step2():
        for d, p in relays[::-1]:
            w_fwd(d, p).wait_recv()
        for dy in y_offs:
            w_share(2, dy).start()
        w_pass(2, 0).start()

    def w_step3():
        for s in (1, n_x - 1):
            for dy in y_offs:
                w_share(s, dy).wait_recv()
            w_pass(s, 1).start()

    def w_step4():
        for dy in y_offs:
            w_share(2, dy).wait_recv()
        w_pass(2, 1).start()

    load_o.wait()
    for d, p in own_sends:
        w_own(d, p).start()
    for p in range(2):
        w_pass(0, p).start()

    x_own(1, 1).wait_recv()
    project(1)
    x_own(-1, 0).wait_recv()
    project(n_x - 1)
    relay(0)
    x_fwd(1).wait_recv()
    x_fwd(-1).wait_recv()
    project(2)
    for s in (1, n_x - 1, 2):
        relay(s)
    for s in range(n_x):
        for dy in range(n_cp):
            kv_send(s, dy).wait_recv()

    c_exp = hd ** -0.5 * 1.4426950408889634
    nt = (((1,), (1,)), ((), ()))

    def o_copy(b, u):
        hi = b // n_cp
        dst_cp = b * (1 - hi) + (2 * n_cp - 1 - b) * hi
        dst_x = hi * units + u
        cols = pl.ds(pl.multiple_of(head * hd, hd), hd)
        cpy = remote(osnd.at[b * units + u], oland.at[:, cols], os_.at[b * units + u], orr.at[head], {'cp': dst_cp, 'tp': dst_x * 2 + core})
        own = jnp.logical_and(dst_cp == cp, dst_x == x_pos)
        return cpy, own, cols

    def flip(b, carry):
        own_u = pl.ds(b * units, units)
        cols = pl.ds(pl.multiple_of(b * blk, blk), blk)
        vt[0, :, cols] = land[own_u, :, 2 * hd:3 * hd].reshape(blk, hd).T
        vt[1, :, cols] = kvp[own_u, :, hd:2 * hd].reshape(blk, hd).T
        return carry

    lax.fori_loop(0, 2 * n_cp, flip, 0)

    def step(b, t, carry, masked):
        mx, den, acc = carry
        q = land[pl.ds(b * units, units), :, 0:hd].reshape(blk, hd)
        own_u = pl.ds(t * units, units)
        cols = pl.ds(pl.multiple_of(t * blk, blk), blk)
        k1 = land[own_u, :, hd:2 * hd].reshape(blk, hd)
        k2 = kvp[own_u, :, 0:hd].reshape(blk, hd)
        s1 = lax.dot_general(k1, q, nt, preferred_element_type=f32)
        s2 = lax.dot_general(k2, q, nt, preferred_element_type=f32)
        if masked:
            s1 = jnp.where(mask[0:blk, :] > 0.5, s1, -1e30)
            s2 = jnp.where(mask[blk:, :] > 0.5, s2, -1e30)
        top = jnp.maximum(jnp.max(s1, axis=0, keepdims=True), jnp.max(s2, axis=0, keepdims=True))
        new = jnp.maximum(mx, top)
        keep = jnp.exp2((mx - new) * c_exp)
        p1 = jnp.exp2((s1 - new) * c_exp)
        p2 = jnp.exp2((s2 - new) * c_exp)
        den = den * keep + jnp.sum(p1, axis=0, keepdims=True) + jnp.sum(p2, axis=0, keepdims=True)
        acc = acc * keep + jnp.dot(vt[0, :, cols], p1.astype(bf), preferred_element_type=f32) + jnp.dot(vt[1, :, cols], p2.astype(bf), preferred_element_type=f32)
        return new, den, acc

    def attend(b, carry):
        for at, todo in zip(RELAY_AT, (w_step1, w_step2, w_step3)):
            pl.when(b == at)(todo)

        start = (jnp.full((1, blk), -1e30, f32), jnp.zeros((1, blk), f32), jnp.zeros((hd, blk), f32))
        start = step(b, b, start, True)
        mx, den, acc = lax.fori_loop(0, b, lambda t, c: step(b, t, c, False), start)
        o = (acc / den).T.astype(bf)
        for u in range(units):
            cpy, own, cols = o_copy(b, u)
            osnd[b * units + u] = o[u * rows:(u + 1) * rows]

            @pl.when(own)
            def _():
                oland[:, cols] = o[u * rows:(u + 1) * rows]

            @pl.when(jnp.logical_not(own))
            def _():
                cpy.start()
        return carry

    lax.fori_loop(0, 2 * n_cp, attend, 0)
    w_step4()
    for dy, dx in offs:
        src = nbr(dx) * n_cp + (cp + dy) % n_cp
        cols = pl.ds(pl.multiple_of(src * hd, hd), hd)
        remote(osnd.at[0], oland.at[:, cols], os_.at[0], orr.at[src], partner).wait_recv()
    for s in range(n_x):
        for p in range(2):
            w_pass(s, p).wait_recv()

    wide = 512
    def out(n, carry):
        cols = pl.ds(pl.multiple_of(n * wide, wide), wide)
        tot = jnp.dot(oland[...], wfull[:, :, cols].reshape(hidden_o, wide), preferred_element_type=f32)
        h_ref[:, cols] = (x_in[:, cols].astype(f32) + tot).astype(bf)
        return carry

    hidden_o = n_x * 2 * wo.shape[0]
    lax.fori_loop(0, hidden // wide, out, 0)

    for d, p in ((1, 0), (-1, 1), (1, 1), (-1, 0)):
        x_own(d, p).wait_send()
    for d, p in own_sends:
        w_own(d, p).wait_send()
    for d, p in relays:
        w_fwd(d, p).wait_send()
    for d in (1, -1):
        x_fwd(d).wait_send()
    w_part.wait_send()
    for s in range(n_x):
        for p in range(2):
            w_pass(s, p).wait_send()
        for dy in y_offs:
            if s:
                w_share(s, dy).wait_send()
        for dy in range(n_cp):
            kv_send(s, dy).wait_send()
            if dy:
                q_send(s, dy).wait_send()

    def drain(b, carry):
        for u in range(units):
            cpy, own, cols = o_copy(b, u)

            @pl.when(jnp.logical_not(own))
            def _():
                cpy.wait_send()
        return carry

    lax.fori_loop(0, 2 * n_cp, drain, 0)


RELAY_AT = (3, 5, 7)


def attention_residual(mesh, hidden_in, w_query, w_key, w_value, w_out):
    n_cp, n_x = mesh.shape['cp'], mesh.shape['tp'] // 2
    rows, hidden = hidden_in.shape
    heads, hd = w_query.shape[1:]
    wq, wk, wv = (w.reshape(hidden * heads, hd) for w in (w_query, w_key, w_value))
    wo = w_out.reshape(heads * hd, hidden)
    units = n_x // 2
    n_units = n_cp * n_x
    blk = units * rows
    bf = jnp.bfloat16
    dma = pltpu.SemaphoreType.DMA
    vm = pl.BlockSpec(memory_space=pltpu.VMEM)
    hb = pl.BlockSpec(memory_space=pl.ANY)
    return pl.pallas_call(
        functools.partial(attn_kernel, (n_cp, n_x, hd)),
        out_shape=jax.ShapeDtypeStruct((rows, hidden), bf),
        in_specs=[vm, hb, hb, hb, hb],
        out_specs=vm,
        scratch_shapes=[
            pltpu.VMEM((3, heads * hidden, hd), bf),
            pltpu.VMEM((heads * 256, hd), jnp.float32),
            pltpu.VMEM((n_x - 1, rows, hidden), bf),
            pltpu.VMEM((2, hidden, heads * 3 * hd), bf),
            pltpu.VMEM((n_x, n_cp - 1, rows, 3 * hd), bf),
            pltpu.VMEM((n_units, rows, 3 * hd), bf),
            pltpu.VMEM((n_units, rows, 2 * hd), bf),
            pltpu.VMEM((2, hd, n_units * rows), bf),
            pltpu.VMEM((2 * blk, blk), jnp.float32),
            pltpu.VMEM((n_units, rows, hd), bf),
            pltpu.VMEM((rows, n_units * hd), bf),
            pltpu.VMEM((2 * n_x, heads * hd, hidden), bf),
            dma((4,)), dma((n_x - 1, 2)), dma((n_x - 1, 2)), dma((n_x - 1, 3)), dma((n_x - 1, 3)),
            dma((n_x, n_cp - 1)), dma((n_x, n_cp - 1)), dma((n_x, n_cp)), dma((n_x, n_cp)),
            dma((n_units,)), dma((n_units,)), dma((1,)), dma((1,)), dma((n_x, 2)), dma((n_x, 2)),
            dma((n_x - 1, n_cp - 1)), dma((n_x - 1, n_cp - 1)),
        ],
        compiler_params=pltpu.CompilerParams(collective_id=2, has_side_effects=True, vmem_limit_bytes=60 * 1024 * 1024),
        name='attn',
    )(hidden_in, wq, wk, wv, wo)


def moe_kernel(dims, h_in, idx_ref, gate_ref, wg_hbm, wu_hbm, wd_hbm, y_ref,
               wg, wu, wd, send, recv, ret, slots, gates, tabs, held, dmat, gmat, acc, hid,
               wsem, ssem, rsem, bsem, csem, tsem, tgot, hsem, hgot):
    n_cp, n_x, top_k, experts, cap, local_exp = dims
    per_grp = 2 * n_x
    rows = h_in.shape[0]
    hidden = h_in.shape[1]
    cp, tp = lax.axis_index('cp'), lax.axis_index('tp')
    x_pos, core = tp // 2, tp % 2

    chips = [(dy, dx) for dy in range(n_cp) for dx in range(n_x)]
    near = [(0, 1), (1, 0), (0, n_x - 1), (n_cp - 1, 0)]
    odd = [o for o in chips if o[0] % 2 and o[1] % 2]
    even = [o for o in chips if not (o[0] % 2 or o[1] % 2)][::-1]
    rest = [o for o in chips if o not in near + odd + even]
    plan = [[(dy, dx, dc) for dc in range(2) for dy, dx in g] for g in (near, odd, even, rest)]
    n_grp = len(plan)

    def fwd(j, r):
        dy, dx, dc = plan[j][r]
        return (cp + dy) % n_cp, ((x_pos + dx) % n_x) * 2 + (core + dc) % 2

    def back(j, r):
        dy, dx, dc = plan[j][r]
        return (cp + n_cp - dy) % n_cp, ((x_pos + n_x - dx) % n_x) * 2 + (core + dc) % 2

    def local(j, r):
        return plan[j][r] == (0, 0, 0)

    barrier = pltpu.get_barrier_semaphore()
    for j in range(n_grp):
        for r in range(per_grp):
            if not local(j, r):
                c, t = fwd(j, r)
                pl.semaphore_signal(barrier, inc=1, device_id={'cp': c, 'tp': t}, device_id_type=MESH)
    loads = [pltpu.make_async_copy(wg_hbm, wg, wsem.at[0]), pltpu.make_async_copy(wu_hbm, wu, wsem.at[1]), pltpu.make_async_copy(wd_hbm, wd, wsem.at[2])]
    for ld in loads:
        ld.start()

    e_iota = lax.broadcasted_iota(jnp.int32, (experts, rows), 0)
    hit = jnp.zeros((experts, rows), jnp.float32)
    gsel = jnp.zeros((experts, rows), jnp.float32)
    for k in range(top_k):
        m = idx_ref[k:k + 1, :] == e_iota
        hit = hit + jnp.where(m, 1.0, 0.0)
        gsel = gsel + jnp.where(m, gate_ref[k:k + 1, :], 0.0)
    before = jnp.where(lax.broadcasted_iota(jnp.int32, (rows, rows), 0) < lax.broadcasted_iota(jnp.int32, (rows, rows), 1), 1.0, 0.0)
    count = jnp.dot(hit.astype(jnp.bfloat16), before.astype(jnp.bfloat16), preferred_element_type=jnp.float32)
    slots[...] = jnp.where(hit > 0.5, count, -1.0)
    gates[...] = gsel
    c_iota = lax.broadcasted_iota(jnp.int32, (cap, rows), 0).astype(jnp.float32)

    def build(j, ref):
        for e in range(local_exp):
            for r in range(per_grp):
                c, t = fwd(j, r)
                expert = (c * (2 * n_x) + t) * local_exp + e
                eq = jnp.broadcast_to(slots[pl.ds(expert, 1), :], (cap, rows)) == c_iota
                val = jnp.broadcast_to(gates[pl.ds(expert, 1), :], (cap, rows))
                ref[pl.ds((e * per_grp + r) * cap, cap), :] = jnp.where(eq, val, 0.0)

    steps = (0, 1, n_x - 1, 2)
    where_is = {plan[j][r]: (j, r) for j in range(n_grp) for r in range(per_grp)}
    mid = hidden // 2
    cols_of = (pl.ds(0, mid), pl.ds(mid, mid))

    def peer(axis, d, dc):
        if axis == 0:
            return cp, ((x_pos + d) % n_x) * 2 + (core + dc) % 2
        return (cp + d) % n_cp, x_pos * 2 + (core + dc) % 2

    def table(axis, d):
        c, t = peer(axis, d, 0)
        return pltpu.make_async_remote_copy(slots, tabs.at[axis, d - 1], tsem.at[axis, d - 1], tgot.at[axis, d - 1], device_id={'cp': c, 'tp': t}, device_id_type=MESH)

    def spread(axis, d):
        c, t = peer(axis, d, 0)
        return pltpu.make_async_remote_copy(h_in.at[:, cols_of[axis]], held.at[axis, d - 1], hsem.at[axis, d - 1], hgot.at[axis, d - 1], device_id={'cp': c, 'tp': t}, device_id_type=MESH)

    def piece(axis, s, d, dc, e):
        c, t = peer(1 - axis, d, dc)
        k = e * per_grp + d * 2 + dc
        j, r = where_is[(d, s, dc) if axis == 0 else (s, d, dc)]
        src, dst = send.at[axis, s, k], recv.at[j, e * per_grp + r, :, cols_of[axis]]
        got = rsem.at[axis, j, e * per_grp + r]
        if d == 0 and dc == 0:
            return pltpu.make_async_copy(src, dst, got)
        return pltpu.make_async_remote_copy(src, dst, ssem.at[axis, s, k], got, device_id={'cp': c, 'tp': t}, device_id_type=MESH)

    def pieces():
        return [(axis, d, dc, e) for e in range(local_exp) for dc in range(2) for d in steps for axis in range(2)]

    def select(axis, s):
        tab = slots if s == 0 else tabs.at[axis, s - 1]
        for d in range(n_x):
            for dc in range(2):
                c, t = peer(1 - axis, d, dc)
                for e in range(local_exp):
                    expert = (c * (2 * n_x) + t) * local_exp + e
                    eq = jnp.broadcast_to(tab[pl.ds(expert, 1), :], (cap, rows)) == c_iota
                    dmat[pl.ds((e * per_grp + d * 2 + dc) * cap, cap), :] = jnp.where(eq, 1.0, 0.0)

        def fill(n, carry):
            cols = pl.ds(pl.multiple_of(n * wide, wide), wide)
            if s == 0:
                from_h = h_in[:, pl.ds(pl.multiple_of(axis * mid + n * wide, wide), wide)]
            else:
                from_h = held[axis, s - 1, :, cols]
            picked = jnp.dot(dmat[...].astype(jnp.bfloat16), from_h, preferred_element_type=jnp.float32).astype(jnp.bfloat16)
            send[axis, s, :, :, cols] = picked.reshape(local_exp * per_grp, cap, wide)
            return carry

        lax.fori_loop(0, mid // wide, fill, 0)

    def giveback(j, r, e):
        c, t = back(j, r)
        if local(j, r):
            return (pltpu.make_async_copy(recv.at[j, e * per_grp + r], ret.at[j, e * per_grp + r], csem.at[j, e * per_grp + r]))
        return (pltpu.make_async_remote_copy(recv.at[j, e * per_grp + r], ret.at[j, e * per_grp + r], bsem.at[j, e * per_grp + r], csem.at[j, e * per_grp + r], device_id={'cp': c, 'tp': t}, device_id_type=MESH))

    grp_rows = local_exp * per_grp * cap
    half = per_grp * cap
    wide = 512
    order = range(per_grp)
    for axis in range(2):
        select(axis, 0)
    pl.semaphore_wait(barrier, n_grp * per_grp - 1)
    for d in steps[1:]:
        for axis in range(2):
            table(axis, d).start()
    for d in steps[1:]:
        for axis in range(2):
            spread(axis, d).start()
    for axis, d, dc, e in pieces():
        piece(axis, 0, d, dc, e).start()
    for s in steps[1:]:
        for axis in range(2):
            table(axis, s).wait_recv()
            spread(axis, s).wait_recv()
            select(axis, s)
        for axis, d, dc, e in pieces():
            piece(axis, s, d, dc, e).start()

    def init(n, carry):
        cols = pl.ds(pl.multiple_of(n * wide, wide), wide)
        acc[:, cols] = h_in[:, cols].astype(jnp.float32)
        return carry

    lax.fori_loop(0, hidden // wide, init, 0)
    for ld in loads:
        ld.wait()
    ffn = wg.shape[2]
    for j in range(n_grp):
        for e in range(local_exp):
            for r in order:
                dy, dx, dc = plan[j][r]
                for axis, (s, d) in enumerate(((dx, dy), (dy, dx))):
                    cpy = piece(axis, s, d, dc, e)
                    if d == 0 and dc == 0:
                        cpy.wait()
                    else:
                        cpy.wait_recv()

            def up(n, carry, j=j, e=e):
                cols = pl.ds(pl.multiple_of(n * 256, 256), 256)
                rows_in = recv[j, pl.ds(e * per_grp, per_grp)].reshape(half, hidden)
                g = jnp.dot(rows_in, wg[e, :, cols], preferred_element_type=jnp.float32)
                u = jnp.dot(rows_in, wu[e, :, cols], preferred_element_type=jnp.float32)
                hid[:, cols] = (g * (1.0 / (1.0 + jnp.exp(-g))) * u).astype(jnp.bfloat16)
                return carry

            def down(n, carry, j=j, e=e):
                cols = pl.ds(pl.multiple_of(n * wide, wide), wide)
                z = jnp.dot(hid[...], wd[e, :, cols], preferred_element_type=jnp.float32).astype(jnp.bfloat16)
                recv[j, pl.ds(e * per_grp, per_grp), :, cols] = z.reshape(per_grp, cap, wide)
                return carry

            lax.fori_loop(0, ffn // 256, up, 0)
            lax.fori_loop(0, hidden // wide, down, 0)
            for r in order:
                giveback(j, r, e).start()

    for j in range(n_grp):
        build(j, gmat)
        for e in range(local_exp):
            for r in order:
                if local(j, r):
                    giveback(j, r, e).wait()
                else:
                    giveback(j, r, e).wait_recv()

        def comb(n, carry, j=j):
            cols = pl.ds(pl.multiple_of(n * wide, wide), wide)
            g0 = gmat[...]
            hi = g0.astype(jnp.bfloat16)
            g1 = g0 - hi.astype(jnp.float32)
            mid = g1.astype(jnp.bfloat16)
            lo = (g1 - mid.astype(jnp.float32)).astype(jnp.bfloat16)
            z = ret[j, :, :, cols].reshape(grp_rows, wide)
            dims_t = (((0,), (0,)), ((), ()))
            tot = lax.dot_general(lo, z, dims_t, preferred_element_type=jnp.float32)
            tot = tot + lax.dot_general(mid, z, dims_t, preferred_element_type=jnp.float32)
            tot = tot + lax.dot_general(hi, z, dims_t, preferred_element_type=jnp.float32)
            acc[:, cols] += tot
            return carry

        lax.fori_loop(0, hidden // wide, comb, 0)

    def fin(n, carry):
        cols = pl.ds(pl.multiple_of(n * wide, wide), wide)
        y_ref[:, cols] = acc[:, cols].astype(jnp.bfloat16)
        return carry

    lax.fori_loop(0, hidden // wide, fin, 0)
    for j in range(n_grp):
        for r in range(per_grp):
            if not local(j, r):
                for e in range(local_exp):
                    giveback(j, r, e).wait_send()
    for axis in range(2):
        for d in steps[1:]:
            table(axis, d).wait_send()
            spread(axis, d).wait_send()
    for s in steps:
        for axis, d, dc, e in pieces():
            if d or dc:
                piece(axis, s, d, dc, e).wait_send()


def expert_layer(mesh, resid_h, expert_idx, gate_vals, w_gate, w_up, w_down):
    n_cp, n_x = mesh.shape['cp'], mesh.shape['tp'] // 2
    rows, hidden = resid_h.shape
    top_k = expert_idx.shape[1]
    local_exp, _, ffn = w_gate.shape
    experts = local_exp * n_cp * n_x * 2
    cap = rows * top_k // experts
    slots = local_exp * 2 * n_x
    dims = (n_cp, n_x, top_k, experts, cap, local_exp)
    vm = pl.BlockSpec(memory_space=pltpu.VMEM)
    hb = pl.BlockSpec(memory_space=pl.ANY)
    dma = pltpu.SemaphoreType.DMA
    sems = [dma((2, n_x, slots)), dma((2, n_cp, slots)), dma((n_cp, slots)), dma((n_cp, slots))] + [dma((2, n_x - 1))] * 4
    return pl.pallas_call(
        functools.partial(moe_kernel, dims),
        out_shape=jax.ShapeDtypeStruct((rows, hidden), jnp.bfloat16),
        in_specs=[vm, vm, vm, hb, hb, hb],
        out_specs=vm,
        scratch_shapes=[
            pltpu.VMEM((local_exp, hidden, ffn), jnp.bfloat16),
            pltpu.VMEM((local_exp, hidden, ffn), jnp.bfloat16),
            pltpu.VMEM((local_exp, ffn, hidden), jnp.bfloat16),
            pltpu.VMEM((2, n_x, slots, cap, hidden // 2), jnp.bfloat16),
            pltpu.VMEM((n_cp, slots, cap, hidden), jnp.bfloat16),
            pltpu.VMEM((n_cp, slots, cap, hidden), jnp.bfloat16),
            pltpu.VMEM((experts, rows), jnp.float32),
            pltpu.VMEM((experts, rows), jnp.float32),
            pltpu.VMEM((2, n_x - 1, experts, rows), jnp.float32),
            pltpu.VMEM((2, n_x - 1, rows, hidden // 2), jnp.bfloat16),
            pltpu.VMEM((slots * cap, rows), jnp.float32),
            pltpu.VMEM((slots * cap, rows), jnp.float32),
            pltpu.VMEM((rows, hidden), jnp.float32),
            pltpu.VMEM((2 * n_x * cap, ffn), jnp.bfloat16),
            pltpu.SemaphoreType.DMA((3,)),
        ] + sems,
        compiler_params=pltpu.CompilerParams(collective_id=1, has_side_effects=True, vmem_limit_bytes=64 * 1024 * 1024 - 65536),
        name='moe',
    )(resid_h, expert_idx.T, gate_vals.T, w_gate, w_up, w_down)


def solution(mesh):
    row_spec = P(('dp', 'cp', 'tp'), None)
    head_spec = P(None, 'tp', None)
    expert_spec = P(('cp', 'tp'), None, None)

    def device_step(hidden_in, w_query, w_key, w_value, w_out, expert_idx, gate_vals, w_gate, w_up, w_down):
        resid_h = attention_residual(mesh, hidden_in, w_query, w_key, w_value, w_out)
        return expert_layer(mesh, resid_h, expert_idx, gate_vals, w_gate, w_up, w_down)

    return jax.shard_map(device_step, mesh=mesh, in_specs=(row_spec, head_spec, head_spec, head_spec, P('tp', None, None), row_spec, row_spec, expert_spec, expert_spec, expert_spec), out_specs=row_spec, check_vma=False)
```

```python
import functools
import jax
import jax.numpy as jnp
from jax import lax
from jax.experimental import pallas as pl
from jax.experimental.pallas import tpu as pltpu
from jax.sharding import PartitionSpec as P

MESH = pl.DeviceIdType.MESH


def attn_kernel(dims, x_in, wq, wk, wv, wo, h_ref,
                stage, pair, xbuf, wall, snd, land, kvp, vt, mask, osnd, oland, wfull,
                lsem, xs, xr, ws, wr, qs, qr, ks, kr, os_, orr, gs, gr, ps, pr, ys, yr):
    n_cp, n_x, hd = dims
    rows, hidden = x_in.shape
    half = rows // 2
    units = n_x // 2
    n_units = n_cp * n_x
    blk = units * rows
    bf, f32 = jnp.bfloat16, jnp.float32
    cp, tp = lax.axis_index('cp'), lax.axis_index('tp')
    x_pos, core = tp // 2, tp % 2
    head = x_pos * n_cp + cp
    nbr = lambda d: (x_pos + d + n_x) % n_x
    at_x = lambda xx: {'cp': cp, 'tp': xx * 2 + core}
    at_y = lambda yy: {'cp': yy, 'tp': tp}
    partner = {'cp': cp, 'tp': x_pos * 2 + 1 - core}

    def remote(src, dst, s_sem, r_sem, dev):
        return pltpu.make_async_remote_copy(src, dst, s_sem, r_sem, device_id=dev, device_id_type=MESH)

    def place(c, xx):
        hi = xx // units
        return (c * (1 - hi) + (2 * n_cp - 1 - c) * hi) * units + xx % units

    barrier = pltpu.get_barrier_semaphore()
    offs = [(dy, dx) for dy in range(n_cp) for dx in range(n_x) if dy or dx]
    for dy, dx in offs:
        pl.semaphore_signal(barrier, inc=1, device_id={'cp': (cp + dy) % n_cp, 'tp': nbr(dx) * 2 + core}, device_id_type=MESH)
    pl.semaphore_signal(barrier, inc=1, device_id=partner, device_id_type=MESH)
    loads = [pltpu.make_async_copy(w, stage.at[m], lsem.at[m + 1]) for m, w in enumerate((wq, wk, wv))]
    load_o = pltpu.make_async_copy(wo, wfull.at[tp], lsem.at[0])
    for ld in loads:
        ld.start()
    load_o.start()
    pl.semaphore_wait(barrier, len(offs) + 1)

    parts = [pl.ds(0, half), pl.ds(half, half)]
    def x_own(d, p):
        slot = 0 if d == 1 else n_x - 2
        return remote(x_in.at[parts[p]], xbuf.at[slot, parts[p]], xs.at[slot, p], xr.at[slot, p], at_x(nbr(d)))

    def x_fwd(d):
        slot, p = (0, 0) if d == 1 else (n_x - 2, 1)
        return remote(xbuf.at[slot, parts[p]], xbuf.at[1, parts[p]], xs.at[1, p], xr.at[1, p], at_x(nbr(d)))

    for d, p in ((1, 0), (-1, 1), (1, 1), (-1, 0)):
        x_own(d, p).start()
    w_part = remote(wall.at[core], wall.at[core], gs.at[0], gr.at[0], partner)
    heads = wall.shape[2] // (3 * hd)
    rows_d = pair.shape[0] // heads
    for ld in loads:
        ld.wait()

    def unpack(n, carry):
        for m in range(3):
            pair[...] = stage[m, pl.ds(pl.multiple_of(n * rows_d * heads, rows_d * heads), rows_d * heads), :].astype(f32)
            for i in range(heads):
                wall[core, pl.ds(pl.multiple_of(n * rows_d, rows_d), rows_d), (i * 3 + m) * hd:(i * 3 + m + 1) * hd] = pair[pl.ds(i, rows_d, stride=heads), :].astype(bf)
        return carry

    lax.fori_loop(0, hidden // rows_d, unpack, 0)
    w_part.start()

    r_io = lax.broadcasted_iota(jnp.int32, (blk, blk), 0)
    c_io = lax.broadcasted_iota(jnp.int32, (blk, blk), 1)
    q_pos = c_io + jnp.where(c_io >= rows, rows, 0) + core * rows
    k_pos = r_io + jnp.where(r_io >= rows, rows, 0)
    mask[0:blk, :] = jnp.where(k_pos + core * rows <= q_pos, 1.0, 0.0)
    mask[blk:, :] = jnp.where(k_pos + (1 - core) * rows <= q_pos, 1.0, 0.0)

    def span(p):
        return pl.ds(0, rows) if p is None else parts[p]

    def q_copy(s, p, dy, u):
        at = span(p)
        k = p or 0
        return remote(snd.at[s, dy - 1, at], land.at[u, at], qs.at[s, k, dy - 1], qr.at[s, k, dy - 1], at_y((cp + dy) % n_cp))

    def q_send(s, p, dy):
        return q_copy(s, p, dy, place(cp, nbr(-s)))

    def q_recv(s, p, dy):
        return q_copy(s, p, dy, place((cp - dy + n_cp) % n_cp, nbr(-s)))

    def kv_send(s, dy):
        u = place((cp - dy + n_cp) % n_cp, nbr(-s))
        return remote(land.at[u, :, pl.ds(hd, 2 * hd)], kvp.at[u], ks.at[s, dy], kr.at[s, dy], partner)

    def project(s, p=None):
        at = span(p)
        for dy in (1, n_cp - 1, 2, 0):
            i = (cp + dy) % n_cp
            cols = pl.ds(pl.multiple_of((i % 2) * 3 * hd, 3 * hd), 3 * hd)
            xv = x_in[at] if s == 0 else xbuf[s - 1, at]
            res = jnp.dot(xv, wall[i // 2, :, cols], preferred_element_type=f32).astype(bf)
            if dy:
                snd[s, dy - 1, at] = res
                q_send(s, p, dy).start()
            else:
                land[place(cp, nbr(-s)), at] = res
                if p is None or (s, p) in ((1, 1), (n_x - 1, 0)):
                    kv_send(s, 0).start()

    def halves(s):
        return (0, 1) if s in (1, n_x - 1) else (None,)

    def relay(s):
        for dy in (1, n_cp - 1, 2):
            for p in halves(s):
                q_recv(s, p, dy).wait_recv()
            kv_send(s, dy).start()

    x_own(1, 0).wait_recv()
    x_fwd(1).start()
    x_own(-1, 1).wait_recv()
    x_fwd(-1).start()
    w_part.wait_recv()
    project(0)

    w_mid = wo.shape[0] * 3 // 4
    w_qtr = (wo.shape[0] - w_mid) // n_cp
    w_cut = w_mid // 2
    tp_at = lambda s: nbr(-s) * 2 + core

    def w_rows(p, y):
        if p == 0:
            return pl.ds(0, w_cut)
        if p == 1:
            return pl.ds(w_cut, w_mid - w_cut)
        return pl.ds(pl.multiple_of(w_mid + y * w_qtr, w_qtr), w_qtr)

    def w_own(d, p):
        slot = 0 if d == 1 else n_x - 2
        blk_ref = wfull.at[tp, w_rows(p, cp)]
        return remote(blk_ref, blk_ref, ws.at[slot, p], wr.at[slot, p], at_x(nbr(d)))

    def w_fwd(d, p):
        blk_ref = wfull.at[nbr(-d) * 2 + core, w_rows(p, cp)]
        return remote(blk_ref, blk_ref, ws.at[1, p], wr.at[1, p], at_x(nbr(d)))

    def w_share(s, dy):
        blk_ref = wfull.at[tp_at(s), w_rows(2, cp)]
        return remote(blk_ref, blk_ref, ys.at[s - 1, dy - 1], yr.at[s - 1, dy - 1], at_y((cp + dy) % n_cp))

    def w_pass(s, p):
        blk_ref = wfull.at[tp_at(s), pl.ds(p * w_mid, w_mid if p == 0 else wo.shape[0] - w_mid)]
        return remote(blk_ref, blk_ref, ps.at[s, p], pr.at[s, p], partner)

    relays = ((1, 0), (-1, 1), (-1, 2))
    own_sends = ((1, 0), (-1, 2), (-1, 1), (1, 2), (-1, 0), (1, 1))
    y_offs = (1, n_cp - 1, 2)

    def w_step0():
        for d, p in relays:
            w_own(d, p).wait_recv()
            w_fwd(d, p).start()
        for dy in y_offs:
            w_share(n_x - 1, dy).start()

    def w_step1():
        w_own(1, 2).wait_recv()
        for dy in y_offs:
            w_share(1, dy).start()
        w_own(1, 1).wait_recv()
        w_own(-1, 0).wait_recv()
        w_pass(1, 0).start()
        w_pass(n_x - 1, 0).start()

    def w_step2():
        for d, p in relays[::-1]:
            w_fwd(d, p).wait_recv()
        for dy in y_offs:
            w_share(2, dy).start()
        w_pass(2, 0).start()

    def w_step3():
        for s in (1, n_x - 1):
            for dy in y_offs:
                w_share(s, dy).wait_recv()
            w_pass(s, 1).start()

    def w_step4():
        for dy in y_offs:
            w_share(2, dy).wait_recv()
        w_pass(2, 1).start()

    load_o.wait()
    for d, p in own_sends:
        w_own(d, p).start()
    for p in range(2):
        w_pass(0, p).start()

    project(1, 0)
    project(n_x - 1, 1)
    x_own(1, 1).wait_recv()
    project(1, 1)
    x_own(-1, 0).wait_recv()
    project(n_x - 1, 0)
    relay(0)
    x_fwd(1).wait_recv()
    x_fwd(-1).wait_recv()
    project(2)
    for s in (1, n_x - 1, 2):
        relay(s)
    for s in range(n_x):
        for dy in range(n_cp):
            kv_send(s, dy).wait_recv()
    w_step0()

    c_exp = hd ** -0.5 * 1.4426950408889634
    nt = (((1,), (1,)), ((), ()))

    def o_copy(b, u):
        hi = b // n_cp
        dst_cp = b * (1 - hi) + (2 * n_cp - 1 - b) * hi
        dst_x = hi * units + u
        cols = pl.ds(pl.multiple_of(head * hd, hd), hd)
        cpy = remote(osnd.at[b * units + u], oland.at[:, cols], os_.at[b * units + u], orr.at[head], {'cp': dst_cp, 'tp': dst_x * 2 + core})
        own = jnp.logical_and(dst_cp == cp, dst_x == x_pos)
        return cpy, own, cols

    def flip(b, carry):
        own_u = pl.ds(b * units, units)
        cols = pl.ds(pl.multiple_of(b * blk, blk), blk)
        vt[0, :, cols] = land[own_u, :, 2 * hd:3 * hd].reshape(blk, hd).T
        vt[1, :, cols] = kvp[own_u, :, hd:2 * hd].reshape(blk, hd).T
        return carry

    lax.fori_loop(0, 2 * n_cp, flip, 0)

    def step(b, t, carry, masked):
        mx, den, acc = carry
        q = land[pl.ds(b * units, units), :, 0:hd].reshape(blk, hd)
        own_u = pl.ds(t * units, units)
        cols = pl.ds(pl.multiple_of(t * blk, blk), blk)
        k1 = land[own_u, :, hd:2 * hd].reshape(blk, hd)
        k2 = kvp[own_u, :, 0:hd].reshape(blk, hd)
        s1 = lax.dot_general(k1, q, nt, preferred_element_type=f32)
        s2 = lax.dot_general(k2, q, nt, preferred_element_type=f32)
        if masked:
            s1 = jnp.where(mask[0:blk, :] > 0.5, s1, -1e30)
            s2 = jnp.where(mask[blk:, :] > 0.5, s2, -1e30)
        m1 = jnp.maximum(mx, jnp.max(s1, axis=0, keepdims=True))
        p1 = jnp.exp2((s1 - m1) * c_exp)
        new = jnp.maximum(m1, jnp.max(s2, axis=0, keepdims=True))
        p2 = jnp.exp2((s2 - new) * c_exp)
        keep = jnp.exp2((mx - new) * c_exp)
        mend = jnp.exp2((m1 - new) * c_exp)
        den = den * keep + jnp.sum(p1, axis=0, keepdims=True) * mend + jnp.sum(p2, axis=0, keepdims=True)
        acc = acc * keep + jnp.dot(vt[0, :, cols], p1.astype(bf), preferred_element_type=f32) * mend + jnp.dot(vt[1, :, cols], p2.astype(bf), preferred_element_type=f32)
        return new, den, acc

    def attend(b, carry):
        for at, todo in zip(RELAY_AT, (w_step1, w_step2, w_step3)):
            pl.when(b == at)(todo)

        start = (jnp.full((1, blk), -1e30, f32), jnp.zeros((1, blk), f32), jnp.zeros((hd, blk), f32))
        start = step(b, b, start, True)
        start = lax.fori_loop(0, b // 2, lambda t, c: step(b, 2 * t + 1, step(b, 2 * t, c, False), False), start)
        mx, den, acc = lax.fori_loop(b // 2 * 2, b, lambda t, c: step(b, t, c, False), start)
        o = (acc / den).T.astype(bf)
        for u in range(units):
            cpy, own, cols = o_copy(b, u)
            osnd[b * units + u] = o[u * rows:(u + 1) * rows]

            @pl.when(own)
            def _():
                oland[:, cols] = o[u * rows:(u + 1) * rows]

            @pl.when(jnp.logical_not(own))
            def _():
                cpy.start()
        return carry

    lax.fori_loop(0, 2 * n_cp, attend, 0)
    w_step4()
    for dy, dx in offs:
        src = nbr(dx) * n_cp + (cp + dy) % n_cp
        cols = pl.ds(pl.multiple_of(src * hd, hd), hd)
        remote(osnd.at[0], oland.at[:, cols], os_.at[0], orr.at[src], partner).wait_recv()
    for s in range(n_x):
        for p in range(2):
            w_pass(s, p).wait_recv()

    wide = 512
    def out(n, carry):
        cols = pl.ds(pl.multiple_of(n * wide, wide), wide)
        tot = jnp.dot(oland[...], wfull[:, :, cols].reshape(hidden_o, wide), preferred_element_type=f32)
        h_ref[:, cols] = (x_in[:, cols].astype(f32) + tot).astype(bf)
        return carry

    hidden_o = n_x * 2 * wo.shape[0]
    lax.fori_loop(0, hidden // wide, out, 0)

    for d, p in ((1, 0), (-1, 1), (1, 1), (-1, 0)):
        x_own(d, p).wait_send()
    for d, p in own_sends:
        w_own(d, p).wait_send()
    for d, p in relays:
        w_fwd(d, p).wait_send()
    for d in (1, -1):
        x_fwd(d).wait_send()
    w_part.wait_send()
    for s in range(n_x):
        for p in range(2):
            w_pass(s, p).wait_send()
        for dy in y_offs:
            if s:
                w_share(s, dy).wait_send()
        for dy in range(n_cp):
            kv_send(s, dy).wait_send()
            if dy:
                for p in halves(s):
                    q_send(s, p, dy).wait_send()

    def drain(b, carry):
        for u in range(units):
            cpy, own, cols = o_copy(b, u)

            @pl.when(jnp.logical_not(own))
            def _():
                cpy.wait_send()
        return carry

    lax.fori_loop(0, 2 * n_cp, drain, 0)


RELAY_AT = (4, 6, 7)


def attention_residual(mesh, hidden_in, w_query, w_key, w_value, w_out):
    n_cp, n_x = mesh.shape['cp'], mesh.shape['tp'] // 2
    rows, hidden = hidden_in.shape
    heads, hd = w_query.shape[1:]
    wq, wk, wv = (w.reshape(hidden * heads, hd) for w in (w_query, w_key, w_value))
    wo = w_out.reshape(heads * hd, hidden)
    units = n_x // 2
    n_units = n_cp * n_x
    blk = units * rows
    bf = jnp.bfloat16
    dma = pltpu.SemaphoreType.DMA
    vm = pl.BlockSpec(memory_space=pltpu.VMEM)
    hb = pl.BlockSpec(memory_space=pl.ANY)
    return pl.pallas_call(
        functools.partial(attn_kernel, (n_cp, n_x, hd)),
        out_shape=jax.ShapeDtypeStruct((rows, hidden), bf),
        in_specs=[vm, hb, hb, hb, hb],
        out_specs=vm,
        scratch_shapes=[
            pltpu.VMEM((3, heads * hidden, hd), bf),
            pltpu.VMEM((heads * 256, hd), jnp.float32),
            pltpu.VMEM((n_x - 1, rows, hidden), bf),
            pltpu.VMEM((2, hidden, heads * 3 * hd), bf),
            pltpu.VMEM((n_x, n_cp - 1, rows, 3 * hd), bf),
            pltpu.VMEM((n_units, rows, 3 * hd), bf),
            pltpu.VMEM((n_units, rows, 2 * hd), bf),
            pltpu.VMEM((2, hd, n_units * rows), bf),
            pltpu.VMEM((2 * blk, blk), jnp.float32),
            pltpu.VMEM((n_units, rows, hd), bf),
            pltpu.VMEM((rows, n_units * hd), bf),
            pltpu.VMEM((2 * n_x, heads * hd, hidden), bf),
            dma((4,)), dma((n_x - 1, 2)), dma((n_x - 1, 2)), dma((n_x - 1, 3)), dma((n_x - 1, 3)),
            dma((n_x, 2, n_cp - 1)), dma((n_x, 2, n_cp - 1)), dma((n_x, n_cp)), dma((n_x, n_cp)),
            dma((n_units,)), dma((n_units,)), dma((1,)), dma((1,)), dma((n_x, 2)), dma((n_x, 2)),
            dma((n_x - 1, n_cp - 1)), dma((n_x - 1, n_cp - 1)),
        ],
        compiler_params=pltpu.CompilerParams(collective_id=2, has_side_effects=True, vmem_limit_bytes=60 * 1024 * 1024),
        name='attn',
    )(hidden_in, wq, wk, wv, wo)


def moe_kernel(dims, h_in, idx_ref, gate_ref, wg_hbm, wu_hbm, wd_hbm, y_ref,
               wg, wu, wd, send, recv, ret, slots, gates, tabs, held, dmat, gmat, acc, hid,
               wsem, ssem, rsem, bsem, csem, tsem, tgot, hsem, hgot):
    n_cp, n_x, top_k, experts, cap, local_exp = dims
    per_grp = 2 * n_x
    rows = h_in.shape[0]
    hidden = h_in.shape[1]
    cp, tp = lax.axis_index('cp'), lax.axis_index('tp')
    x_pos, core = tp // 2, tp % 2

    chips = [(dy, dx) for dy in range(n_cp) for dx in range(n_x)]
    near = [(0, 1), (1, 0), (0, n_x - 1), (n_cp - 1, 0)]
    odd = [o for o in chips if o[0] % 2 and o[1] % 2]
    even = [o for o in chips if not (o[0] % 2 or o[1] % 2)][::-1]
    rest = [o for o in chips if o not in near + odd + even]
    plan = [[(dy, dx, dc) for dc in range(2) for dy, dx in g] for g in (near, odd, even, rest)]
    n_grp = len(plan)

    def fwd(j, r):
        dy, dx, dc = plan[j][r]
        return (cp + dy) % n_cp, ((x_pos + dx) % n_x) * 2 + (core + dc) % 2

    def back(j, r):
        dy, dx, dc = plan[j][r]
        return (cp + n_cp - dy) % n_cp, ((x_pos + n_x - dx) % n_x) * 2 + (core + dc) % 2

    def local(j, r):
        return plan[j][r] == (0, 0, 0)

    barrier = pltpu.get_barrier_semaphore()
    for j in range(n_grp):
        for r in range(per_grp):
            if not local(j, r):
                c, t = fwd(j, r)
                pl.semaphore_signal(barrier, inc=1, device_id={'cp': c, 'tp': t}, device_id_type=MESH)
    loads = [pltpu.make_async_copy(wg_hbm, wg, wsem.at[0]), pltpu.make_async_copy(wu_hbm, wu, wsem.at[1]), pltpu.make_async_copy(wd_hbm, wd, wsem.at[2])]
    for ld in loads:
        ld.start()

    e_iota = lax.broadcasted_iota(jnp.int32, (experts, rows), 0)
    hit = jnp.zeros((experts, rows), jnp.float32)
    gsel = jnp.zeros((experts, rows), jnp.float32)
    for k in range(top_k):
        m = idx_ref[k:k + 1, :] == e_iota
        hit = hit + jnp.where(m, 1.0, 0.0)
        gsel = gsel + jnp.where(m, gate_ref[k:k + 1, :], 0.0)
    before = jnp.where(lax.broadcasted_iota(jnp.int32, (rows, rows), 0) < lax.broadcasted_iota(jnp.int32, (rows, rows), 1), 1.0, 0.0)
    count = jnp.dot(hit.astype(jnp.bfloat16), before.astype(jnp.bfloat16), preferred_element_type=jnp.float32)
    slots[...] = jnp.where(hit > 0.5, count, -1.0)
    gates[...] = gsel
    c_iota = lax.broadcasted_iota(jnp.int32, (cap, rows), 0).astype(jnp.float32)

    def build(j, ref):
        for e in range(local_exp):
            for r in range(per_grp):
                c, t = fwd(j, r)
                expert = (c * (2 * n_x) + t) * local_exp + e
                eq = jnp.broadcast_to(slots[pl.ds(expert, 1), :], (cap, rows)) == c_iota
                val = jnp.broadcast_to(gates[pl.ds(expert, 1), :], (cap, rows))
                ref[pl.ds((e * per_grp + r) * cap, cap), :] = jnp.where(eq, val, 0.0)

    steps = (0, 1, n_x - 1, 2)
    where_is = {plan[j][r]: (j, r) for j in range(n_grp) for r in range(per_grp)}
    mid = hidden // 2
    cols_of = (pl.ds(0, mid), pl.ds(mid, mid))

    def peer(axis, d, dc):
        if axis == 0:
            return cp, ((x_pos + d) % n_x) * 2 + (core + dc) % 2
        return (cp + d) % n_cp, x_pos * 2 + (core + dc) % 2

    def table(axis, d):
        c, t = peer(axis, d, 0)
        return pltpu.make_async_remote_copy(slots, tabs.at[axis, d - 1], tsem.at[axis, d - 1], tgot.at[axis, d - 1], device_id={'cp': c, 'tp': t}, device_id_type=MESH)

    def spread(axis, d):
        c, t = peer(axis, d, 0)
        return pltpu.make_async_remote_copy(h_in.at[:, cols_of[axis]], held.at[axis, d - 1], hsem.at[axis, d - 1], hgot.at[axis, d - 1], device_id={'cp': c, 'tp': t}, device_id_type=MESH)

    def piece(axis, s, d, dc, e):
        c, t = peer(1 - axis, d, dc)
        k = e * per_grp + d * 2 + dc
        j, r = where_is[(d, s, dc) if axis == 0 else (s, d, dc)]
        src, dst = send.at[axis, s, k], recv.at[j, e * per_grp + r, :, cols_of[axis]]
        got = rsem.at[axis, j, e * per_grp + r]
        if d == 0 and dc == 0:
            return pltpu.make_async_copy(src, dst, got)
        return pltpu.make_async_remote_copy(src, dst, ssem.at[axis, s, k], got, device_id={'cp': c, 'tp': t}, device_id_type=MESH)

    def pieces():
        return [(axis, d, dc, e) for e in range(local_exp) for dc in range(2) for d in steps for axis in range(2)]

    def select(axis, s):
        tab = slots if s == 0 else tabs.at[axis, s - 1]
        for d in range(n_x):
            for dc in range(2):
                c, t = peer(1 - axis, d, dc)
                for e in range(local_exp):
                    expert = (c * (2 * n_x) + t) * local_exp + e
                    eq = jnp.broadcast_to(tab[pl.ds(expert, 1), :], (cap, rows)) == c_iota
                    dmat[pl.ds((e * per_grp + d * 2 + dc) * cap, cap), :] = jnp.where(eq, 1.0, 0.0)

        def fill(n, carry):
            cols = pl.ds(pl.multiple_of(n * wide, wide), wide)
            if s == 0:
                from_h = h_in[:, pl.ds(pl.multiple_of(axis * mid + n * wide, wide), wide)]
            else:
                from_h = held[axis, s - 1, :, cols]
            picked = jnp.dot(dmat[...].astype(jnp.bfloat16), from_h, preferred_element_type=jnp.float32).astype(jnp.bfloat16)
            send[axis, s, :, :, cols] = picked.reshape(local_exp * per_grp, cap, wide)
            return carry

        lax.fori_loop(0, mid // wide, fill, 0)

    def giveback(j, r, e):
        c, t = back(j, r)
        if local(j, r):
            return (pltpu.make_async_copy(recv.at[j, e * per_grp + r], ret.at[j, e * per_grp + r], csem.at[j, e * per_grp + r]))
        return (pltpu.make_async_remote_copy(recv.at[j, e * per_grp + r], ret.at[j, e * per_grp + r], bsem.at[j, e * per_grp + r], csem.at[j, e * per_grp + r], device_id={'cp': c, 'tp': t}, device_id_type=MESH))

    grp_rows = local_exp * per_grp * cap
    half = per_grp * cap
    wide = 512
    order = range(per_grp)
    for axis in range(2):
        select(axis, 0)
    pl.semaphore_wait(barrier, n_grp * per_grp - 1)
    for d in steps[1:]:
        for axis in range(2):
            table(axis, d).start()
    for d in steps[1:]:
        for axis in range(2):
            spread(axis, d).start()
    for axis, d, dc, e in pieces():
        piece(axis, 0, d, dc, e).start()
    for s in steps[1:]:
        for axis in range(2):
            table(axis, s).wait_recv()
            spread(axis, s).wait_recv()
            select(axis, s)
        for axis, d, dc, e in pieces():
            piece(axis, s, d, dc, e).start()

    def init(n, carry):
        cols = pl.ds(pl.multiple_of(n * wide, wide), wide)
        acc[:, cols] = h_in[:, cols].astype(jnp.float32)
        return carry

    lax.fori_loop(0, hidden // wide, init, 0)
    for ld in loads:
        ld.wait()
    ffn = wg.shape[2]
    for j in range(n_grp):
        for e in range(local_exp):
            for r in order:
                dy, dx, dc = plan[j][r]
                for axis, (s, d) in enumerate(((dx, dy), (dy, dx))):
                    cpy = piece(axis, s, d, dc, e)
                    if d == 0 and dc == 0:
                        cpy.wait()
                    else:
                        cpy.wait_recv()

            def up(n, carry, j=j, e=e):
                cols = pl.ds(pl.multiple_of(n * 256, 256), 256)
                rows_in = recv[j, pl.ds(e * per_grp, per_grp)].reshape(half, hidden)
                g = jnp.dot(rows_in, wg[e, :, cols], preferred_element_type=jnp.float32)
                u = jnp.dot(rows_in, wu[e, :, cols], preferred_element_type=jnp.float32)
                hid[:, cols] = (g * (1.0 / (1.0 + jnp.exp(-g))) * u).astype(jnp.bfloat16)
                return carry

            def down(n, carry, j=j, e=e):
                cols = pl.ds(pl.multiple_of(n * wide, wide), wide)
                z = jnp.dot(hid[...], wd[e, :, cols], preferred_element_type=jnp.float32).astype(jnp.bfloat16)
                recv[j, pl.ds(e * per_grp, per_grp), :, cols] = z.reshape(per_grp, cap, wide)
                return carry

            lax.fori_loop(0, ffn // 256, up, 0)
            lax.fori_loop(0, hidden // wide, down, 0)
            for r in order:
                giveback(j, r, e).start()

    for j in range(n_grp):
        build(j, gmat)
        for e in range(local_exp):
            for r in order:
                if local(j, r):
                    giveback(j, r, e).wait()
                else:
                    giveback(j, r, e).wait_recv()

        def comb(n, carry, j=j):
            cols = pl.ds(pl.multiple_of(n * wide, wide), wide)
            g0 = gmat[...]
            hi = g0.astype(jnp.bfloat16)
            g1 = g0 - hi.astype(jnp.float32)
            mid = g1.astype(jnp.bfloat16)
            lo = (g1 - mid.astype(jnp.float32)).astype(jnp.bfloat16)
            z = ret[j, :, :, cols].reshape(grp_rows, wide)
            dims_t = (((0,), (0,)), ((), ()))
            tot = lax.dot_general(lo, z, dims_t, preferred_element_type=jnp.float32)
            tot = tot + lax.dot_general(mid, z, dims_t, preferred_element_type=jnp.float32)
            tot = tot + lax.dot_general(hi, z, dims_t, preferred_element_type=jnp.float32)
            acc[:, cols] += tot
            return carry

        lax.fori_loop(0, hidden // wide, comb, 0)

    def fin(n, carry):
        cols = pl.ds(pl.multiple_of(n * wide, wide), wide)
        y_ref[:, cols] = acc[:, cols].astype(jnp.bfloat16)
        return carry

    lax.fori_loop(0, hidden // wide, fin, 0)
    for j in range(n_grp):
        for r in range(per_grp):
            if not local(j, r):
                for e in range(local_exp):
                    giveback(j, r, e).wait_send()
    for axis in range(2):
        for d in steps[1:]:
            table(axis, d).wait_send()
            spread(axis, d).wait_send()
    for s in steps:
        for axis, d, dc, e in pieces():
            if d or dc:
                piece(axis, s, d, dc, e).wait_send()


def expert_layer(mesh, resid_h, expert_idx, gate_vals, w_gate, w_up, w_down):
    n_cp, n_x = mesh.shape['cp'], mesh.shape['tp'] // 2
    rows, hidden = resid_h.shape
    top_k = expert_idx.shape[1]
    local_exp, _, ffn = w_gate.shape
    experts = local_exp * n_cp * n_x * 2
    cap = rows * top_k // experts
    slots = local_exp * 2 * n_x
    dims = (n_cp, n_x, top_k, experts, cap, local_exp)
    vm = pl.BlockSpec(memory_space=pltpu.VMEM)
    hb = pl.BlockSpec(memory_space=pl.ANY)
    dma = pltpu.SemaphoreType.DMA
    sems = [dma((2, n_x, slots)), dma((2, n_cp, slots)), dma((n_cp, slots)), dma((n_cp, slots))] + [dma((2, n_x - 1))] * 4
    return pl.pallas_call(
        functools.partial(moe_kernel, dims),
        out_shape=jax.ShapeDtypeStruct((rows, hidden), jnp.bfloat16),
        in_specs=[vm, vm, vm, hb, hb, hb],
        out_specs=vm,
        scratch_shapes=[
            pltpu.VMEM((local_exp, hidden, ffn), jnp.bfloat16),
            pltpu.VMEM((local_exp, hidden, ffn), jnp.bfloat16),
            pltpu.VMEM((local_exp, ffn, hidden), jnp.bfloat16),
            pltpu.VMEM((2, n_x, slots, cap, hidden // 2), jnp.bfloat16),
            pltpu.VMEM((n_cp, slots, cap, hidden), jnp.bfloat16),
            pltpu.VMEM((n_cp, slots, cap, hidden), jnp.bfloat16),
            pltpu.VMEM((experts, rows), jnp.float32),
            pltpu.VMEM((experts, rows), jnp.float32),
            pltpu.VMEM((2, n_x - 1, experts, rows), jnp.float32),
            pltpu.VMEM((2, n_x - 1, rows, hidden // 2), jnp.bfloat16),
            pltpu.VMEM((slots * cap, rows), jnp.float32),
            pltpu.VMEM((slots * cap, rows), jnp.float32),
            pltpu.VMEM((rows, hidden), jnp.float32),
            pltpu.VMEM((2 * n_x * cap, ffn), jnp.bfloat16),
            pltpu.SemaphoreType.DMA((3,)),
        ] + sems,
        compiler_params=pltpu.CompilerParams(collective_id=1, has_side_effects=True, vmem_limit_bytes=64 * 1024 * 1024 - 65536),
        name='moe',
    )(resid_h, expert_idx.T, gate_vals.T, w_gate, w_up, w_down)


def solution(mesh):
    row_spec = P(('dp', 'cp', 'tp'), None)
    head_spec = P(None, 'tp', None)
    expert_spec = P(('cp', 'tp'), None, None)

    def device_step(hidden_in, w_query, w_key, w_value, w_out, expert_idx, gate_vals, w_gate, w_up, w_down):
        resid_h = attention_residual(mesh, hidden_in, w_query, w_key, w_value, w_out)
        return expert_layer(mesh, resid_h, expert_idx, gate_vals, w_gate, w_up, w_down)

    return jax.shard_map(device_step, mesh=mesh, in_specs=(row_spec, head_spec, head_spec, head_spec, P('tp', None, None), row_spec, row_spec, expert_spec, expert_spec, expert_spec), out_specs=row_spec, check_vma=False)
```

```python
import functools
import jax
import jax.numpy as jnp
from jax import lax
from jax.experimental import pallas as pl
from jax.experimental.pallas import tpu as pltpu
from jax.sharding import PartitionSpec as P

MESH = pl.DeviceIdType.MESH


def attn_kernel(dims, x_in, wq, wk, wv, wo, h_ref,
                stage, pair, xbuf, wall, snd, land, kvp, vt, mask, osnd, oland, wfull,
                lsem, xs, xr, ws, wr, qs, qr, ks, kr, os_, orr, gs, gr, ps, pr, ys, yr):
    n_cp, n_x, hd = dims
    rows, hidden = x_in.shape
    half = rows // 2
    units = n_x // 2
    n_units = n_cp * n_x
    blk = units * rows
    bf, f32 = jnp.bfloat16, jnp.float32
    cp, tp = lax.axis_index('cp'), lax.axis_index('tp')
    x_pos, core = tp // 2, tp % 2
    head = x_pos * n_cp + cp
    nbr = lambda d: (x_pos + d + n_x) % n_x
    at_x = lambda xx: {'cp': cp, 'tp': xx * 2 + core}
    at_y = lambda yy: {'cp': yy, 'tp': tp}
    partner = {'cp': cp, 'tp': x_pos * 2 + 1 - core}

    def remote(src, dst, s_sem, r_sem, dev):
        return pltpu.make_async_remote_copy(src, dst, s_sem, r_sem, device_id=dev, device_id_type=MESH)

    def place(c, xx):
        hi = xx // units
        return (c * (1 - hi) + (2 * n_cp - 1 - c) * hi) * units + xx % units

    barrier = pltpu.get_barrier_semaphore()
    offs = [(dy, dx) for dy in range(n_cp) for dx in range(n_x) if dy or dx]
    for dy, dx in offs:
        pl.semaphore_signal(barrier, inc=1, device_id={'cp': (cp + dy) % n_cp, 'tp': nbr(dx) * 2 + core}, device_id_type=MESH)
    pl.semaphore_signal(barrier, inc=1, device_id=partner, device_id_type=MESH)
    loads = [pltpu.make_async_copy(w, stage.at[m], lsem.at[m + 1]) for m, w in enumerate((wq, wk, wv))]
    load_o = pltpu.make_async_copy(wo, wfull.at[tp], lsem.at[0])
    for ld in loads:
        ld.start()
    load_o.start()
    pl.semaphore_wait(barrier, len(offs) + 1)

    parts = [pl.ds(0, half), pl.ds(half, half)]
    def x_own(d, p):
        slot = 0 if d == 1 else n_x - 2
        return remote(x_in.at[parts[p]], xbuf.at[slot, parts[p]], xs.at[slot, p], xr.at[slot, p], at_x(nbr(d)))

    def x_fwd(d):
        slot, p = (0, 0) if d == 1 else (n_x - 2, 1)
        return remote(xbuf.at[slot, parts[p]], xbuf.at[1, parts[p]], xs.at[1, p], xr.at[1, p], at_x(nbr(d)))

    for d, p in ((1, 0), (-1, 1), (1, 1), (-1, 0)):
        x_own(d, p).start()
    w_part = remote(wall.at[core], wall.at[core], gs.at[0], gr.at[0], partner)
    heads = wall.shape[2] // (3 * hd)
    rows_d = pair.shape[0] // heads
    for ld in loads:
        ld.wait()

    def unpack(n, carry):
        for m in range(3):
            pair[...] = stage[m, pl.ds(pl.multiple_of(n * rows_d * heads, rows_d * heads), rows_d * heads), :].astype(f32)
            for i in range(heads):
                wall[core, pl.ds(pl.multiple_of(n * rows_d, rows_d), rows_d), (i * 3 + m) * hd:(i * 3 + m + 1) * hd] = pair[pl.ds(i, rows_d, stride=heads), :].astype(bf)
        return carry

    lax.fori_loop(0, hidden // rows_d, unpack, 0)
    w_part.start()

    r_io = lax.broadcasted_iota(jnp.int32, (blk, blk), 0)
    c_io = lax.broadcasted_iota(jnp.int32, (blk, blk), 1)
    q_pos = c_io + jnp.where(c_io >= rows, rows, 0) + core * rows
    k_pos = r_io + jnp.where(r_io >= rows, rows, 0)
    mask[0:blk, :] = jnp.where(k_pos + core * rows <= q_pos, 1.0, 0.0)
    mask[blk:, :] = jnp.where(k_pos + (1 - core) * rows <= q_pos, 1.0, 0.0)

    def span(p):
        return pl.ds(0, rows) if p is None else parts[p]

    def q_copy(s, p, dy, u):
        at = span(p)
        k = p or 0
        return remote(snd.at[s, dy - 1, at], land.at[u, at], qs.at[s, k, dy - 1], qr.at[s, k, dy - 1], at_y((cp + dy) % n_cp))

    def q_send(s, p, dy):
        return q_copy(s, p, dy, place(cp, nbr(-s)))

    def q_recv(s, p, dy):
        return q_copy(s, p, dy, place((cp - dy + n_cp) % n_cp, nbr(-s)))

    def kv_send(s, dy):
        u = place((cp - dy + n_cp) % n_cp, nbr(-s))
        return remote(land.at[u, :, pl.ds(hd, 2 * hd)], kvp.at[u], ks.at[s, dy], kr.at[s, dy], partner)

    def project(s, p=None):
        at = span(p)
        for dy in (1, n_cp - 1, 2, 0):
            i = (cp + dy) % n_cp
            cols = pl.ds(pl.multiple_of((i % 2) * 3 * hd, 3 * hd), 3 * hd)
            xv = x_in[at] if s == 0 else xbuf[s - 1, at]
            res = jnp.dot(xv, wall[i // 2, :, cols], preferred_element_type=f32).astype(bf)
            if dy:
                snd[s, dy - 1, at] = res
                q_send(s, p, dy).start()
            else:
                land[place(cp, nbr(-s)), at] = res
                if p is None or (s, p) in ((1, 1), (n_x - 1, 0)):
                    kv_send(s, 0).start()

    def halves(s):
        return (0, 1) if s in (1, n_x - 1) else (None,)

    def relay(s):
        for dy in (1, n_cp - 1, 2):
            for p in halves(s):
                q_recv(s, p, dy).wait_recv()
            kv_send(s, dy).start()

    x_own(1, 0).wait_recv()
    x_fwd(1).start()
    x_own(-1, 1).wait_recv()
    x_fwd(-1).start()
    w_part.wait_recv()
    project(0)

    w_mid = wo.shape[0] * 3 // 4
    w_qtr = (wo.shape[0] - w_mid) // n_cp
    w_cut = w_mid // 2
    tp_at = lambda s: nbr(-s) * 2 + core

    def w_rows(p, y):
        if p == 0:
            return pl.ds(0, w_cut)
        if p == 1:
            return pl.ds(w_cut, w_mid - w_cut)
        return pl.ds(pl.multiple_of(w_mid + y * w_qtr, w_qtr), w_qtr)

    def w_own(d, p):
        slot = 0 if d == 1 else n_x - 2
        blk_ref = wfull.at[tp, w_rows(p, cp)]
        return remote(blk_ref, blk_ref, ws.at[slot, p], wr.at[slot, p], at_x(nbr(d)))

    def w_fwd(d, p):
        blk_ref = wfull.at[nbr(-d) * 2 + core, w_rows(p, cp)]
        return remote(blk_ref, blk_ref, ws.at[1, p], wr.at[1, p], at_x(nbr(d)))

    def w_share(s, dy):
        blk_ref = wfull.at[tp_at(s), w_rows(2, cp)]
        return remote(blk_ref, blk_ref, ys.at[s - 1, dy - 1], yr.at[s - 1, dy - 1], at_y((cp + dy) % n_cp))

    def w_pass(s, p):
        blk_ref = wfull.at[tp_at(s), pl.ds(p * w_mid, w_mid if p == 0 else wo.shape[0] - w_mid)]
        return remote(blk_ref, blk_ref, ps.at[s, p], pr.at[s, p], partner)

    relays = ((1, 0), (-1, 1), (-1, 2))
    own_sends = ((1, 0), (-1, 2), (-1, 1), (1, 2), (-1, 0), (1, 1))
    y_offs = (1, n_cp - 1, 2)

    def w_step0():
        for d, p in relays:
            w_own(d, p).wait_recv()
            w_fwd(d, p).start()
        for dy in y_offs:
            w_share(n_x - 1, dy).start()

    def w_step1():
        w_own(1, 2).wait_recv()
        for dy in y_offs:
            w_share(1, dy).start()
        w_own(1, 1).wait_recv()
        w_own(-1, 0).wait_recv()
        w_pass(1, 0).start()
        w_pass(n_x - 1, 0).start()

    def w_step2():
        for d, p in relays[::-1]:
            w_fwd(d, p).wait_recv()
        for dy in y_offs:
            w_share(2, dy).start()
        w_pass(2, 0).start()

    def w_step3():
        for s in (1, n_x - 1):
            for dy in y_offs:
                w_share(s, dy).wait_recv()
            w_pass(s, 1).start()

    def w_step4():
        for dy in y_offs:
            w_share(2, dy).wait_recv()
        w_pass(2, 1).start()

    load_o.wait()
    for d, p in own_sends:
        w_own(d, p).start()
    for p in range(2):
        w_pass(0, p).start()

    project(1, 0)
    project(n_x - 1, 1)
    x_own(1, 1).wait_recv()
    project(1, 1)
    x_own(-1, 0).wait_recv()
    project(n_x - 1, 0)
    relay(0)
    x_fwd(1).wait_recv()
    x_fwd(-1).wait_recv()
    project(2)
    for s in (1, n_x - 1, 2):
        relay(s)
    for s in range(n_x):
        for dy in range(n_cp):
            kv_send(s, dy).wait_recv()
    w_step0()

    c_exp = hd ** -0.5 * 1.4426950408889634
    nt = (((1,), (1,)), ((), ()))

    def o_copy(b, u):
        hi = b // n_cp
        dst_cp = b * (1 - hi) + (2 * n_cp - 1 - b) * hi
        dst_x = hi * units + u
        cols = pl.ds(pl.multiple_of(head * hd, hd), hd)
        cpy = remote(osnd.at[b * units + u], oland.at[:, cols], os_.at[b * units + u], orr.at[head], {'cp': dst_cp, 'tp': dst_x * 2 + core})
        own = jnp.logical_and(dst_cp == cp, dst_x == x_pos)
        return cpy, own, cols

    def flip(b):
        own_u = pl.ds(b * units, units)
        cols = pl.ds(pl.multiple_of(b * blk, blk), blk)
        vt[0, :, cols] = land[own_u, :, 2 * hd:3 * hd].reshape(blk, hd).T
        vt[1, :, cols] = kvp[own_u, :, hd:2 * hd].reshape(blk, hd).T


    def step(b, t, carry, masked):
        mx, den, acc = carry
        q = land[pl.ds(b * units, units), :, 0:hd].reshape(blk, hd)
        own_u = pl.ds(t * units, units)
        cols = pl.ds(pl.multiple_of(t * blk, blk), blk)
        k1 = land[own_u, :, hd:2 * hd].reshape(blk, hd)
        k2 = kvp[own_u, :, 0:hd].reshape(blk, hd)
        s1 = lax.dot_general(k1, q, nt, preferred_element_type=f32)
        s2 = lax.dot_general(k2, q, nt, preferred_element_type=f32)
        if masked:
            s1 = jnp.where(mask[0:blk, :] > 0.5, s1, -1e30)
            s2 = jnp.where(mask[blk:, :] > 0.5, s2, -1e30)
        m1 = jnp.maximum(mx, jnp.max(s1, axis=0, keepdims=True))
        p1 = jnp.exp2((s1 - m1) * c_exp)
        new = jnp.maximum(m1, jnp.max(s2, axis=0, keepdims=True))
        p2 = jnp.exp2((s2 - new) * c_exp)
        keep = jnp.exp2((mx - new) * c_exp)
        mend = jnp.exp2((m1 - new) * c_exp)
        den = den * keep + jnp.sum(p1, axis=0, keepdims=True) * mend + jnp.sum(p2, axis=0, keepdims=True)
        acc = acc * keep + jnp.dot(vt[0, :, cols], p1.astype(bf), preferred_element_type=f32) * mend + jnp.dot(vt[1, :, cols], p2.astype(bf), preferred_element_type=f32)
        return new, den, acc

    def attend(b, carry):
        for at, todo in zip(RELAY_AT, (w_step1, w_step2, w_step3)):
            pl.when(b == at)(todo)

        start = (jnp.full((1, blk), -1e30, f32), jnp.zeros((1, blk), f32), jnp.zeros((hd, blk), f32))
        flip(b)
        start = step(b, b, start, True)
        start = lax.fori_loop(0, b // 2, lambda t, c: step(b, 2 * t + 1, step(b, 2 * t, c, False), False), start)
        mx, den, acc = lax.fori_loop(b // 2 * 2, b, lambda t, c: step(b, t, c, False), start)
        o = (acc / den).T.astype(bf)
        for u in range(units):
            cpy, own, cols = o_copy(b, u)
            osnd[b * units + u] = o[u * rows:(u + 1) * rows]

            @pl.when(own)
            def _():
                oland[:, cols] = o[u * rows:(u + 1) * rows]

            @pl.when(jnp.logical_not(own))
            def _():
                cpy.start()
        return carry

    lax.fori_loop(0, 2 * n_cp, attend, 0)
    w_step4()
    for dy, dx in offs:
        src = nbr(dx) * n_cp + (cp + dy) % n_cp
        cols = pl.ds(pl.multiple_of(src * hd, hd), hd)
        remote(osnd.at[0], oland.at[:, cols], os_.at[0], orr.at[src], partner).wait_recv()
    for s in range(n_x):
        for p in range(2):
            w_pass(s, p).wait_recv()

    wide = 512
    def out(n, carry):
        cols = pl.ds(pl.multiple_of(n * wide, wide), wide)
        tot = jnp.dot(oland[...], wfull[:, :, cols].reshape(hidden_o, wide), preferred_element_type=f32)
        h_ref[:, cols] = (x_in[:, cols].astype(f32) + tot).astype(bf)
        return carry

    hidden_o = n_x * 2 * wo.shape[0]
    lax.fori_loop(0, hidden // wide, out, 0)

    for d, p in ((1, 0), (-1, 1), (1, 1), (-1, 0)):
        x_own(d, p).wait_send()
    for d, p in own_sends:
        w_own(d, p).wait_send()
    for d, p in relays:
        w_fwd(d, p).wait_send()
    for d in (1, -1):
        x_fwd(d).wait_send()
    w_part.wait_send()
    for s in range(n_x):
        for p in range(2):
            w_pass(s, p).wait_send()
        for dy in y_offs:
            if s:
                w_share(s, dy).wait_send()
        for dy in range(n_cp):
            kv_send(s, dy).wait_send()
            if dy:
                for p in halves(s):
                    q_send(s, p, dy).wait_send()

    def drain(b, carry):
        for u in range(units):
            cpy, own, cols = o_copy(b, u)

            @pl.when(jnp.logical_not(own))
            def _():
                cpy.wait_send()
        return carry

    lax.fori_loop(0, 2 * n_cp, drain, 0)


RELAY_AT = (4, 6, 7)


def attention_residual(mesh, hidden_in, w_query, w_key, w_value, w_out):
    n_cp, n_x = mesh.shape['cp'], mesh.shape['tp'] // 2
    rows, hidden = hidden_in.shape
    heads, hd = w_query.shape[1:]
    wq, wk, wv = (w.reshape(hidden * heads, hd) for w in (w_query, w_key, w_value))
    wo = w_out.reshape(heads * hd, hidden)
    units = n_x // 2
    n_units = n_cp * n_x
    blk = units * rows
    bf = jnp.bfloat16
    dma = pltpu.SemaphoreType.DMA
    vm = pl.BlockSpec(memory_space=pltpu.VMEM)
    hb = pl.BlockSpec(memory_space=pl.ANY)
    return pl.pallas_call(
        functools.partial(attn_kernel, (n_cp, n_x, hd)),
        out_shape=jax.ShapeDtypeStruct((rows, hidden), bf),
        in_specs=[vm, hb, hb, hb, hb],
        out_specs=vm,
        scratch_shapes=[
            pltpu.VMEM((3, heads * hidden, hd), bf),
            pltpu.VMEM((heads * 256, hd), jnp.float32),
            pltpu.VMEM((n_x - 1, rows, hidden), bf),
            pltpu.VMEM((2, hidden, heads * 3 * hd), bf),
            pltpu.VMEM((n_x, n_cp - 1, rows, 3 * hd), bf),
            pltpu.VMEM((n_units, rows, 3 * hd), bf),
            pltpu.VMEM((n_units, rows, 2 * hd), bf),
            pltpu.VMEM((2, hd, n_units * rows), bf),
            pltpu.VMEM((2 * blk, blk), jnp.float32),
            pltpu.VMEM((n_units, rows, hd), bf),
            pltpu.VMEM((rows, n_units * hd), bf),
            pltpu.VMEM((2 * n_x, heads * hd, hidden), bf),
            dma((4,)), dma((n_x - 1, 2)), dma((n_x - 1, 2)), dma((n_x - 1, 3)), dma((n_x - 1, 3)),
            dma((n_x, 2, n_cp - 1)), dma((n_x, 2, n_cp - 1)), dma((n_x, n_cp)), dma((n_x, n_cp)),
            dma((n_units,)), dma((n_units,)), dma((1,)), dma((1,)), dma((n_x, 2)), dma((n_x, 2)),
            dma((n_x - 1, n_cp - 1)), dma((n_x - 1, n_cp - 1)),
        ],
        compiler_params=pltpu.CompilerParams(collective_id=2, has_side_effects=True, vmem_limit_bytes=60 * 1024 * 1024),
        name='attn',
    )(hidden_in, wq, wk, wv, wo)


def moe_kernel(dims, h_in, idx_ref, gate_ref, wg_hbm, wu_hbm, wd_hbm, y_ref,
               wg, wu, wd, send, recv, ret, slots, gates, tabs, held, dmat, gmat, gsp, acc, hid,
               wsem, ssem, rsem, bsem, csem, tsem, tgot, hsem, hgot):
    n_cp, n_x, top_k, experts, cap, local_exp = dims
    per_grp = 2 * n_x
    rows = h_in.shape[0]
    hidden = h_in.shape[1]
    cp, tp = lax.axis_index('cp'), lax.axis_index('tp')
    x_pos, core = tp // 2, tp % 2

    chips = [(dy, dx) for dy in range(n_cp) for dx in range(n_x)]
    near = [(0, 1), (1, 0), (0, n_x - 1), (n_cp - 1, 0)]
    odd = [o for o in chips if o[0] % 2 and o[1] % 2]
    even = [o for o in chips if not (o[0] % 2 or o[1] % 2)][::-1]
    rest = [o for o in chips if o not in near + odd + even]
    plan = [[(dy, dx, dc) for dc in range(2) for dy, dx in g] for g in (near, odd, even, rest)]
    n_grp = len(plan)

    def fwd(j, r):
        dy, dx, dc = plan[j][r]
        return (cp + dy) % n_cp, ((x_pos + dx) % n_x) * 2 + (core + dc) % 2

    def back(j, r):
        dy, dx, dc = plan[j][r]
        return (cp + n_cp - dy) % n_cp, ((x_pos + n_x - dx) % n_x) * 2 + (core + dc) % 2

    def local(j, r):
        return plan[j][r] == (0, 0, 0)

    barrier = pltpu.get_barrier_semaphore()
    for j in range(n_grp):
        for r in range(per_grp):
            if not local(j, r):
                c, t = fwd(j, r)
                pl.semaphore_signal(barrier, inc=1, device_id={'cp': c, 'tp': t}, device_id_type=MESH)
    loads = [pltpu.make_async_copy(wg_hbm, wg, wsem.at[0]), pltpu.make_async_copy(wu_hbm, wu, wsem.at[1]), pltpu.make_async_copy(wd_hbm, wd, wsem.at[2])]
    for ld in loads:
        ld.start()

    e_iota = lax.broadcasted_iota(jnp.int32, (experts, rows), 0)
    hit = jnp.zeros((experts, rows), jnp.float32)
    gsel = jnp.zeros((experts, rows), jnp.float32)
    for k in range(top_k):
        m = idx_ref[k:k + 1, :] == e_iota
        hit = hit + jnp.where(m, 1.0, 0.0)
        gsel = gsel + jnp.where(m, gate_ref[k:k + 1, :], 0.0)
    before = jnp.where(lax.broadcasted_iota(jnp.int32, (rows, rows), 0) < lax.broadcasted_iota(jnp.int32, (rows, rows), 1), 1.0, 0.0)
    count = jnp.dot(hit.astype(jnp.bfloat16), before.astype(jnp.bfloat16), preferred_element_type=jnp.float32)
    slots[...] = jnp.where(hit > 0.5, count, -1.0)
    gates[...] = gsel
    c_iota = lax.broadcasted_iota(jnp.int32, (cap, rows), 0).astype(jnp.float32)

    def build(j, ref):
        for e in range(local_exp):
            for r in range(per_grp):
                c, t = fwd(j, r)
                expert = (c * (2 * n_x) + t) * local_exp + e
                eq = jnp.broadcast_to(slots[pl.ds(expert, 1), :], (cap, rows)) == c_iota
                val = jnp.broadcast_to(gates[pl.ds(expert, 1), :], (cap, rows))
                ref[pl.ds((e * per_grp + r) * cap, cap), :] = jnp.where(eq, val, 0.0)

    steps = (0, 1, n_x - 1, 2)
    where_is = {plan[j][r]: (j, r) for j in range(n_grp) for r in range(per_grp)}
    mid = hidden // 2
    cols_of = (pl.ds(0, mid), pl.ds(mid, mid))

    def peer(axis, d, dc):
        if axis == 0:
            return cp, ((x_pos + d) % n_x) * 2 + (core + dc) % 2
        return (cp + d) % n_cp, x_pos * 2 + (core + dc) % 2

    def table(axis, d):
        c, t = peer(axis, d, 0)
        return pltpu.make_async_remote_copy(slots, tabs.at[axis, d - 1], tsem.at[axis, d - 1], tgot.at[axis, d - 1], device_id={'cp': c, 'tp': t}, device_id_type=MESH)

    h_half = rows // 2
    h_parts = (pl.ds(0, h_half), pl.ds(h_half, h_half))

    def spread(axis, d, p):
        c, t = peer(axis, d, 0)
        return pltpu.make_async_remote_copy(h_in.at[h_parts[p], cols_of[axis]], held.at[axis, d - 1, h_parts[p]], hsem.at[axis, d - 1, p], hgot.at[axis, d - 1, p], device_id={'cp': c, 'tp': t}, device_id_type=MESH)

    def onward(axis, p):
        d = (1, n_x - 1)[p]
        c, t = peer(axis, d, 0)
        return pltpu.make_async_remote_copy(held.at[axis, d - 1, h_parts[p]], held.at[axis, 1, h_parts[p]], hsem.at[axis, 1, p], hgot.at[axis, 1, p], device_id={'cp': c, 'tp': t}, device_id_type=MESH)

    spreads = [(axis, d, p) for d, p in ((1, 0), (n_x - 1, 1), (1, 1), (n_x - 1, 0)) for axis in range(2)]
    onwards = [(axis, p) for p in range(2) for axis in range(2)]

    def piece(axis, s, d, dc, e):
        c, t = peer(1 - axis, d, dc)
        k = e * per_grp + d * 2 + dc
        j, r = where_is[(d, s, dc) if axis == 0 else (s, d, dc)]
        src, dst = send.at[axis, s, k], recv.at[j, e * per_grp + r, :, cols_of[axis]]
        got = rsem.at[axis, j, e * per_grp + r]
        if d == 0 and dc == 0:
            return pltpu.make_async_copy(src, dst, got)
        return pltpu.make_async_remote_copy(src, dst, ssem.at[axis, s, k], got, device_id={'cp': c, 'tp': t}, device_id_type=MESH)

    def pieces():
        return [(axis, d, dc, e) for e in range(local_exp) for dc in range(2) for d in steps for axis in range(2)]

    def select(axis, s):
        tab = slots if s == 0 else tabs.at[axis, s - 1]
        for d in range(n_x):
            for dc in range(2):
                c, t = peer(1 - axis, d, dc)
                for e in range(local_exp):
                    expert = (c * (2 * n_x) + t) * local_exp + e
                    eq = jnp.broadcast_to(tab[pl.ds(expert, 1), :], (cap, rows)) == c_iota
                    dmat[pl.ds((e * per_grp + d * 2 + dc) * cap, cap), :] = jnp.where(eq, 1.0, 0.0)

        def fill(n, carry):
            cols = pl.ds(pl.multiple_of(n * wide, wide), wide)
            if s == 0:
                from_h = h_in[:, pl.ds(pl.multiple_of(axis * mid + n * wide, wide), wide)]
            else:
                from_h = held[axis, s - 1, :, cols]
            picked = jnp.dot(dmat[...].astype(jnp.bfloat16), from_h, preferred_element_type=jnp.float32).astype(jnp.bfloat16)
            send[axis, s, :, :, cols] = picked.reshape(local_exp * per_grp, cap, wide)
            return carry

        lax.fori_loop(0, mid // wide, fill, 0)

    def giveback(j, r, e):
        c, t = back(j, r)
        if local(j, r):
            return (pltpu.make_async_copy(recv.at[j, e * per_grp + r], ret.at[j, e * per_grp + r], csem.at[j, e * per_grp + r]))
        return (pltpu.make_async_remote_copy(recv.at[j, e * per_grp + r], ret.at[j, e * per_grp + r], bsem.at[j, e * per_grp + r], csem.at[j, e * per_grp + r], device_id={'cp': c, 'tp': t}, device_id_type=MESH))

    grp_rows = local_exp * per_grp * cap
    half = per_grp * cap
    wide = 512
    order = range(per_grp)
    pl.semaphore_wait(barrier, n_grp * per_grp - 1)
    for axis, d, p in spreads:
        spread(axis, d, p).start()
    for d in steps[1:]:
        for axis in range(2):
            table(axis, d).start()
    for axis in range(2):
        select(axis, 0)
    for axis, p in onwards:
        spread(axis, (1, n_x - 1)[p], p).wait_recv()
        onward(axis, p).start()
    for axis, d, dc, e in pieces():
        piece(axis, 0, d, dc, e).start()
    for s in steps[1:]:
        for axis in range(2):
            table(axis, s).wait_recv()
            if s == 2:
                for p in range(2):
                    onward(axis, p).wait_recv()
            else:
                spread(axis, s, 1 if s == 1 else 0).wait_recv()
            select(axis, s)
        for axis, d, dc, e in pieces():
            piece(axis, s, d, dc, e).start()

    def init(n, carry):
        cols = pl.ds(pl.multiple_of(n * wide, wide), wide)
        acc[:, cols] = h_in[:, cols].astype(jnp.float32)
        return carry

    lax.fori_loop(0, hidden // wide, init, 0)
    for ld in loads:
        ld.wait()
    ffn = wg.shape[2]
    for j in range(n_grp):
        for e in range(local_exp):
            for r in order:
                dy, dx, dc = plan[j][r]
                for axis, (s, d) in enumerate(((dx, dy), (dy, dx))):
                    cpy = piece(axis, s, d, dc, e)
                    if d == 0 and dc == 0:
                        cpy.wait()
                    else:
                        cpy.wait_recv()

            def up(n, carry, j=j, e=e):
                cols = pl.ds(pl.multiple_of(n * 256, 256), 256)
                rows_in = recv[j, pl.ds(e * per_grp, per_grp)].reshape(half, hidden)
                g = jnp.dot(rows_in, wg[e, :, cols], preferred_element_type=jnp.float32)
                u = jnp.dot(rows_in, wu[e, :, cols], preferred_element_type=jnp.float32)
                hid[:, cols] = (g * (1.0 / (1.0 + jnp.exp(-g))) * u).astype(jnp.bfloat16)
                return carry

            def down(n, carry, j=j, e=e):
                cols = pl.ds(pl.multiple_of(n * wide, wide), wide)
                z = jnp.dot(hid[...], wd[e, :, cols], preferred_element_type=jnp.float32).astype(jnp.bfloat16)
                recv[j, pl.ds(e * per_grp, per_grp), :, cols] = z.reshape(per_grp, cap, wide)
                return carry

            lax.fori_loop(0, ffn // 256, up, 0)
            lax.fori_loop(0, hidden // wide, down, 0)
            for r in order:
                giveback(j, r, e).start()

    for j in range(n_grp):
        build(j, gmat)
        g0 = gmat[...].T
        hi = g0.astype(jnp.bfloat16)
        g1 = g0 - hi.astype(jnp.float32)
        mid_g = g1.astype(jnp.bfloat16)
        gsp[0] = hi
        gsp[1] = mid_g
        gsp[2] = (g1 - mid_g.astype(jnp.float32)).astype(jnp.bfloat16)
        for e in range(local_exp):
            for r in order:
                if local(j, r):
                    giveback(j, r, e).wait()
                else:
                    giveback(j, r, e).wait_recv()

        def comb(n, carry, j=j):
            cols = pl.ds(pl.multiple_of(n * wide, wide), wide)
            z = ret[j, :, :, cols].reshape(grp_rows, wide)
            tot = jnp.dot(gsp[2], z, preferred_element_type=jnp.float32)
            tot = tot + jnp.dot(gsp[1], z, preferred_element_type=jnp.float32)
            tot = tot + jnp.dot(gsp[0], z, preferred_element_type=jnp.float32)
            acc[:, cols] += tot
            return carry

        lax.fori_loop(0, hidden // wide, comb, 0)

    def fin(n, carry):
        cols = pl.ds(pl.multiple_of(n * wide, wide), wide)
        y_ref[:, cols] = acc[:, cols].astype(jnp.bfloat16)
        return carry

    lax.fori_loop(0, hidden // wide, fin, 0)
    for j in range(n_grp):
        for r in range(per_grp):
            if not local(j, r):
                for e in range(local_exp):
                    giveback(j, r, e).wait_send()
    for axis in range(2):
        for d in steps[1:]:
            table(axis, d).wait_send()
        for p in range(2):
            onward(axis, p).wait_send()
    for axis, d, p in spreads:
        spread(axis, d, p).wait_send()
    for s in steps:
        for axis, d, dc, e in pieces():
            if d or dc:
                piece(axis, s, d, dc, e).wait_send()


def expert_layer(mesh, resid_h, expert_idx, gate_vals, w_gate, w_up, w_down):
    n_cp, n_x = mesh.shape['cp'], mesh.shape['tp'] // 2
    rows, hidden = resid_h.shape
    top_k = expert_idx.shape[1]
    local_exp, _, ffn = w_gate.shape
    experts = local_exp * n_cp * n_x * 2
    cap = rows * top_k // experts
    slots = local_exp * 2 * n_x
    dims = (n_cp, n_x, top_k, experts, cap, local_exp)
    vm = pl.BlockSpec(memory_space=pltpu.VMEM)
    hb = pl.BlockSpec(memory_space=pl.ANY)
    dma = pltpu.SemaphoreType.DMA
    sems = [dma((2, n_x, slots)), dma((2, n_cp, slots)), dma((n_cp, slots)), dma((n_cp, slots))] + [dma((2, n_x - 1))] * 2 + [dma((2, n_x - 1, 2))] * 2
    return pl.pallas_call(
        functools.partial(moe_kernel, dims),
        out_shape=jax.ShapeDtypeStruct((rows, hidden), jnp.bfloat16),
        in_specs=[vm, vm, vm, hb, hb, hb],
        out_specs=vm,
        scratch_shapes=[
            pltpu.VMEM((local_exp, hidden, ffn), jnp.bfloat16),
            pltpu.VMEM((local_exp, hidden, ffn), jnp.bfloat16),
            pltpu.VMEM((local_exp, ffn, hidden), jnp.bfloat16),
            pltpu.VMEM((2, n_x, slots, cap, hidden // 2), jnp.bfloat16),
            pltpu.VMEM((n_cp, slots, cap, hidden), jnp.bfloat16),
            pltpu.VMEM((n_cp, slots, cap, hidden), jnp.bfloat16),
            pltpu.VMEM((experts, rows), jnp.float32),
            pltpu.VMEM((experts, rows), jnp.float32),
            pltpu.VMEM((2, n_x - 1, experts, rows), jnp.float32),
            pltpu.VMEM((2, n_x - 1, rows, hidden // 2), jnp.bfloat16),
            pltpu.VMEM((slots * cap, rows), jnp.float32),
            pltpu.VMEM((slots * cap, rows), jnp.float32),
            pltpu.VMEM((3, rows, slots * cap), jnp.bfloat16),
            pltpu.VMEM((rows, hidden), jnp.float32),
            pltpu.VMEM((2 * n_x * cap, ffn), jnp.bfloat16),
            pltpu.SemaphoreType.DMA((3,)),
        ] + sems,
        compiler_params=pltpu.CompilerParams(collective_id=1, has_side_effects=True, vmem_limit_bytes=64 * 1024 * 1024 - 65536),
        name='moe',
    )(resid_h, expert_idx.T, gate_vals.T, w_gate, w_up, w_down)


def solution(mesh):
    row_spec = P(('dp', 'cp', 'tp'), None)
    head_spec = P(None, 'tp', None)
    expert_spec = P(('cp', 'tp'), None, None)

    def device_step(hidden_in, w_query, w_key, w_value, w_out, expert_idx, gate_vals, w_gate, w_up, w_down):
        resid_h = attention_residual(mesh, hidden_in, w_query, w_key, w_value, w_out)
        return expert_layer(mesh, resid_h, expert_idx, gate_vals, w_gate, w_up, w_down)

    return jax.shard_map(device_step, mesh=mesh, in_specs=(row_spec, head_spec, head_spec, head_spec, P('tp', None, None), row_spec, row_spec, expert_spec, expert_spec, expert_spec), out_specs=row_spec, check_vma=False)
```

```python
import functools
import jax
import jax.numpy as jnp
from jax import lax
from jax.experimental import pallas as pl
from jax.experimental.pallas import tpu as pltpu
from jax.sharding import PartitionSpec as P

MESH = pl.DeviceIdType.MESH


def attn_kernel(dims, x_in, wq, wk, wv, wo, h_ref,
                stage, pair, xbuf, wall, snd, land, kvp, vt, mask, osnd, oland, wfull,
                lsem, xs, xr, ws, wr, qs, qr, ks, kr, os_, orr, gs, gr, ps, pr, ys, yr):
    n_cp, n_x, hd = dims
    rows, hidden = x_in.shape
    half = rows // 2
    units = n_x // 2
    n_units = n_cp * n_x
    blk = units * rows
    bf, f32 = jnp.bfloat16, jnp.float32
    cp, tp = lax.axis_index('cp'), lax.axis_index('tp')
    x_pos, core = tp // 2, tp % 2
    head = x_pos * n_cp + cp
    nbr = lambda d: (x_pos + d + n_x) % n_x
    at_x = lambda xx: {'cp': cp, 'tp': xx * 2 + core}
    at_y = lambda yy: {'cp': yy, 'tp': tp}
    partner = {'cp': cp, 'tp': x_pos * 2 + 1 - core}

    def remote(src, dst, s_sem, r_sem, dev):
        return pltpu.make_async_remote_copy(src, dst, s_sem, r_sem, device_id=dev, device_id_type=MESH)

    def place(c, xx):
        hi = xx // units
        return (c * (1 - hi) + (2 * n_cp - 1 - c) * hi) * units + xx % units

    barrier = pltpu.get_barrier_semaphore()
    offs = [(dy, dx) for dy in range(n_cp) for dx in range(n_x) if dy or dx]
    for dy, dx in offs:
        pl.semaphore_signal(barrier, inc=1, device_id={'cp': (cp + dy) % n_cp, 'tp': nbr(dx) * 2 + core}, device_id_type=MESH)
    pl.semaphore_signal(barrier, inc=1, device_id=partner, device_id_type=MESH)
    loads = [pltpu.make_async_copy(w, stage.at[m], lsem.at[m + 1]) for m, w in enumerate((wq, wk, wv))]
    load_o = pltpu.make_async_copy(wo, wfull.at[tp], lsem.at[0])
    for ld in loads:
        ld.start()
    load_o.start()
    pl.semaphore_wait(barrier, len(offs) + 1)

    parts = [pl.ds(0, half), pl.ds(half, half)]
    def x_own(d, p):
        slot = 0 if d == 1 else n_x - 2
        return remote(x_in.at[parts[p]], xbuf.at[slot, parts[p]], xs.at[slot, p], xr.at[slot, p], at_x(nbr(d)))

    def x_fwd(d):
        slot, p = (0, 0) if d == 1 else (n_x - 2, 1)
        return remote(xbuf.at[slot, parts[p]], xbuf.at[1, parts[p]], xs.at[1, p], xr.at[1, p], at_x(nbr(d)))

    for d, p in ((1, 0), (-1, 1), (1, 1), (-1, 0)):
        x_own(d, p).start()
    w_part = remote(wall.at[core], wall.at[core], gs.at[0], gr.at[0], partner)
    heads = wall.shape[2] // (3 * hd)
    rows_d = pair.shape[0] // heads
    for ld in loads:
        ld.wait()

    def unpack(n, carry):
        for m in range(3):
            pair[...] = stage[m, pl.ds(pl.multiple_of(n * rows_d * heads, rows_d * heads), rows_d * heads), :].astype(f32)
            for i in range(heads):
                wall[core, pl.ds(pl.multiple_of(n * rows_d, rows_d), rows_d), (i * 3 + m) * hd:(i * 3 + m + 1) * hd] = pair[pl.ds(i, rows_d, stride=heads), :].astype(bf)
        return carry

    lax.fori_loop(0, hidden // rows_d, unpack, 0)
    w_part.start()

    r_io = lax.broadcasted_iota(jnp.int32, (blk, blk), 0)
    c_io = lax.broadcasted_iota(jnp.int32, (blk, blk), 1)
    q_pos = c_io + jnp.where(c_io >= rows, rows, 0) + core * rows
    k_pos = r_io + jnp.where(r_io >= rows, rows, 0)
    mask[0:blk, :] = jnp.where(k_pos + core * rows <= q_pos, 1.0, 0.0)
    mask[blk:, :] = jnp.where(k_pos + (1 - core) * rows <= q_pos, 1.0, 0.0)

    def span(p):
        return pl.ds(0, rows) if p is None else parts[p]

    def q_copy(s, p, dy, u):
        at = span(p)
        k = p or 0
        return remote(snd.at[s, dy - 1, at], land.at[u, at], qs.at[s, k, dy - 1], qr.at[s, k, dy - 1], at_y((cp + dy) % n_cp))

    def q_send(s, p, dy):
        return q_copy(s, p, dy, place(cp, nbr(-s)))

    def q_recv(s, p, dy):
        return q_copy(s, p, dy, place((cp - dy + n_cp) % n_cp, nbr(-s)))

    def kv_send(s, dy):
        u = place((cp - dy + n_cp) % n_cp, nbr(-s))
        return remote(land.at[u, :, pl.ds(hd, 2 * hd)], kvp.at[u], ks.at[s, dy], kr.at[s, dy], partner)

    def project(s, p=None):
        at = span(p)
        for dy in (1, n_cp - 1, 2, 0):
            i = (cp + dy) % n_cp
            cols = pl.ds(pl.multiple_of((i % 2) * 3 * hd, 3 * hd), 3 * hd)
            xv = x_in[at] if s == 0 else xbuf[s - 1, at]
            res = jnp.dot(xv, wall[i // 2, :, cols], preferred_element_type=f32).astype(bf)
            if dy:
                snd[s, dy - 1, at] = res
                q_send(s, p, dy).start()
            else:
                land[place(cp, nbr(-s)), at] = res
                if p is None or (s, p) in ((1, 1), (n_x - 1, 0)):
                    kv_send(s, 0).start()

    def halves(s):
        return (0, 1) if s in (1, n_x - 1) else (None,)

    def relay(s):
        for dy in (1, n_cp - 1, 2):
            for p in halves(s):
                q_recv(s, p, dy).wait_recv()
            kv_send(s, dy).start()

    x_own(1, 0).wait_recv()
    x_fwd(1).start()
    x_own(-1, 1).wait_recv()
    x_fwd(-1).start()
    w_part.wait_recv()
    project(0)

    w_mid = wo.shape[0] * 3 // 4
    w_qtr = (wo.shape[0] - w_mid) // n_cp
    w_cut = w_mid // 2
    tp_at = lambda s: nbr(-s) * 2 + core

    def w_rows(p, y):
        if p == 0:
            return pl.ds(0, w_cut)
        if p == 1:
            return pl.ds(w_cut, w_mid - w_cut)
        return pl.ds(pl.multiple_of(w_mid + y * w_qtr, w_qtr), w_qtr)

    def w_own(d, p):
        slot = 0 if d == 1 else n_x - 2
        blk_ref = wfull.at[tp, w_rows(p, cp)]
        return remote(blk_ref, blk_ref, ws.at[slot, p], wr.at[slot, p], at_x(nbr(d)))

    def w_fwd(d, p):
        blk_ref = wfull.at[nbr(-d) * 2 + core, w_rows(p, cp)]
        return remote(blk_ref, blk_ref, ws.at[1, p], wr.at[1, p], at_x(nbr(d)))

    def w_share(s, dy):
        blk_ref = wfull.at[tp_at(s), w_rows(2, cp)]
        return remote(blk_ref, blk_ref, ys.at[s - 1, dy - 1], yr.at[s - 1, dy - 1], at_y((cp + dy) % n_cp))

    def w_pass(s, p):
        blk_ref = wfull.at[tp_at(s), pl.ds(p * w_mid, w_mid if p == 0 else wo.shape[0] - w_mid)]
        return remote(blk_ref, blk_ref, ps.at[s, p], pr.at[s, p], partner)

    relays = ((1, 0), (-1, 1), (-1, 2))
    own_sends = ((1, 0), (-1, 2), (-1, 1), (1, 2), (-1, 0), (1, 1))
    y_offs = (1, n_cp - 1, 2)

    def w_step0():
        for d, p in relays:
            w_own(d, p).wait_recv()
            w_fwd(d, p).start()
        for dy in y_offs:
            w_share(n_x - 1, dy).start()

    def w_step1():
        w_own(1, 2).wait_recv()
        for dy in y_offs:
            w_share(1, dy).start()
        w_own(1, 1).wait_recv()
        w_own(-1, 0).wait_recv()
        w_pass(1, 0).start()
        w_pass(n_x - 1, 0).start()

    def w_step2():
        for d, p in relays[::-1]:
            w_fwd(d, p).wait_recv()
        for dy in y_offs:
            w_share(2, dy).start()
        w_pass(2, 0).start()

    def w_step3():
        for s in (1, n_x - 1):
            for dy in y_offs:
                w_share(s, dy).wait_recv()
            w_pass(s, 1).start()

    def w_step4():
        for dy in y_offs:
            w_share(2, dy).wait_recv()
        w_pass(2, 1).start()

    load_o.wait()
    for d, p in own_sends:
        w_own(d, p).start()
    for p in range(2):
        w_pass(0, p).start()

    project(1, 0)
    project(n_x - 1, 1)
    x_own(1, 1).wait_recv()
    project(1, 1)
    x_own(-1, 0).wait_recv()
    project(n_x - 1, 0)
    relay(0)
    x_fwd(1).wait_recv()
    x_fwd(-1).wait_recv()
    project(2)
    for s in (1, n_x - 1, 2):
        relay(s)
    for s in range(n_x):
        for dy in range(n_cp):
            kv_send(s, dy).wait_recv()
    w_step0()

    c_exp = hd ** -0.5 * 1.4426950408889634
    nt = (((1,), (1,)), ((), ()))

    def o_copy(b, u):
        hi = b // n_cp
        dst_cp = b * (1 - hi) + (2 * n_cp - 1 - b) * hi
        dst_x = hi * units + u
        cols = pl.ds(pl.multiple_of(head * hd, hd), hd)
        cpy = remote(osnd.at[b * units + u], oland.at[:, cols], os_.at[b * units + u], orr.at[head], {'cp': dst_cp, 'tp': dst_x * 2 + core})
        own = jnp.logical_and(dst_cp == cp, dst_x == x_pos)
        return cpy, own, cols

    def flip(b):
        own_u = pl.ds(b * units, units)
        cols = pl.ds(pl.multiple_of(b * blk, blk), blk)
        vt[0, :, cols] = land[own_u, :, 2 * hd:3 * hd].reshape(blk, hd).T
        vt[1, :, cols] = kvp[own_u, :, hd:2 * hd].reshape(blk, hd).T


    def step(b, t, carry, masked):
        mx, den, acc = carry
        q = land[pl.ds(b * units, units), :, 0:hd].reshape(blk, hd)
        own_u = pl.ds(t * units, units)
        cols = pl.ds(pl.multiple_of(t * blk, blk), blk)
        k1 = land[own_u, :, hd:2 * hd].reshape(blk, hd)
        k2 = kvp[own_u, :, 0:hd].reshape(blk, hd)
        s1 = lax.dot_general(k1, q, nt, preferred_element_type=f32)
        s2 = lax.dot_general(k2, q, nt, preferred_element_type=f32)
        if masked:
            s1 = jnp.where(mask[0:blk, :] > 0.5, s1, -1e30)
            s2 = jnp.where(mask[blk:, :] > 0.5, s2, -1e30)
        m1 = jnp.maximum(mx, jnp.max(s1, axis=0, keepdims=True))
        p1 = jnp.exp2((s1 - m1) * c_exp)
        new = jnp.maximum(m1, jnp.max(s2, axis=0, keepdims=True))
        p2 = jnp.exp2((s2 - new) * c_exp)
        keep = jnp.exp2((mx - new) * c_exp)
        mend = jnp.exp2((m1 - new) * c_exp)
        den = den * keep + jnp.sum(p1, axis=0, keepdims=True) * mend + jnp.sum(p2, axis=0, keepdims=True)
        acc = acc * keep + jnp.dot(vt[0, :, cols], p1.astype(bf), preferred_element_type=f32) * mend + jnp.dot(vt[1, :, cols], p2.astype(bf), preferred_element_type=f32)
        return new, den, acc

    def attend(b, carry):
        for at, todo in zip(RELAY_AT, (w_step1, w_step2, w_step3)):
            pl.when(b == at)(todo)

        start = (jnp.full((1, blk), -1e30, f32), jnp.zeros((1, blk), f32), jnp.zeros((hd, blk), f32))
        flip(b)
        start = step(b, b, start, True)
        start = lax.fori_loop(0, b // 2, lambda t, c: step(b, 2 * t + 1, step(b, 2 * t, c, False), False), start)
        mx, den, acc = lax.fori_loop(b // 2 * 2, b, lambda t, c: step(b, t, c, False), start)
        o = (acc / den).T.astype(bf)
        for u in range(units):
            cpy, own, cols = o_copy(b, u)
            osnd[b * units + u] = o[u * rows:(u + 1) * rows]

            @pl.when(own)
            def _():
                oland[:, cols] = o[u * rows:(u + 1) * rows]

            @pl.when(jnp.logical_not(own))
            def _():
                cpy.start()
        return carry

    lax.fori_loop(0, 2 * n_cp, attend, 0)
    w_step4()
    for dy, dx in offs:
        src = nbr(dx) * n_cp + (cp + dy) % n_cp
        cols = pl.ds(pl.multiple_of(src * hd, hd), hd)
        remote(osnd.at[0], oland.at[:, cols], os_.at[0], orr.at[src], partner).wait_recv()
    for s in range(n_x):
        for p in range(2):
            w_pass(s, p).wait_recv()

    wide = 512
    def out(n, carry):
        cols = pl.ds(pl.multiple_of(n * wide, wide), wide)
        tot = jnp.dot(oland[...], wfull[:, :, cols].reshape(hidden_o, wide), preferred_element_type=f32)
        h_ref[:, cols] = (x_in[:, cols].astype(f32) + tot).astype(bf)
        return carry

    hidden_o = n_x * 2 * wo.shape[0]
    lax.fori_loop(0, hidden // wide, out, 0)

    for d, p in ((1, 0), (-1, 1), (1, 1), (-1, 0)):
        x_own(d, p).wait_send()
    for d, p in own_sends:
        w_own(d, p).wait_send()
    for d, p in relays:
        w_fwd(d, p).wait_send()
    for d in (1, -1):
        x_fwd(d).wait_send()
    w_part.wait_send()
    for s in range(n_x):
        for p in range(2):
            w_pass(s, p).wait_send()
        for dy in y_offs:
            if s:
                w_share(s, dy).wait_send()
        for dy in range(n_cp):
            kv_send(s, dy).wait_send()
            if dy:
                for p in halves(s):
                    q_send(s, p, dy).wait_send()

    def drain(b, carry):
        for u in range(units):
            cpy, own, cols = o_copy(b, u)

            @pl.when(jnp.logical_not(own))
            def _():
                cpy.wait_send()
        return carry

    lax.fori_loop(0, 2 * n_cp, drain, 0)


RELAY_AT = (4, 6, 7)


def attention_residual(mesh, hidden_in, w_query, w_key, w_value, w_out):
    n_cp, n_x = mesh.shape['cp'], mesh.shape['tp'] // 2
    rows, hidden = hidden_in.shape
    heads, hd = w_query.shape[1:]
    wq, wk, wv = (w.reshape(hidden * heads, hd) for w in (w_query, w_key, w_value))
    wo = w_out.reshape(heads * hd, hidden)
    units = n_x // 2
    n_units = n_cp * n_x
    blk = units * rows
    bf = jnp.bfloat16
    dma = pltpu.SemaphoreType.DMA
    vm = pl.BlockSpec(memory_space=pltpu.VMEM)
    hb = pl.BlockSpec(memory_space=pl.ANY)
    return pl.pallas_call(
        functools.partial(attn_kernel, (n_cp, n_x, hd)),
        out_shape=jax.ShapeDtypeStruct((rows, hidden), bf),
        in_specs=[vm, hb, hb, hb, hb],
        out_specs=vm,
        scratch_shapes=[
            pltpu.VMEM((3, heads * hidden, hd), bf),
            pltpu.VMEM((heads * 256, hd), jnp.float32),
            pltpu.VMEM((n_x - 1, rows, hidden), bf),
            pltpu.VMEM((2, hidden, heads * 3 * hd), bf),
            pltpu.VMEM((n_x, n_cp - 1, rows, 3 * hd), bf),
            pltpu.VMEM((n_units, rows, 3 * hd), bf),
            pltpu.VMEM((n_units, rows, 2 * hd), bf),
            pltpu.VMEM((2, hd, n_units * rows), bf),
            pltpu.VMEM((2 * blk, blk), jnp.float32),
            pltpu.VMEM((n_units, rows, hd), bf),
            pltpu.VMEM((rows, n_units * hd), bf),
            pltpu.VMEM((2 * n_x, heads * hd, hidden), bf),
            dma((4,)), dma((n_x - 1, 2)), dma((n_x - 1, 2)), dma((n_x - 1, 3)), dma((n_x - 1, 3)),
            dma((n_x, 2, n_cp - 1)), dma((n_x, 2, n_cp - 1)), dma((n_x, n_cp)), dma((n_x, n_cp)),
            dma((n_units,)), dma((n_units,)), dma((1,)), dma((1,)), dma((n_x, 2)), dma((n_x, 2)),
            dma((n_x - 1, n_cp - 1)), dma((n_x - 1, n_cp - 1)),
        ],
        compiler_params=pltpu.CompilerParams(collective_id=2, has_side_effects=True, vmem_limit_bytes=60 * 1024 * 1024),
        name='attn',
    )(hidden_in, wq, wk, wv, wo)


def moe_kernel(dims, h_in, idx_ref, gate_ref, wg_hbm, wu_hbm, wd_hbm, y_ref,
               wg, wu, wd, send, recv, ret, slots, gates, slots16, slots_of, tabs, held, dmat, gmat, gsp, acc, hid,
               wsem, ssem, rsem, bsem, csem, tsem, tgot, hsem, hgot):
    n_cp, n_x, top_k, experts, cap, local_exp = dims
    per_grp = 2 * n_x
    rows = h_in.shape[0]
    hidden = h_in.shape[1]
    cp, tp = lax.axis_index('cp'), lax.axis_index('tp')
    x_pos, core = tp // 2, tp % 2

    chips = [(dy, dx) for dy in range(n_cp) for dx in range(n_x)]
    near = [(0, 1), (1, 0), (0, n_x - 1), (n_cp - 1, 0)]
    odd = [o for o in chips if o[0] % 2 and o[1] % 2]
    even = [o for o in chips if not (o[0] % 2 or o[1] % 2)][::-1]
    rest = [o for o in chips if o not in near + odd + even]
    plan = [[(dy, dx, dc) for dc in range(2) for dy, dx in g] for g in (near, odd, even, rest)]
    n_grp = len(plan)

    def fwd(j, r):
        dy, dx, dc = plan[j][r]
        return (cp + dy) % n_cp, ((x_pos + dx) % n_x) * 2 + (core + dc) % 2

    def back(j, r):
        dy, dx, dc = plan[j][r]
        return (cp + n_cp - dy) % n_cp, ((x_pos + n_x - dx) % n_x) * 2 + (core + dc) % 2

    def local(j, r):
        return plan[j][r] == (0, 0, 0)

    barrier = pltpu.get_barrier_semaphore()
    for j in range(n_grp):
        for r in range(per_grp):
            if not local(j, r):
                c, t = fwd(j, r)
                pl.semaphore_signal(barrier, inc=1, device_id={'cp': c, 'tp': t}, device_id_type=MESH)
    loads = [pltpu.make_async_copy(wg_hbm, wg, wsem.at[0]), pltpu.make_async_copy(wu_hbm, wu, wsem.at[1]), pltpu.make_async_copy(wd_hbm, wd, wsem.at[2])]
    for ld in loads:
        ld.start()

    e_iota = lax.broadcasted_iota(jnp.int32, (experts, rows), 0)
    hit = jnp.zeros((experts, rows), jnp.float32)
    gsel = jnp.zeros((experts, rows), jnp.float32)
    for k in range(top_k):
        m = idx_ref[k:k + 1, :] == e_iota
        hit = hit + jnp.where(m, 1.0, 0.0)
        gsel = gsel + jnp.where(m, gate_ref[k:k + 1, :], 0.0)
    before = jnp.where(lax.broadcasted_iota(jnp.int32, (rows, rows), 0) < lax.broadcasted_iota(jnp.int32, (rows, rows), 1), 1.0, 0.0)
    count = jnp.dot(hit.astype(jnp.bfloat16), before.astype(jnp.bfloat16), preferred_element_type=jnp.float32)
    slots[...] = jnp.where(hit > 0.5, count, -1.0)
    slots16[...] = slots[...].astype(jnp.bfloat16)
    gates[...] = gsel
    c_iota = lax.broadcasted_iota(jnp.int32, (cap, rows), 0).astype(jnp.float32)

    def build(j, ref):
        for e in range(local_exp):
            for r in range(per_grp):
                c, t = fwd(j, r)
                expert = (c * (2 * n_x) + t) * local_exp + e
                eq = jnp.broadcast_to(slots[pl.ds(expert, 1), :], (cap, rows)) == c_iota
                val = jnp.broadcast_to(gates[pl.ds(expert, 1), :], (cap, rows))
                ref[pl.ds((e * per_grp + r) * cap, cap), :] = jnp.where(eq, val, 0.0)

    steps = (0, 1, n_x - 1, 2)
    where_is = {plan[j][r]: (j, r) for j in range(n_grp) for r in range(per_grp)}
    mid = hidden // 2
    cols_of = (pl.ds(0, mid), pl.ds(mid, mid))

    def peer(axis, d, dc):
        if axis == 0:
            return cp, ((x_pos + d) % n_x) * 2 + (core + dc) % 2
        return (cp + d) % n_cp, x_pos * 2 + (core + dc) % 2

    def table(axis, d):
        c, t = peer(axis, d, 0)
        return pltpu.make_async_remote_copy(slots16, tabs.at[axis, d - 1], tsem.at[axis, d - 1], tgot.at[axis, d - 1], device_id={'cp': c, 'tp': t}, device_id_type=MESH)

    h_half = rows // 2
    h_parts = (pl.ds(0, h_half), pl.ds(h_half, h_half))

    def spread(axis, d, p):
        c, t = peer(axis, d, 0)
        return pltpu.make_async_remote_copy(h_in.at[h_parts[p], cols_of[axis]], held.at[axis, d - 1, h_parts[p]], hsem.at[axis, d - 1, p], hgot.at[axis, d - 1, p], device_id={'cp': c, 'tp': t}, device_id_type=MESH)

    def onward(axis, p):
        d = (1, n_x - 1)[p]
        c, t = peer(axis, d, 0)
        return pltpu.make_async_remote_copy(held.at[axis, d - 1, h_parts[p]], held.at[axis, 1, h_parts[p]], hsem.at[axis, 1, p], hgot.at[axis, 1, p], device_id={'cp': c, 'tp': t}, device_id_type=MESH)

    spreads = [(axis, d, p) for d, p in ((1, 0), (n_x - 1, 1), (1, 1), (n_x - 1, 0)) for axis in range(2)]
    onwards = [(axis, p) for p in range(2) for axis in range(2)]

    def piece(axis, s, d, dc, e):
        c, t = peer(1 - axis, d, dc)
        k = e * per_grp + d * 2 + dc
        j, r = where_is[(d, s, dc) if axis == 0 else (s, d, dc)]
        src, dst = send.at[axis, s, k], recv.at[j, e * per_grp + r, :, cols_of[axis]]
        got = rsem.at[axis, j, e * per_grp + r]
        if d == 0 and dc == 0:
            return pltpu.make_async_copy(src, dst, got)
        return pltpu.make_async_remote_copy(src, dst, ssem.at[axis, s, k], got, device_id={'cp': c, 'tp': t}, device_id_type=MESH)

    def pieces():
        return [(axis, d, dc, e) for e in range(local_exp) for dc in range(2) for d in steps for axis in range(2)]

    def select(axis, s):
        tab = slots if s == 0 else slots_of
        if s:
            slots_of[...] = tabs[axis, s - 1].astype(jnp.float32)
        for d in range(n_x):
            for dc in range(2):
                c, t = peer(1 - axis, d, dc)
                for e in range(local_exp):
                    expert = (c * (2 * n_x) + t) * local_exp + e
                    eq = jnp.broadcast_to(tab[pl.ds(expert, 1), :], (cap, rows)) == c_iota
                    dmat[pl.ds((e * per_grp + d * 2 + dc) * cap, cap), :] = jnp.where(eq, 1.0, 0.0)

        def fill(n, carry):
            cols = pl.ds(pl.multiple_of(n * wide, wide), wide)
            if s == 0:
                from_h = h_in[:, pl.ds(pl.multiple_of(axis * mid + n * wide, wide), wide)]
            else:
                from_h = held[axis, s - 1, :, cols]
            picked = jnp.dot(dmat[...].astype(jnp.bfloat16), from_h, preferred_element_type=jnp.float32).astype(jnp.bfloat16)
            send[axis, s, :, :, cols] = picked.reshape(local_exp * per_grp, cap, wide)
            return carry

        lax.fori_loop(0, mid // wide, fill, 0)

    def giveback(j, r, e):
        c, t = back(j, r)
        if local(j, r):
            return (pltpu.make_async_copy(recv.at[j, e * per_grp + r], ret.at[j, e * per_grp + r], csem.at[j, e * per_grp + r]))
        return (pltpu.make_async_remote_copy(recv.at[j, e * per_grp + r], ret.at[j, e * per_grp + r], bsem.at[j, e * per_grp + r], csem.at[j, e * per_grp + r], device_id={'cp': c, 'tp': t}, device_id_type=MESH))

    grp_rows = local_exp * per_grp * cap
    half = per_grp * cap
    wide = 512
    order = range(per_grp)
    pl.semaphore_wait(barrier, n_grp * per_grp - 1)
    for axis, d, p in spreads:
        spread(axis, d, p).start()
    for d in steps[1:]:
        for axis in range(2):
            table(axis, d).start()
    for axis in range(2):
        select(axis, 0)
    for axis, p in onwards:
        spread(axis, (1, n_x - 1)[p], p).wait_recv()
        onward(axis, p).start()
    for axis, d, dc, e in pieces():
        piece(axis, 0, d, dc, e).start()
    for s in steps[1:]:
        for axis in range(2):
            table(axis, s).wait_recv()
            if s == 2:
                for p in range(2):
                    onward(axis, p).wait_recv()
            else:
                spread(axis, s, 1 if s == 1 else 0).wait_recv()
            select(axis, s)
        for axis, d, dc, e in pieces():
            piece(axis, s, d, dc, e).start()

    def init(n, carry):
        cols = pl.ds(pl.multiple_of(n * wide, wide), wide)
        acc[:, cols] = h_in[:, cols].astype(jnp.float32)
        return carry

    lax.fori_loop(0, hidden // wide, init, 0)
    for ld in loads:
        ld.wait()
    ffn = wg.shape[2]
    for j in range(n_grp):
        for e in range(local_exp):
            for r in order:
                dy, dx, dc = plan[j][r]
                for axis, (s, d) in enumerate(((dx, dy), (dy, dx))):
                    cpy = piece(axis, s, d, dc, e)
                    if d == 0 and dc == 0:
                        cpy.wait()
                    else:
                        cpy.wait_recv()

            def up(n, carry, j=j, e=e):
                cols = pl.ds(pl.multiple_of(n * 256, 256), 256)
                rows_in = recv[j, pl.ds(e * per_grp, per_grp)].reshape(half, hidden)
                g = jnp.dot(rows_in, wg[e, :, cols], preferred_element_type=jnp.float32)
                u = jnp.dot(rows_in, wu[e, :, cols], preferred_element_type=jnp.float32)
                hid[:, cols] = (g * (1.0 / (1.0 + jnp.exp(-g))) * u).astype(jnp.bfloat16)
                return carry

            def down(n, carry, j=j, e=e):
                cols = pl.ds(pl.multiple_of(n * wide, wide), wide)
                z = jnp.dot(hid[...], wd[e, :, cols], preferred_element_type=jnp.float32).astype(jnp.bfloat16)
                recv[j, pl.ds(e * per_grp, per_grp), :, cols] = z.reshape(per_grp, cap, wide)
                return carry

            lax.fori_loop(0, ffn // 256, up, 0)
            lax.fori_loop(0, hidden // wide, down, 0)
            for r in order:
                giveback(j, r, e).start()

    for j in range(n_grp):
        build(j, gmat)
        g0 = gmat[...].T
        hi = g0.astype(jnp.bfloat16)
        g1 = g0 - hi.astype(jnp.float32)
        mid_g = g1.astype(jnp.bfloat16)
        gsp[0] = hi
        gsp[1] = mid_g
        gsp[2] = (g1 - mid_g.astype(jnp.float32)).astype(jnp.bfloat16)
        for e in range(local_exp):
            for r in order:
                if local(j, r):
                    giveback(j, r, e).wait()
                else:
                    giveback(j, r, e).wait_recv()

        def comb(n, carry, j=j):
            cols = pl.ds(pl.multiple_of(n * wide, wide), wide)
            z = ret[j, :, :, cols].reshape(grp_rows, wide)
            tot = jnp.dot(gsp[2], z, preferred_element_type=jnp.float32)
            tot = tot + jnp.dot(gsp[1], z, preferred_element_type=jnp.float32)
            tot = tot + jnp.dot(gsp[0], z, preferred_element_type=jnp.float32)
            if j == n_grp - 1:
                y_ref[:, cols] = (acc[:, cols] + tot).astype(jnp.bfloat16)
            else:
                acc[:, cols] += tot
            return carry

        lax.fori_loop(0, hidden // wide, comb, 0)

    for j in range(n_grp):
        for r in range(per_grp):
            if not local(j, r):
                for e in range(local_exp):
                    giveback(j, r, e).wait_send()
    for axis in range(2):
        for d in steps[1:]:
            table(axis, d).wait_send()
        for p in range(2):
            onward(axis, p).wait_send()
    for axis, d, p in spreads:
        spread(axis, d, p).wait_send()
    for s in steps:
        for axis, d, dc, e in pieces():
            if d or dc:
                piece(axis, s, d, dc, e).wait_send()


def expert_layer(mesh, resid_h, expert_idx, gate_vals, w_gate, w_up, w_down):
    n_cp, n_x = mesh.shape['cp'], mesh.shape['tp'] // 2
    rows, hidden = resid_h.shape
    top_k = expert_idx.shape[1]
    local_exp, _, ffn = w_gate.shape
    experts = local_exp * n_cp * n_x * 2
    cap = rows * top_k // experts
    slots = local_exp * 2 * n_x
    dims = (n_cp, n_x, top_k, experts, cap, local_exp)
    vm = pl.BlockSpec(memory_space=pltpu.VMEM)
    hb = pl.BlockSpec(memory_space=pl.ANY)
    dma = pltpu.SemaphoreType.DMA
    sems = [dma((2, n_x, slots)), dma((2, n_cp, slots)), dma((n_cp, slots)), dma((n_cp, slots))] + [dma((2, n_x - 1))] * 2 + [dma((2, n_x - 1, 2))] * 2
    return pl.pallas_call(
        functools.partial(moe_kernel, dims),
        out_shape=jax.ShapeDtypeStruct((rows, hidden), jnp.bfloat16),
        in_specs=[vm, vm, vm, hb, hb, hb],
        out_specs=vm,
        scratch_shapes=[
            pltpu.VMEM((local_exp, hidden, ffn), jnp.bfloat16),
            pltpu.VMEM((local_exp, hidden, ffn), jnp.bfloat16),
            pltpu.VMEM((local_exp, ffn, hidden), jnp.bfloat16),
            pltpu.VMEM((2, n_x, slots, cap, hidden // 2), jnp.bfloat16),
            pltpu.VMEM((n_cp, slots, cap, hidden), jnp.bfloat16),
            pltpu.VMEM((n_cp, slots, cap, hidden), jnp.bfloat16),
            pltpu.VMEM((experts, rows), jnp.float32),
            pltpu.VMEM((experts, rows), jnp.float32),
            pltpu.VMEM((experts, rows), jnp.bfloat16),
            pltpu.VMEM((experts, rows), jnp.float32),
            pltpu.VMEM((2, n_x - 1, experts, rows), jnp.bfloat16),
            pltpu.VMEM((2, n_x - 1, rows, hidden // 2), jnp.bfloat16),
            pltpu.VMEM((slots * cap, rows), jnp.float32),
            pltpu.VMEM((slots * cap, rows), jnp.float32),
            pltpu.VMEM((3, rows, slots * cap), jnp.bfloat16),
            pltpu.VMEM((rows, hidden), jnp.float32),
            pltpu.VMEM((2 * n_x * cap, ffn), jnp.bfloat16),
            pltpu.SemaphoreType.DMA((3,)),
        ] + sems,
        compiler_params=pltpu.CompilerParams(collective_id=1, has_side_effects=True, vmem_limit_bytes=64 * 1024 * 1024 - 65536),
        name='moe',
    )(resid_h, expert_idx.T, gate_vals.T, w_gate, w_up, w_down)


def solution(mesh):
    row_spec = P(('dp', 'cp', 'tp'), None)
    head_spec = P(None, 'tp', None)
    expert_spec = P(('cp', 'tp'), None, None)

    def device_step(hidden_in, w_query, w_key, w_value, w_out, expert_idx, gate_vals, w_gate, w_up, w_down):
        resid_h = attention_residual(mesh, hidden_in, w_query, w_key, w_value, w_out)
        return expert_layer(mesh, resid_h, expert_idx, gate_vals, w_gate, w_up, w_down)

    return jax.shard_map(device_step, mesh=mesh, in_specs=(row_spec, head_spec, head_spec, head_spec, P('tp', None, None), row_spec, row_spec, expert_spec, expert_spec, expert_spec), out_specs=row_spec, check_vma=False)
```

```python
import functools
import jax
import jax.numpy as jnp
from jax import lax
from jax.experimental import pallas as pl
from jax.experimental.pallas import tpu as pltpu
from jax.sharding import PartitionSpec as P

MESH = pl.DeviceIdType.MESH


def attn_kernel(dims, x_in, wq, wk, wv, wo, h_ref,
                stage, pair, xbuf, wall, snd, land, kvp, vt, mask, osnd, oland, wfull,
                lsem, xs, xr, ws, wr, qs, qr, ks, kr, os_, orr, gs, gr, ps, pr, ys, yr):
    n_cp, n_x, hd = dims
    rows, hidden = x_in.shape
    half = rows // 2
    units = n_x // 2
    n_units = n_cp * n_x
    blk = units * rows
    bf, f32 = jnp.bfloat16, jnp.float32
    cp, tp = lax.axis_index('cp'), lax.axis_index('tp')
    x_pos, core = tp // 2, tp % 2
    head = x_pos * n_cp + cp
    nbr = lambda d: (x_pos + d + n_x) % n_x
    at_x = lambda xx: {'cp': cp, 'tp': xx * 2 + core}
    at_y = lambda yy: {'cp': yy, 'tp': tp}
    partner = {'cp': cp, 'tp': x_pos * 2 + 1 - core}

    def remote(src, dst, s_sem, r_sem, dev):
        return pltpu.make_async_remote_copy(src, dst, s_sem, r_sem, device_id=dev, device_id_type=MESH)

    def place(c, xx):
        hi = xx // units
        return (c * (1 - hi) + (2 * n_cp - 1 - c) * hi) * units + xx % units

    barrier = pltpu.get_barrier_semaphore()
    offs = [(dy, dx) for dy in range(n_cp) for dx in range(n_x) if dy or dx]
    for dy, dx in offs:
        pl.semaphore_signal(barrier, inc=1, device_id={'cp': (cp + dy) % n_cp, 'tp': nbr(dx) * 2 + core}, device_id_type=MESH)
    pl.semaphore_signal(barrier, inc=1, device_id=partner, device_id_type=MESH)
    loads = [pltpu.make_async_copy(w, stage.at[m], lsem.at[m + 1]) for m, w in enumerate((wq, wk, wv))]
    load_o = pltpu.make_async_copy(wo, wfull.at[tp], lsem.at[0])
    for ld in loads:
        ld.start()
    load_o.start()
    pl.semaphore_wait(barrier, len(offs) + 1)

    parts = [pl.ds(0, half), pl.ds(half, half)]
    def x_own(d, p):
        slot = 0 if d == 1 else n_x - 2
        return remote(x_in.at[parts[p]], xbuf.at[slot, parts[p]], xs.at[slot, p], xr.at[slot, p], at_x(nbr(d)))

    def x_fwd(d):
        slot, p = (0, 0) if d == 1 else (n_x - 2, 1)
        return remote(xbuf.at[slot, parts[p]], xbuf.at[1, parts[p]], xs.at[1, p], xr.at[1, p], at_x(nbr(d)))

    for d, p in ((1, 0), (-1, 1), (1, 1), (-1, 0)):
        x_own(d, p).start()
    w_part = remote(wall.at[core], wall.at[core], gs.at[0], gr.at[0], partner)
    heads = wall.shape[2] // (3 * hd)
    rows_d = pair.shape[0] // heads
    for ld in loads:
        ld.wait()

    def unpack(n, carry):
        for m in range(3):
            pair[...] = stage[m, pl.ds(pl.multiple_of(n * rows_d * heads, rows_d * heads), rows_d * heads), :].astype(f32)
            for i in range(heads):
                wall[core, pl.ds(pl.multiple_of(n * rows_d, rows_d), rows_d), (i * 3 + m) * hd:(i * 3 + m + 1) * hd] = pair[pl.ds(i, rows_d, stride=heads), :].astype(bf)
        return carry

    lax.fori_loop(0, hidden // rows_d, unpack, 0)
    w_part.start()

    r_io = lax.broadcasted_iota(jnp.int32, (blk, blk), 0)
    c_io = lax.broadcasted_iota(jnp.int32, (blk, blk), 1)
    q_pos = c_io + jnp.where(c_io >= rows, rows, 0) + core * rows
    k_pos = r_io + jnp.where(r_io >= rows, rows, 0)
    mask[0:blk, :] = jnp.where(k_pos + core * rows <= q_pos, 1.0, 0.0)
    mask[blk:, :] = jnp.where(k_pos + (1 - core) * rows <= q_pos, 1.0, 0.0)

    def span(p):
        return pl.ds(0, rows) if p is None else parts[p]

    def q_copy(s, p, dy, u):
        at = span(p)
        k = p or 0
        return remote(snd.at[s, dy - 1, at], land.at[u, at], qs.at[s, k, dy - 1], qr.at[s, k, dy - 1], at_y((cp + dy) % n_cp))

    def q_send(s, p, dy):
        return q_copy(s, p, dy, place(cp, nbr(-s)))

    def q_recv(s, p, dy):
        return q_copy(s, p, dy, place((cp - dy + n_cp) % n_cp, nbr(-s)))

    def kv_send(s, dy):
        u = place((cp - dy + n_cp) % n_cp, nbr(-s))
        return remote(land.at[u, :, pl.ds(hd, 2 * hd)], kvp.at[u], ks.at[s, dy], kr.at[s, dy], partner)

    def project(s, p=None):
        at = span(p)
        for dy in (1, n_cp - 1, 2, 0):
            i = (cp + dy) % n_cp
            cols = pl.ds(pl.multiple_of((i % 2) * 3 * hd, 3 * hd), 3 * hd)
            xv = x_in[at] if s == 0 else xbuf[s - 1, at]
            res = jnp.dot(xv, wall[i // 2, :, cols], preferred_element_type=f32).astype(bf)
            if dy:
                snd[s, dy - 1, at] = res
                q_send(s, p, dy).start()
            else:
                land[place(cp, nbr(-s)), at] = res
                if p is None or (s, p) in ((1, 1), (n_x - 1, 0)):
                    kv_send(s, 0).start()

    def halves(s):
        return (0, 1) if s in (1, n_x - 1) else (None,)

    def relay(s):
        for dy in (1, n_cp - 1, 2):
            for p in halves(s):
                q_recv(s, p, dy).wait_recv()
            kv_send(s, dy).start()

    x_own(1, 0).wait_recv()
    x_fwd(1).start()
    x_own(-1, 1).wait_recv()
    x_fwd(-1).start()
    w_part.wait_recv()
    project(0)

    w_mid = wo.shape[0] * 3 // 4
    w_qtr = (wo.shape[0] - w_mid) // n_cp
    w_cut = w_mid // 2
    tp_at = lambda s: nbr(-s) * 2 + core

    def w_rows(p, y):
        if p == 0:
            return pl.ds(0, w_cut)
        if p == 1:
            return pl.ds(w_cut, w_mid - w_cut)
        return pl.ds(pl.multiple_of(w_mid + y * w_qtr, w_qtr), w_qtr)

    def w_own(d, p):
        slot = 0 if d == 1 else n_x - 2
        blk_ref = wfull.at[tp, w_rows(p, cp)]
        return remote(blk_ref, blk_ref, ws.at[slot, p], wr.at[slot, p], at_x(nbr(d)))

    def w_fwd(d, p):
        blk_ref = wfull.at[nbr(-d) * 2 + core, w_rows(p, cp)]
        return remote(blk_ref, blk_ref, ws.at[1, p], wr.at[1, p], at_x(nbr(d)))

    def w_share(s, dy):
        blk_ref = wfull.at[tp_at(s), w_rows(2, cp)]
        return remote(blk_ref, blk_ref, ys.at[s - 1, dy - 1], yr.at[s - 1, dy - 1], at_y((cp + dy) % n_cp))

    def w_pass(s, p):
        blk_ref = wfull.at[tp_at(s), pl.ds(p * w_mid, w_mid if p == 0 else wo.shape[0] - w_mid)]
        return remote(blk_ref, blk_ref, ps.at[s, p], pr.at[s, p], partner)

    relays = ((1, 0), (-1, 1), (-1, 2))
    own_sends = ((1, 0), (-1, 2), (-1, 1), (1, 2), (-1, 0), (1, 1))
    y_offs = (1, n_cp - 1, 2)

    def w_step0():
        for d, p in relays:
            w_own(d, p).wait_recv()
            w_fwd(d, p).start()
        for dy in y_offs:
            w_share(n_x - 1, dy).start()

    def w_step1():
        w_own(1, 2).wait_recv()
        for dy in y_offs:
            w_share(1, dy).start()
        w_own(1, 1).wait_recv()
        w_own(-1, 0).wait_recv()
        w_pass(1, 0).start()
        w_pass(n_x - 1, 0).start()

    def w_step2():
        for d, p in relays[::-1]:
            w_fwd(d, p).wait_recv()
        for dy in y_offs:
            w_share(2, dy).start()
        w_pass(2, 0).start()

    def w_step3():
        for s in (1, n_x - 1):
            for dy in y_offs:
                w_share(s, dy).wait_recv()
            w_pass(s, 1).start()

    def w_step4():
        for dy in y_offs:
            w_share(2, dy).wait_recv()
        w_pass(2, 1).start()

    load_o.wait()
    for d, p in own_sends:
        w_own(d, p).start()
    for p in range(2):
        w_pass(0, p).start()

    project(1, 0)
    project(n_x - 1, 1)
    x_own(1, 1).wait_recv()
    project(1, 1)
    x_own(-1, 0).wait_recv()
    project(n_x - 1, 0)
    relay(0)
    x_fwd(1).wait_recv()
    x_fwd(-1).wait_recv()
    project(2)
    for s in (1, n_x - 1, 2):
        relay(s)
    for s in range(n_x):
        for dy in range(n_cp):
            kv_send(s, dy).wait_recv()
    w_step0()

    c_exp = hd ** -0.5 * 1.4426950408889634
    nt = (((1,), (1,)), ((), ()))

    def o_copy(b, u):
        hi = b // n_cp
        dst_cp = b * (1 - hi) + (2 * n_cp - 1 - b) * hi
        dst_x = hi * units + u
        cols = pl.ds(pl.multiple_of(head * hd, hd), hd)
        cpy = remote(osnd.at[b * units + u], oland.at[:, cols], os_.at[b * units + u], orr.at[head], {'cp': dst_cp, 'tp': dst_x * 2 + core})
        own = jnp.logical_and(dst_cp == cp, dst_x == x_pos)
        return cpy, own, cols

    def flip(b):
        own_u = pl.ds(b * units, units)
        cols = pl.ds(pl.multiple_of(b * blk, blk), blk)
        vt[0, :, cols] = land[own_u, :, 2 * hd:3 * hd].reshape(blk, hd).T
        vt[1, :, cols] = kvp[own_u, :, hd:2 * hd].reshape(blk, hd).T


    def step(b, t, carry, masked):
        mx, den, acc = carry
        q = land[pl.ds(b * units, units), :, 0:hd].reshape(blk, hd)
        own_u = pl.ds(t * units, units)
        cols = pl.ds(pl.multiple_of(t * blk, blk), blk)
        k1 = land[own_u, :, hd:2 * hd].reshape(blk, hd)
        k2 = kvp[own_u, :, 0:hd].reshape(blk, hd)
        s1 = lax.dot_general(k1, q, nt, preferred_element_type=f32)
        s2 = lax.dot_general(k2, q, nt, preferred_element_type=f32)
        if masked:
            s1 = jnp.where(mask[0:blk, :] > 0.5, s1, -1e30)
            s2 = jnp.where(mask[blk:, :] > 0.5, s2, -1e30)
        m1 = jnp.maximum(mx, jnp.max(s1, axis=0, keepdims=True))
        p1 = jnp.exp2((s1 - m1) * c_exp)
        new = jnp.maximum(m1, jnp.max(s2, axis=0, keepdims=True))
        p2 = jnp.exp2((s2 - new) * c_exp)
        keep = jnp.exp2((mx - new) * c_exp)
        mend = jnp.exp2((m1 - new) * c_exp)
        den = den * keep + jnp.sum(p1, axis=0, keepdims=True) * mend + jnp.sum(p2, axis=0, keepdims=True)
        acc = acc * keep + jnp.dot(vt[0, :, cols], p1.astype(bf), preferred_element_type=f32) * mend + jnp.dot(vt[1, :, cols], p2.astype(bf), preferred_element_type=f32)
        return new, den, acc

    def attend(b, carry):
        for at, todo in zip(RELAY_AT, (w_step1, w_step2, w_step3)):
            pl.when(b == at)(todo)

        start = (jnp.full((1, blk), -1e30, f32), jnp.zeros((1, blk), f32), jnp.zeros((hd, blk), f32))
        flip(b)
        start = step(b, b, start, True)
        start = lax.fori_loop(0, b // 2, lambda t, c: step(b, 2 * t + 1, step(b, 2 * t, c, False), False), start)
        mx, den, acc = lax.fori_loop(b // 2 * 2, b, lambda t, c: step(b, t, c, False), start)
        o = (acc / den).T.astype(bf)
        for u in range(units):
            cpy, own, cols = o_copy(b, u)
            osnd[b * units + u] = o[u * rows:(u + 1) * rows]

            @pl.when(own)
            def _():
                oland[:, cols] = o[u * rows:(u + 1) * rows]

            @pl.when(jnp.logical_not(own))
            def _():
                cpy.start()
        return carry

    lax.fori_loop(0, 2 * n_cp, attend, 0)
    w_step4()
    for dy, dx in offs:
        src = nbr(dx) * n_cp + (cp + dy) % n_cp
        cols = pl.ds(pl.multiple_of(src * hd, hd), hd)
        remote(osnd.at[0], oland.at[:, cols], os_.at[0], orr.at[src], partner).wait_recv()
    for s in range(n_x):
        for p in range(2):
            w_pass(s, p).wait_recv()

    wide = 512
    def out(n, carry):
        cols = pl.ds(pl.multiple_of(n * wide, wide), wide)
        tot = jnp.dot(oland[...], wfull[:, :, cols].reshape(hidden_o, wide), preferred_element_type=f32)
        h_ref[:, cols] = (x_in[:, cols].astype(f32) + tot).astype(bf)
        return carry

    hidden_o = n_x * 2 * wo.shape[0]
    lax.fori_loop(0, hidden // wide, out, 0)

    for d, p in ((1, 0), (-1, 1), (1, 1), (-1, 0)):
        x_own(d, p).wait_send()
    for d, p in own_sends:
        w_own(d, p).wait_send()
    for d, p in relays:
        w_fwd(d, p).wait_send()
    for d in (1, -1):
        x_fwd(d).wait_send()
    w_part.wait_send()
    for s in range(n_x):
        for p in range(2):
            w_pass(s, p).wait_send()
        for dy in y_offs:
            if s:
                w_share(s, dy).wait_send()
        for dy in range(n_cp):
            kv_send(s, dy).wait_send()
            if dy:
                for p in halves(s):
                    q_send(s, p, dy).wait_send()

    def drain(b, carry):
        for u in range(units):
            cpy, own, cols = o_copy(b, u)

            @pl.when(jnp.logical_not(own))
            def _():
                cpy.wait_send()
        return carry

    lax.fori_loop(0, 2 * n_cp, drain, 0)


RELAY_AT = (4, 6, 7)


def attention_residual(mesh, hidden_in, w_query, w_key, w_value, w_out):
    n_cp, n_x = mesh.shape['cp'], mesh.shape['tp'] // 2
    rows, hidden = hidden_in.shape
    heads, hd = w_query.shape[1:]
    wq, wk, wv = (w.reshape(hidden * heads, hd) for w in (w_query, w_key, w_value))
    wo = w_out.reshape(heads * hd, hidden)
    units = n_x // 2
    n_units = n_cp * n_x
    blk = units * rows
    bf = jnp.bfloat16
    dma = pltpu.SemaphoreType.DMA
    vm = pl.BlockSpec(memory_space=pltpu.VMEM)
    hb = pl.BlockSpec(memory_space=pl.ANY)
    return pl.pallas_call(
        functools.partial(attn_kernel, (n_cp, n_x, hd)),
        out_shape=jax.ShapeDtypeStruct((rows, hidden), bf),
        in_specs=[vm, hb, hb, hb, hb],
        out_specs=vm,
        scratch_shapes=[
            pltpu.VMEM((3, heads * hidden, hd), bf),
            pltpu.VMEM((heads * 256, hd), jnp.float32),
            pltpu.VMEM((n_x - 1, rows, hidden), bf),
            pltpu.VMEM((2, hidden, heads * 3 * hd), bf),
            pltpu.VMEM((n_x, n_cp - 1, rows, 3 * hd), bf),
            pltpu.VMEM((n_units, rows, 3 * hd), bf),
            pltpu.VMEM((n_units, rows, 2 * hd), bf),
            pltpu.VMEM((2, hd, n_units * rows), bf),
            pltpu.VMEM((2 * blk, blk), jnp.float32),
            pltpu.VMEM((n_units, rows, hd), bf),
            pltpu.VMEM((rows, n_units * hd), bf),
            pltpu.VMEM((2 * n_x, heads * hd, hidden), bf),
            dma((4,)), dma((n_x - 1, 2)), dma((n_x - 1, 2)), dma((n_x - 1, 3)), dma((n_x - 1, 3)),
            dma((n_x, 2, n_cp - 1)), dma((n_x, 2, n_cp - 1)), dma((n_x, n_cp)), dma((n_x, n_cp)),
            dma((n_units,)), dma((n_units,)), dma((1,)), dma((1,)), dma((n_x, 2)), dma((n_x, 2)),
            dma((n_x - 1, n_cp - 1)), dma((n_x - 1, n_cp - 1)),
        ],
        compiler_params=pltpu.CompilerParams(collective_id=2, has_side_effects=True, vmem_limit_bytes=60 * 1024 * 1024),
        name='attn',
    )(hidden_in, wq, wk, wv, wo)


def moe_kernel(dims, h_in, idx_ref, gate_ref, wg_hbm, wu_hbm, wd_hbm, y_ref,
               wg, wu, wd, send, recv, ret, slots, gates, slots16, slots_of, tabs, held, dmat, gmat, gsp, acc, hid,
               wsem, ssem, rsem, bsem, csem, tsem, tgot, hsem, hgot):
    n_cp, n_x, top_k, experts, cap, local_exp = dims
    per_grp = 2 * n_x
    rows = h_in.shape[0]
    hidden = h_in.shape[1]
    cp, tp = lax.axis_index('cp'), lax.axis_index('tp')
    x_pos, core = tp // 2, tp % 2

    chips = [(dy, dx) for dy in range(n_cp) for dx in range(n_x)]
    near = [(0, 1), (1, 0), (0, n_x - 1), (n_cp - 1, 0)]
    odd = [o for o in chips if o[0] % 2 and o[1] % 2]
    even = [o for o in chips if not (o[0] % 2 or o[1] % 2)][::-1]
    rest = [o for o in chips if o not in near + odd + even]
    plan = [[(dy, dx, dc) for dc in range(2) for dy, dx in g] for g in (near, odd, even, rest)]
    n_grp = len(plan)

    def fwd(j, r):
        dy, dx, dc = plan[j][r]
        return (cp + dy) % n_cp, ((x_pos + dx) % n_x) * 2 + (core + dc) % 2

    def back(j, r):
        dy, dx, dc = plan[j][r]
        return (cp + n_cp - dy) % n_cp, ((x_pos + n_x - dx) % n_x) * 2 + (core + dc) % 2

    def local(j, r):
        return plan[j][r] == (0, 0, 0)

    barrier = pltpu.get_barrier_semaphore()
    for j in range(n_grp):
        for r in range(per_grp):
            if not local(j, r):
                c, t = fwd(j, r)
                pl.semaphore_signal(barrier, inc=1, device_id={'cp': c, 'tp': t}, device_id_type=MESH)
    loads = [pltpu.make_async_copy(wg_hbm, wg, wsem.at[0]), pltpu.make_async_copy(wu_hbm, wu, wsem.at[1]), pltpu.make_async_copy(wd_hbm, wd, wsem.at[2])]
    for ld in loads:
        ld.start()

    e_iota = lax.broadcasted_iota(jnp.int32, (experts, rows), 0)
    hit = jnp.zeros((experts, rows), jnp.float32)
    gsel = jnp.zeros((experts, rows), jnp.float32)
    for k in range(top_k):
        m = idx_ref[k:k + 1, :] == e_iota
        hit = hit + jnp.where(m, 1.0, 0.0)
        gsel = gsel + jnp.where(m, gate_ref[k:k + 1, :], 0.0)
    before = jnp.where(lax.broadcasted_iota(jnp.int32, (rows, rows), 0) < lax.broadcasted_iota(jnp.int32, (rows, rows), 1), 1.0, 0.0)
    count = jnp.dot(hit.astype(jnp.bfloat16), before.astype(jnp.bfloat16), preferred_element_type=jnp.float32)
    slots[...] = jnp.where(hit > 0.5, count, -1.0)
    slots16[...] = slots[...].astype(jnp.bfloat16)
    gates[...] = gsel
    c_iota = lax.broadcasted_iota(jnp.int32, (cap, rows), 0).astype(jnp.float32)

    def build(j, ref):
        for e in range(local_exp):
            for r in range(per_grp):
                c, t = fwd(j, r)
                expert = (c * (2 * n_x) + t) * local_exp + e
                eq = jnp.broadcast_to(slots[pl.ds(expert, 1), :], (cap, rows)) == c_iota
                val = jnp.broadcast_to(gates[pl.ds(expert, 1), :], (cap, rows))
                ref[pl.ds((e * per_grp + r) * cap, cap), :] = jnp.where(eq, val, 0.0)

    steps = (0, 1, n_x - 1, 2)
    where_is = {plan[j][r]: (j, r) for j in range(n_grp) for r in range(per_grp)}
    mid = hidden // 2
    cols_of = (pl.ds(0, mid), pl.ds(mid, mid))

    def peer(axis, d, dc):
        if axis == 0:
            return cp, ((x_pos + d) % n_x) * 2 + (core + dc) % 2
        return (cp + d) % n_cp, x_pos * 2 + (core + dc) % 2

    def table(axis, d):
        c, t = peer(axis, d, 0)
        return pltpu.make_async_remote_copy(slots16, tabs.at[axis, d - 1], tsem.at[axis, d - 1], tgot.at[axis, d - 1], device_id={'cp': c, 'tp': t}, device_id_type=MESH)

    h_half = rows // 2
    h_parts = (pl.ds(0, h_half), pl.ds(h_half, h_half))

    def spread(axis, d, p):
        c, t = peer(axis, d, 0)
        return pltpu.make_async_remote_copy(h_in.at[h_parts[p], cols_of[axis]], held.at[axis, d - 1, h_parts[p]], hsem.at[axis, d - 1, p], hgot.at[axis, d - 1, p], device_id={'cp': c, 'tp': t}, device_id_type=MESH)

    def onward(axis, p):
        d = (1, n_x - 1)[p]
        c, t = peer(axis, d, 0)
        return pltpu.make_async_remote_copy(held.at[axis, d - 1, h_parts[p]], held.at[axis, 1, h_parts[p]], hsem.at[axis, 1, p], hgot.at[axis, 1, p], device_id={'cp': c, 'tp': t}, device_id_type=MESH)

    spreads = [(axis, d, p) for d, p in ((1, 0), (n_x - 1, 1), (1, 1), (n_x - 1, 0)) for axis in range(2)]
    onwards = [(axis, p) for p in range(2) for axis in range(2)]

    def piece(axis, s, d, dc, e):
        c, t = peer(1 - axis, d, dc)
        k = e * per_grp + d * 2 + dc
        j, r = where_is[(d, s, dc) if axis == 0 else (s, d, dc)]
        src, dst = send.at[axis, s, k], recv.at[j, e * per_grp + r, :, cols_of[axis]]
        got = rsem.at[axis, j, e * per_grp + r]
        if d == 0 and dc == 0:
            return pltpu.make_async_copy(src, dst, got)
        return pltpu.make_async_remote_copy(src, dst, ssem.at[axis, s, k], got, device_id={'cp': c, 'tp': t}, device_id_type=MESH)

    def pieces():
        return [(axis, d, dc, e) for e in range(local_exp) for d in (2, 1, n_x - 1, 0) for dc in range(2) for axis in range(2)]

    def select(axis, s):
        tab = slots if s == 0 else slots_of
        if s:
            slots_of[...] = tabs[axis, s - 1].astype(jnp.float32)
        for d in range(n_x):
            for dc in range(2):
                c, t = peer(1 - axis, d, dc)
                for e in range(local_exp):
                    expert = (c * (2 * n_x) + t) * local_exp + e
                    eq = jnp.broadcast_to(tab[pl.ds(expert, 1), :], (cap, rows)) == c_iota
                    dmat[pl.ds((e * per_grp + d * 2 + dc) * cap, cap), :] = jnp.where(eq, 1.0, 0.0)

        def fill(n, carry):
            cols = pl.ds(pl.multiple_of(n * wide, wide), wide)
            if s == 0:
                from_h = h_in[:, pl.ds(pl.multiple_of(axis * mid + n * wide, wide), wide)]
            else:
                from_h = held[axis, s - 1, :, cols]
            picked = jnp.dot(dmat[...].astype(jnp.bfloat16), from_h, preferred_element_type=jnp.float32).astype(jnp.bfloat16)
            send[axis, s, :, :, cols] = picked.reshape(local_exp * per_grp, cap, wide)
            return carry

        lax.fori_loop(0, mid // wide, fill, 0)

    def giveback(j, r, e):
        c, t = back(j, r)
        if local(j, r):
            return (pltpu.make_async_copy(recv.at[j, e * per_grp + r], ret.at[j, e * per_grp + r], csem.at[j, e * per_grp + r]))
        return (pltpu.make_async_remote_copy(recv.at[j, e * per_grp + r], ret.at[j, e * per_grp + r], bsem.at[j, e * per_grp + r], csem.at[j, e * per_grp + r], device_id={'cp': c, 'tp': t}, device_id_type=MESH))

    grp_rows = local_exp * per_grp * cap
    half = per_grp * cap
    wide = 512
    order = range(per_grp)
    pl.semaphore_wait(barrier, n_grp * per_grp - 1)
    for axis, d, p in spreads:
        spread(axis, d, p).start()
    for d in steps[1:]:
        for axis in range(2):
            table(axis, d).start()
    for axis in range(2):
        select(axis, 0)
    for axis, p in onwards:
        spread(axis, (1, n_x - 1)[p], p).wait_recv()
        onward(axis, p).start()
    for axis, d, dc, e in pieces():
        piece(axis, 0, d, dc, e).start()
    for s in steps[1:]:
        for axis in range(2):
            table(axis, s).wait_recv()
            if s == 2:
                for p in range(2):
                    onward(axis, p).wait_recv()
            else:
                spread(axis, s, 1 if s == 1 else 0).wait_recv()
            select(axis, s)
        for axis, d, dc, e in pieces():
            piece(axis, s, d, dc, e).start()

    def init(n, carry):
        cols = pl.ds(pl.multiple_of(n * wide, wide), wide)
        acc[:, cols] = h_in[:, cols].astype(jnp.float32)
        return carry

    lax.fori_loop(0, hidden // wide, init, 0)
    for ld in loads:
        ld.wait()
    ffn = wg.shape[2]
    for j in range(n_grp):
        for e in range(local_exp):
            for r in order:
                dy, dx, dc = plan[j][r]
                for axis, (s, d) in enumerate(((dx, dy), (dy, dx))):
                    cpy = piece(axis, s, d, dc, e)
                    if d == 0 and dc == 0:
                        cpy.wait()
                    else:
                        cpy.wait_recv()

            def up(n, carry, j=j, e=e):
                cols = pl.ds(pl.multiple_of(n * 256, 256), 256)
                rows_in = recv[j, pl.ds(e * per_grp, per_grp)].reshape(half, hidden)
                g = jnp.dot(rows_in, wg[e, :, cols], preferred_element_type=jnp.float32)
                u = jnp.dot(rows_in, wu[e, :, cols], preferred_element_type=jnp.float32)
                hid[:, cols] = (g * (1.0 / (1.0 + jnp.exp(-g))) * u).astype(jnp.bfloat16)
                return carry

            def down(n, carry, j=j, e=e):
                cols = pl.ds(pl.multiple_of(n * wide, wide), wide)
                z = jnp.dot(hid[...], wd[e, :, cols], preferred_element_type=jnp.float32).astype(jnp.bfloat16)
                recv[j, pl.ds(e * per_grp, per_grp), :, cols] = z.reshape(per_grp, cap, wide)
                return carry

            lax.fori_loop(0, ffn // 256, up, 0)
            lax.fori_loop(0, hidden // wide, down, 0)
            for r in order:
                giveback(j, r, e).start()

    for j in range(n_grp):
        build(j, gmat)
        g0 = gmat[...].T
        hi = g0.astype(jnp.bfloat16)
        g1 = g0 - hi.astype(jnp.float32)
        mid_g = g1.astype(jnp.bfloat16)
        gsp[0] = hi
        gsp[1] = mid_g
        gsp[2] = (g1 - mid_g.astype(jnp.float32)).astype(jnp.bfloat16)
        for e in range(local_exp):
            for r in order:
                if local(j, r):
                    giveback(j, r, e).wait()
                else:
                    giveback(j, r, e).wait_recv()

        def comb(n, carry, j=j):
            cols = pl.ds(pl.multiple_of(n * wide, wide), wide)
            z = ret[j, :, :, cols].reshape(grp_rows, wide)
            tot = jnp.dot(gsp[2], z, preferred_element_type=jnp.float32)
            tot = tot + jnp.dot(gsp[1], z, preferred_element_type=jnp.float32)
            tot = tot + jnp.dot(gsp[0], z, preferred_element_type=jnp.float32)
            if j == n_grp - 1:
                y_ref[:, cols] = (acc[:, cols] + tot).astype(jnp.bfloat16)
            else:
                acc[:, cols] += tot
            return carry

        lax.fori_loop(0, hidden // wide, comb, 0)

    for j in range(n_grp):
        for r in range(per_grp):
            if not local(j, r):
                for e in range(local_exp):
                    giveback(j, r, e).wait_send()
    for axis in range(2):
        for d in steps[1:]:
            table(axis, d).wait_send()
        for p in range(2):
            onward(axis, p).wait_send()
    for axis, d, p in spreads:
        spread(axis, d, p).wait_send()
    for s in steps:
        for axis, d, dc, e in pieces():
            if d or dc:
                piece(axis, s, d, dc, e).wait_send()


def expert_layer(mesh, resid_h, expert_idx, gate_vals, w_gate, w_up, w_down):
    n_cp, n_x = mesh.shape['cp'], mesh.shape['tp'] // 2
    rows, hidden = resid_h.shape
    top_k = expert_idx.shape[1]
    local_exp, _, ffn = w_gate.shape
    experts = local_exp * n_cp * n_x * 2
    cap = rows * top_k // experts
    slots = local_exp * 2 * n_x
    dims = (n_cp, n_x, top_k, experts, cap, local_exp)
    vm = pl.BlockSpec(memory_space=pltpu.VMEM)
    hb = pl.BlockSpec(memory_space=pl.ANY)
    dma = pltpu.SemaphoreType.DMA
    sems = [dma((2, n_x, slots)), dma((2, n_cp, slots)), dma((n_cp, slots)), dma((n_cp, slots))] + [dma((2, n_x - 1))] * 2 + [dma((2, n_x - 1, 2))] * 2
    return pl.pallas_call(
        functools.partial(moe_kernel, dims),
        out_shape=jax.ShapeDtypeStruct((rows, hidden), jnp.bfloat16),
        in_specs=[vm, vm, vm, hb, hb, hb],
        out_specs=vm,
        scratch_shapes=[
            pltpu.VMEM((local_exp, hidden, ffn), jnp.bfloat16),
            pltpu.VMEM((local_exp, hidden, ffn), jnp.bfloat16),
            pltpu.VMEM((local_exp, ffn, hidden), jnp.bfloat16),
            pltpu.VMEM((2, n_x, slots, cap, hidden // 2), jnp.bfloat16),
            pltpu.VMEM((n_cp, slots, cap, hidden), jnp.bfloat16),
            pltpu.VMEM((n_cp, slots, cap, hidden), jnp.bfloat16),
            pltpu.VMEM((experts, rows), jnp.float32),
            pltpu.VMEM((experts, rows), jnp.float32),
            pltpu.VMEM((experts, rows), jnp.bfloat16),
            pltpu.VMEM((experts, rows), jnp.float32),
            pltpu.VMEM((2, n_x - 1, experts, rows), jnp.bfloat16),
            pltpu.VMEM((2, n_x - 1, rows, hidden // 2), jnp.bfloat16),
            pltpu.VMEM((slots * cap, rows), jnp.float32),
            pltpu.VMEM((slots * cap, rows), jnp.float32),
            pltpu.VMEM((3, rows, slots * cap), jnp.bfloat16),
            pltpu.VMEM((rows, hidden), jnp.float32),
            pltpu.VMEM((2 * n_x * cap, ffn), jnp.bfloat16),
            pltpu.SemaphoreType.DMA((3,)),
        ] + sems,
        compiler_params=pltpu.CompilerParams(collective_id=1, has_side_effects=True, vmem_limit_bytes=64 * 1024 * 1024 - 65536),
        name='moe',
    )(resid_h, expert_idx.T, gate_vals.T, w_gate, w_up, w_down)


def solution(mesh):
    row_spec = P(('dp', 'cp', 'tp'), None)
    head_spec = P(None, 'tp', None)
    expert_spec = P(('cp', 'tp'), None, None)

    def device_step(hidden_in, w_query, w_key, w_value, w_out, expert_idx, gate_vals, w_gate, w_up, w_down):
        resid_h = attention_residual(mesh, hidden_in, w_query, w_key, w_value, w_out)
        return expert_layer(mesh, resid_h, expert_idx, gate_vals, w_gate, w_up, w_down)

    return jax.shard_map(device_step, mesh=mesh, in_specs=(row_spec, head_spec, head_spec, head_spec, P('tp', None, None), row_spec, row_spec, expert_spec, expert_spec, expert_spec), out_specs=row_spec, check_vma=False)
```
